128 devices in a mesh: node: 16 (over z, x), local: 8 (over y, core).
Axes of the slice: x: 4, y: 4, z: 4, core: 2. Of those that a mesh axis runs over, the one named last changes fastest.
Arguments:
- tokens: bfloat16 [65536, 2048], P(('node', 'local')), may hold values from -64 to 64, as said below
- d_out: bfloat16 [65536, 1024], P(('node', 'local')), may hold values from -6 to 6
- w_query: bfloat16 [2048, 1536], P('local'), may hold values from -0.125 to 0.125
- w_down: bfloat16 [2048, 576], P('local'), may hold values from -0.125 to 0.125
- w_up: bfloat16 [512, 2048], P('local'), may hold values from -0.25 to 0.25
- latent_gain: bfloat16 [512], P('local'), may hold values from 0.5 to 1.5
Outputs:
- grad_query: float32 [2048, 1536], P(('node', 'local'))
- grad_down: float32 [2048, 576], P(('node', 'local'))
- grad_up: float32 [512, 2048], P(('node', 'local'))
- grad_gain: float32 [512], P(('node', 'local'))
- grad_tokens: bfloat16 [65536, 2048], P(('node', 'local'))
The draws below stay inside these ranges and needn't reach their ends.
Inputs may be any that keep to these rules, and one draw needn't show every extreme that they name: `tokens`: real-valued rows of the layer's normed input.
All inputs are finite; a program needn't handle non-finite values.
Results may differ from the reference program's by a relative error of at most 0.014.
The reference program's roundings to bfloat16 on the way (of `query`, `normed`, `keyval`, `probs_b`, `dscores`, `query_grad`, `keyval_grad` and `down_grad`) count: a program that leaves them out, or rounds other values in their place, can miss the bound.
Values may be sent and summed in bfloat16 or wider, within the bound.
A program may use at most 128 MiB of HBM per device.

```python
import math
import jax
import jax.numpy as jnp
from jax import lax

D = 2048
H = 8
DN = 128
DR = 64
DV = 128
KVL = 512
SEQ = 512
TOKENS = 65536
NPARAM = 5374464


def draw_tokens(key, part):
    first = jax.random.fold_in(jax.random.fold_in(key, 17), 0)
    base = jax.random.truncated_normal(first, -4.0, 4.0, (TOKENS, D), jnp.float32)
    columns = jnp.exp(jnp.log(3.0) * jnp.arange(D, dtype=jnp.float32) / (D - 1))
    return (base * columns[None, :]).astype(jnp.bfloat16)


def level_of(own_key, extent, cuts, least, largest):
    level, own = 1.0, jax.random.fold_in(own_key, 6)
    for dim, shards_of in cuts:
        draws = jnp.exp(jax.random.uniform(jax.random.fold_in(own, dim), (shards_of,), jnp.float32, least / len(cuts), largest / len(cuts)))
        level = level * jnp.repeat(draws, extent[dim] // shards_of).reshape([-1 if axis == dim else 1 for axis in range(len(extent))])
    return level


def normal_values(key, shape, scale, bound, pieces=(), kind=jnp.bfloat16):
    factor_of = level_of(key, shape, pieces, -0.22, 0.18) if pieces else 1.0
    entries = jax.random.normal(key, shape, jnp.float32) * scale * factor_of
    return jnp.minimum(jnp.maximum(entries, -bound), bound).astype(kind)


def setup_inputs(seed: int = 0) -> dict:
    key_list = jax.random.split(jax.random.key(seed), 7)
    tokens = draw_tokens(jax.random.fold_in(key_list[6], 71), 0)
    d_out = normal_values(key_list[1], (TOKENS, H * DV), 1.0, 6.0, ((0, 128),))
    w_query = normal_values(key_list[2], (D, H * (DN + DR)), D ** -0.5, 0.125, ((0, 8),))
    w_down = normal_values(key_list[3], (D, KVL + DR), D ** -0.5, 0.125, ((0, 8),))
    w_up = normal_values(key_list[4], (KVL, H * (DN + DV)), KVL ** -0.5, 0.25, ((0, 8),))
    latent_gain = jnp.clip(1.0 + 0.1 * jax.random.normal(key_list[5], (KVL,), jnp.float32), 0.5, 1.5).astype(jnp.bfloat16)
    return dict(tokens=tokens, d_out=d_out, w_query=w_query, w_down=w_down, w_up=w_up, latent_gain=latent_gain)


EPSILON = 1e-06
ROPE_BASE = 10000.0

def rope_tables(length, width):
    position = jnp.arange(length, dtype=jnp.float32)[:, None]
    freq = ROPE_BASE ** (-jnp.arange(width // 2, dtype=jnp.float32) * 2.0 / width)
    angle = position * freq[None, :]
    return (jnp.cos(angle), jnp.sin(angle))

def rotate(values, cosine, sine):
    half = values.shape[-1] // 2
    first = values[..., :half]
    second = values[..., half:]
    return jnp.concatenate([first * cosine - second * sine, second * cosine + first * sine], -1)

def local_backward(query32, down32, d_o, w_up, gain):
    length = query32.shape[0]
    cosine, sine = rope_tables(length, DR)
    query = query32.astype(jnp.bfloat16).reshape(length, H, DN + DR)
    latent = down32[:, :KVL]
    rope_raw = down32[:, KVL:]
    inv_rms = lax.rsqrt(lax.optimization_barrier(jnp.mean(latent * latent, axis=-1, keepdims=True)) + EPSILON)
    unit = latent * inv_rms
    gain32 = gain.astype(jnp.float32)
    normed = (unit * gain32).astype(jnp.bfloat16)
    keyval = jnp.dot(normed, w_up, preferred_element_type=jnp.float32).astype(jnp.bfloat16)
    keyval = keyval.reshape(length, H, DN + DV)
    key_nope = keyval[..., :DN]
    values = keyval[..., DN:]
    query_rope = rotate(query[..., DN:].astype(jnp.float32), cosine[:, None, :], sine[:, None, :]).astype(jnp.bfloat16)
    key_rope = rotate(rope_raw, cosine, sine).astype(jnp.bfloat16)
    query_full = jnp.concatenate([query[..., :DN], query_rope], -1)
    key_full = jnp.concatenate([key_nope, jnp.broadcast_to(key_rope[:, None, :], (length, H, DR))], -1)
    scale = 1.0 / math.sqrt(DN + DR)
    scores = jnp.einsum('qhd,khd->hqk', query_full.astype(jnp.float32), key_full.astype(jnp.float32)) * scale
    causal = jnp.arange(length)[:, None] >= jnp.arange(length)[None, :]
    scores = jnp.where(causal[None], scores, -1e+30)
    highest = lax.optimization_barrier(jnp.max(scores, axis=-1, keepdims=True))
    weights = jnp.exp(scores - highest)
    probs = weights / lax.optimization_barrier(jnp.sum(weights, axis=-1, keepdims=True))
    probs_b = probs.astype(jnp.bfloat16)
    grad_out = d_o.reshape(length, H, DV)
    dprobs = jnp.einsum('qhd,khd->hqk', grad_out.astype(jnp.float32), values.astype(jnp.float32))
    delta = lax.optimization_barrier(jnp.sum(probs * dprobs, axis=-1, keepdims=True))
    dscores = (probs * (dprobs - delta) * scale).astype(jnp.bfloat16)
    dquery = jnp.einsum('hqk,khd->qhd', dscores.astype(jnp.float32), key_full.astype(jnp.float32))
    dkey = jnp.einsum('hqk,qhd->khd', dscores.astype(jnp.float32), query_full.astype(jnp.float32))
    dvalues = jnp.einsum('hqk,qhd->khd', probs_b.astype(jnp.float32), grad_out.astype(jnp.float32))
    dquery_rope = rotate(dquery[..., DN:], cosine[:, None, :], -sine[:, None, :])
    query_grad = jnp.concatenate([dquery[..., :DN], dquery_rope], -1).reshape(length, H * (DN + DR)).astype(jnp.bfloat16)
    rope_grad = rotate(lax.optimization_barrier(jnp.sum(dkey[..., DN:], axis=1)), cosine, -sine)
    keyval_grad = jnp.concatenate([dkey[..., :DN], dvalues], -1).reshape(length, H * (DN + DV)).astype(jnp.bfloat16)
    normed_grad = jnp.dot(keyval_grad, w_up.T, preferred_element_type=jnp.float32)
    gain_term = lax.optimization_barrier(jnp.sum(normed_grad * unit, axis=0))
    scaled = normed_grad * gain32
    latent_grad = inv_rms * (scaled - unit * lax.optimization_barrier(jnp.mean(scaled * unit, axis=-1, keepdims=True)))
    down_grad = jnp.concatenate([latent_grad, rope_grad], -1).astype(jnp.bfloat16)
    return (query_grad, down_grad, normed, keyval_grad, gain_term)

def reference(tokens, d_out, w_query, w_down, w_up, latent_gain):
    count = tokens.shape[0] // SEQ
    seq_tokens = tokens.reshape(count, SEQ, D)
    seq_grads = d_out.reshape(count, SEQ, H * DV)

    def one_sequence(pair):
        inputs, d_o = pair
        query32 = jnp.dot(inputs, w_query, preferred_element_type=jnp.float32)
        down32 = jnp.dot(inputs, w_down, preferred_element_type=jnp.float32)
        query_grad, down_grad, normed, keyval_grad, gain_term = local_backward(query32, down32, d_o, w_up, latent_gain)
        input_grad = jnp.dot(query_grad, w_query.T, preferred_element_type=jnp.float32)
        input_grad = input_grad + jnp.dot(down_grad, w_down.T, preferred_element_type=jnp.float32)
        joined = jnp.concatenate([query_grad, down_grad], 1)
        return (input_grad.astype(jnp.bfloat16), joined, normed, keyval_grad, gain_term)
    token_grads, joined, normed, keyval_grad, gain_terms = lax.map(one_sequence, (seq_tokens, seq_grads))
    input_sum = jnp.dot(tokens.T, joined.reshape(-1, joined.shape[-1]), preferred_element_type=jnp.float32)
    up_sum = jnp.dot(normed.reshape(-1, KVL).T, keyval_grad.reshape(-1, H * (DN + DV)), preferred_element_type=jnp.float32)
    gain_sum = lax.optimization_barrier(jnp.sum(gain_terms, axis=0))
    total = jnp.sum(input_sum * input_sum) + jnp.sum(up_sum * up_sum) + jnp.sum(gain_sum * gain_sum)
    clip = jnp.minimum(1.0, lax.rsqrt(total / NPARAM + 1e-06))
    width_query = H * (DN + DR)
    return (input_sum[:, :width_query] * clip, input_sum[:, width_query:] * clip, up_sum * clip, gain_sum * clip, token_grads.reshape(-1, D))
```

```python
import math

import jax
import jax.numpy as jnp
import numpy as np
from jax import lax
from jax.experimental import pallas as pl
from jax.experimental.pallas import tpu as pltpu
from jax.sharding import Mesh
from jax.sharding import PartitionSpec as P

H = 8
DN = 128
DR = 64
DV = 128
KVL = 512
SEQ = 512
D = 2048
NPARAM = 5374464
EPSILON = 1e-06
ROPE_BASE = 10000.0
LOCAL = ("local_0", "local_1")
NODE_LOCAL = ("node_0", "node_1", "local_0", "local_1")
MESH = pl.DeviceIdType.MESH
AZ, AX, AY, AC = NODE_LOCAL

WCOL = 2176
SCALE = 1.0 / math.sqrt(DN + DR)
GROUPS = ((512, AZ, AX, AY), (512, AX, AY, AZ), (384, AY, AZ, AX))
GOFF = (0, 512, 1024)
GTOT = 1408
F32 = jnp.float32
BF16 = jnp.bfloat16


def rope_constants():
    position = np.arange(SEQ, dtype=np.float32)[:, None]
    freq = np.float32(ROPE_BASE) ** (-np.arange(DR // 2, dtype=np.float32) * np.float32(2.0 / DR))
    angle = (position * freq[None, :].astype(np.float32)).astype(np.float32)
    cosine = np.cos(angle).astype(np.float32)
    sine = np.sin(angle).astype(np.float32)
    return np.concatenate([cosine] * 4, 1), np.concatenate([-sine, sine] * 2, 1)


def nt(a, b):
    return lax.dot_general(a, b, (((1,), (1,)), ((), ())), preferred_element_type=F32)


def nn(a, b):
    return jnp.dot(a, b, preferred_element_type=F32)


def tn(a, b):
    return lax.dot_general(a, b, (((0,), (0,)), ((), ())), preferred_element_type=F32)


def mega(
    tokens_hbm, dout_hbm, cos_hbm, sin_hbm, wq_ref, wd_ref, wu_ref, gain_ref,
    fin_ref, clip_ref, tg_hbm,
    tokens, dout, cosr, sinr, wbuf, ubuf, gbuf, tokt, acc, qrope, qnope, nrm, nrt, ng, krp, dkr,
    jb, jp, kvg, kvgp, rg, rgp, rgf, invr, gmat, tgb,
    p0, p1, p2, own0, own1, own2, rx0, rx1, rx2, ra0, ra1, ra2,
    q0, q1, q2, rx20, rx21, rx22, ra20, ra21, ra22,
    s0, s1, s2, rx30, rx31, rx32, ra30, ra31, ra32,
    nbuf, lsem, ssem, rsem,
):
    iz, ix, iy, ic = (lax.axis_index(a) for a in NODE_LOCAL)
    at = {AZ: iz, AX: ix, AY: iy}
    other = 1 - ic

    def step(axis, by):
        return lax.rem(at[axis] + (by + 4), 4)

    sends = []
    table = {}

    def sem_of(key):
        return table.setdefault(key, len(table))

    def send(key, src, dst, peer):
        k = sem_of(key)
        d = pltpu.make_async_remote_copy(
            src_ref=src, dst_ref=dst, send_sem=ssem.at[k], recv_sem=rsem.at[k],
            device_id=peer, device_id_type=MESH)
        d.start()
        sends.append(d)

    def arrived(key, dst):
        k = sem_of(key)
        pltpu.make_async_remote_copy(
            src_ref=dst, dst_ref=dst, send_sem=ssem.at[k], recv_sem=rsem.at[k],
            device_id={AC: other}, device_id_type=MESH).wait_recv()

    mate = {AC: other}
    locals_ = []
    for n, (src, dst) in enumerate(((tokens_hbm, tokens), (dout_hbm, dout), (cos_hbm, cosr), (sin_hbm, sinr))):
        d = pltpu.make_async_copy(src, dst, lsem.at[n])
        d.start()
        locals_.append(d)

    barrier = pltpu.get_barrier_semaphore()
    for axis in (AZ, AX, AY):
        for by in (1, -1, 2):
            pl.semaphore_signal(barrier, inc=1, device_id={axis: step(axis, by)}, device_id_type=MESH)
    pl.semaphore_signal(barrier, inc=1, device_id=mate, device_id_type=MESH)

    for h in range(H):
        wbuf[iy, ic, :, :, h * 128:(h + 1) * 128] = wq_ref[:, h * 192:h * 192 + 128].reshape(8, 32, 128)
    for h in range(0, H, 2):
        pair = jnp.concatenate(
            [wq_ref[:, h * 192 + 128:h * 192 + 192], wq_ref[:, h * 192 + 320:h * 192 + 384]], 1)
        wbuf[iy, ic, :, :, 1024 + h * 64:1024 + h * 64 + 128] = pair.reshape(8, 32, 128)
    wbuf[iy, ic, :, :, 1536:2048] = wd_ref[:, :512].reshape(8, 32, 512)
    last = jnp.concatenate([wd_ref[:, 512:576], jnp.zeros((256, 64), BF16)], 1)
    wbuf[iy, ic, :, :, 2048:2176] = last.reshape(8, 32, 128)
    for p in range(8):
        ubuf[iy, ic, p] = wu_ref[:, p * 256:(p + 1) * 256]
    gbuf[iy, ic] = jnp.broadcast_to(
        jnp.concatenate([gain_ref[...].astype(F32), jnp.zeros((1, 64), F32)], 1), (8, 128))
    pl.semaphore_wait(barrier, 10)

    RING = (AX, AZ)
    YO = (step(AY, -1), step(AY, 1), step(AY, 2))

    def wpiece(yy, k, q):
        return wbuf.at[yy, ic, k * 4 + q]

    def upiece(yy, k, q):
        return ubuf.at[yy, ic, k * 4 + q]

    def halves(ref, rows):
        return ref.at[0:rows // 2], ref.at[rows // 2:rows]

    KIND = {"w": (wpiece, 32), "u": (upiece, 64)}

    def y_send(kind, k):
        piece, _ = KIND[kind]
        r = piece(iy, k, at[RING[k]])
        send((kind, "y", k, 0), r, r, {AY: step(AY, 1)})
        send((kind, "y", k, 1), r, r, {AY: step(AY, -1)})

    def p_send(kind, k, yo):
        piece, _ = KIND[kind]
        r = piece(YO[yo], k, at[RING[k]])
        send((kind, "p", k, yo, 0), r, r, {RING[k]: step(RING[k], 1)})
        send((kind, "p", k, yo, 1), r, r, {RING[k]: step(RING[k], -1)})

    def y_take(kind, k, d):
        piece, rows = KIND[kind]
        r = piece(YO[d], k, at[RING[k]])
        arrived((kind, "y", k, d), r)
        half = halves(r, rows)[d]
        send((kind, "y2", k, d), half, half, {AY: step(AY, 1 if d == 0 else -1)})
        p_send(kind, k, d)

    def y2_take(kind, k):
        piece, rows = KIND[kind]
        r = piece(YO[2], k, at[RING[k]])
        for d in range(2):
            arrived((kind, "y2", k, d), halves(r, rows)[d])
        p_send(kind, k, 2)

    def p_take(kind, k, yo):
        piece, rows = KIND[kind]
        for d in range(2):
            r = piece(YO[yo], k, step(RING[k], -1 if d == 0 else 1))
            arrived((kind, "p", k, yo, d), r)
            half = halves(r, rows)[d]
            send((kind, "p2", k, yo, d), half, half, {RING[k]: step(RING[k], 1 if d == 0 else -1)})

    def p2_take(kind, k, yo):
        piece, rows = KIND[kind]
        r = piece(YO[yo], k, step(RING[k], 2))
        for d in range(2):
            arrived((kind, "p2", k, yo, d), halves(r, rows)[d])

    def to_mate(kind, yo):
        buf = wbuf if kind == "w" else ubuf
        yy = iy if yo is None else YO[yo]
        send((kind, "d", yo), buf.at[yy, ic], buf.at[yy, ic], mate)

    def from_mate(kind, yo):
        buf = wbuf if kind == "w" else ubuf
        yy = iy if yo is None else YO[yo]
        arrived((kind, "d", yo), buf.at[yy, other])

    def project(yo):
        yy = iy if yo is None else YO[yo]
        left = tokens[:, pl.ds(pl.multiple_of(yy * 512, 512), 512)]
        for lo, hi in ((0, 768), (768, 1536), (1536, 2176)):
            w = wbuf[yy, :, :, :, lo:hi].reshape(512, hi - lo)
            if yo is None:
                acc[:, lo:hi] = nn(left, w)
            else:
                acc[:, lo:hi] += nn(left, w)

    for k in range(2):
        y_send("w", k)
    to_mate("w", None)
    to_mate("u", None)
    g = gbuf.at[iy, ic]
    for n, by in enumerate((1, -1, 2)):
        send(("g", n), g, g, {AY: step(AY, by)})
    send(("gd", 3), g, g, mate)

    locals_[0].wait()

    for z in range(4):
        tokt[0, z] = tokens[:, z * 512:(z + 1) * 512].T.reshape(4, 4, 32, 512)
    for k in range(2):
        for d in range(2):
            y_take("w", k, d)
    for k in range(2):
        y_send("u", k)
    send(("tok",), tokt.at[0], tokt.at[1], mate)
    from_mate("w", None)
    project(None)
    for k in range(2):
        y2_take("w", k)
    for k in range(2):
        p_take("w", k, 0)
    for k in range(2):
        for d in range(2):
            y_take("u", k, d)
    for k in range(2):
        p_take("w", k, 1)
    for k in range(2):
        p2_take("w", k, 0)
    to_mate("w", 0)
    for k in range(2):
        y2_take("u", k)
    for k in range(2):
        p2_take("w", k, 1)
    to_mate("w", 1)
    for k in range(2):
        p_take("w", k, 2)
    for yo in range(2):
        for k in range(2):
            p_take("u", k, yo)
    from_mate("w", 0)
    project(0)
    for k in range(2):
        p2_take("w", k, 2)
    to_mate("w", 2)
    for k in range(2):
        p_take("u", k, 2)
    from_mate("w", 1)
    project(1)
    for n, by in enumerate((-1, 1, 2)):
        gg = gbuf.at[step(AY, by), ic]
        arrived(("g", n), gg)
        send(("gd", n), gg, gg, mate)
    for yo in range(3):
        for k in range(2):
            p2_take("u", k, yo)
        to_mate("u", yo)
    from_mate("w", 2)
    project(2)
    for n, by in enumerate((-1, 1, 2)):
        arrived(("gd", n), gbuf.at[step(AY, by), other])
    arrived(("gd", 3), gbuf.at[iy, other])

    for d in locals_[1:]:
        d.wait()

    lane = lax.broadcasted_iota(jnp.int32, (1, 128), 1)
    low = lax.rem(lane, 64) < 32

    def swap(v):
        return jnp.where(low, pltpu.roll(v, 96, 1), pltpu.roll(v, 32, 1))

    def rot(v, sign):
        return v * cosr[...] + swap(v) * (sinr[...] * sign)

    gain = jnp.concatenate([gbuf[y, c, 0:1, 0:64] for y in range(4) for c in range(2)], 1)
    for n in range(4):
        cols = slice(1024 + n * 128, 1152 + n * 128)
        qrope[:, n * 128:(n + 1) * 128] = rot(acc[:, cols].astype(BF16).astype(F32), 1.0).astype(BF16)
    for n in range(8):
        qnope[:, n * 128:(n + 1) * 128] = acc[:, n * 128:(n + 1) * 128].astype(BF16)
    kr = rot(acc[:, 2048:2176], 1.0)
    krp[0] = jnp.where(lane < 64, kr, 0.0).astype(BF16)
    krp[1] = jnp.where(lane < 64, 0.0, pltpu.roll(kr, 64, 1)).astype(BF16)
    for n in range(4):
        rows = slice(n * 128, (n + 1) * 128)
        latent = acc[rows, 1536:2048]
        inv = lax.rsqrt(jnp.mean(latent * latent, axis=-1, keepdims=True) + EPSILON)
        unit = latent * inv
        acc[rows, 1536:2048] = unit
        invr[rows] = jnp.broadcast_to(inv, (128, 128))
        nrm[rows] = (unit * gain).astype(BF16)
    nrt[0] = nrm[...].T
    send(("nrt",), nrt.at[0], nrt.at[1], mate)
    ng[...] = jnp.zeros((512, 512), F32)
    dkr[...] = jnp.zeros((512, 128), F32)
    for yo in range(3):
        from_mate("u", yo)
    from_mate("u", None)

    tri = (lax.broadcasted_iota(jnp.int32, (256, 256), 0)
           <= lax.broadcasted_iota(jnp.int32, (256, 256), 1))

    def block(kf, v, qf, do, diag):
        rows = kf.shape[0]
        s = nt(kf, qf) * SCALE
        masked = jnp.where(tri, s[rows - 256:], -1e30)
        s = masked if rows == 256 else jnp.concatenate([s[:rows - 256], masked], 0)
        w = jnp.exp(s - jnp.max(s, axis=0, keepdims=True))
        probs = w * (1.0 / jnp.sum(w, axis=0, keepdims=True))
        dp = nt(v, do)
        delta = jnp.sum(probs * dp, axis=0, keepdims=True)
        ds = (probs * (dp - delta) * SCALE).astype(BF16)
        return probs.astype(BF16), ds

    def pair(n, carry):
        rope_cols = pl.ds(pl.multiple_of(n * 128, 128), 128)
        qr = qrope[:, rope_cols]
        total = None
        for e in range(2):
            h = 2 * n + e
            hc = pl.ds(pl.multiple_of(h * 128, 128), 128)
            u = ubuf[:, :, h].reshape(512, 256)
            kv = nn(nrm[...], u).astype(BF16)
            kf = jnp.concatenate([kv[:, :128], krp[e]], 1)
            v = kv[:, 128:]
            qf = jnp.concatenate([qnope[:, hc], qr], 1)
            do = dout[:, hc]
            pa, da = block(kf[:256], v[:256], qf[:256], do[:256], True)
            pb, db = block(kf, v, qf[256:], do[256:], False)
            dv = nn(pb, do[256:])
            dv = jnp.concatenate([dv[:256] + nn(pa, do[:256]), dv[256:]], 0)
            dk = nn(db, qf[256:])
            dk = jnp.concatenate([dk[:256] + nn(da, qf[:256]), dk[256:]], 0)
            dq = jnp.concatenate([tn(da, kf[:256]), tn(db, kf)], 0)
            jb[0, :, hc] = dq[:, :128].astype(BF16)
            total = dq[:, 128:] if e == 0 else total + dq[:, 128:]
            keep = lane < 64 if e == 0 else lane >= 64
            dkr[...] += jnp.where(keep, dk[:, 128:], 0.0)
            half, j = n // 2, lax.rem(n, 2) * 2 + e
            jc = pl.ds(pl.multiple_of(j * 128, 128), 128)
            kg = dk[:, :128].astype(BF16)
            vg = dv.astype(BF16)
            kvg[half, 0, :, jc] = kg
            kvg[half, 1, :, jc] = vg
            ng[...] += nt(jnp.concatenate([kg, vg], 1), u)
        jb[1, :, rope_cols] = rot(total, -1.0).astype(BF16)
        return carry

    lax.fori_loop(0, 4, pair, 0)
    send(("kvg",), kvg.at[other], kvgp, mate)

    gterm = jnp.zeros((1, 512), F32)
    for n in range(4):
        rows = slice(n * 128, (n + 1) * 128)
        unit = acc[rows, 1536:2048]
        grad = ng[rows]
        gterm = gterm + jnp.sum(grad * unit, axis=0, keepdims=True)
        scaled = grad * gain
        inner = jnp.mean(scaled * unit, axis=-1, keepdims=True)
        jb[1, rows, 512:1024] = (invr[rows, 0:1] * (scaled - unit * inner)).astype(BF16)
    dk = dkr[...]
    rope = jnp.where(lane < 64, rot(dk + pltpu.roll(dk, 64, 1), -1.0), 0.0)
    rgf[...] = rope.astype(BF16)
    rg[0] = jnp.where(lane < 32, rope, 0.0).astype(BF16)
    rg[1] = jnp.where(lane < 32, pltpu.roll(rope, 96, 1), 0.0).astype(BF16)
    send(("j",), jb.at[other], jp, mate)
    send(("rg",), rg.at[other], rgp, mate)
    column = jnp.broadcast_to(gterm, (128, 512)).T
    column = jnp.where(lane == 32, column, 0.0).reshape(64, 8, 128)
    gmat[...] = jnp.concatenate([column, jnp.zeros((64, 24, 128), F32)], 1).reshape(4, 4, 4, 32, 128)

    tgd = []

    def token_block(n):
        yy, cc = n // 2, n % 2
        w = wbuf[yy, cc].reshape(256, WCOL)
        out = nt(jb[0], w[:, :1024]) + nt(jb[1], w[:, 1024:2048]) + nt(rgf[...], w[:, 2048:])
        tgb[n] = out.astype(BF16)
        d = pltpu.make_async_copy(tgb.at[n], tg_hbm.at[:, n * 256:(n + 1) * 256], lsem.at[4 + n])
        d.start()
        tgd.append(d)

    for n in range(3):
        token_block(n)
    arrived(("tok",), tokt.at[1])
    arrived(("nrt",), nrt.at[1])
    arrived(("kvg",), kvgp)
    arrived(("j",), jp)
    arrived(("rg",), rgp)

    pb = (p0, p1, p2)
    own = (own0, own1, own2)

    def chunk(g, t):
        lo = g * 384
        width = 384 if g < 2 else 256
        total = None
        for n in range(2):
            src = (tokt.at[n, t], tokt.at[n, :, t], tokt.at[n, :, :, t])[g]
            left = src[...].reshape(512, 512)
            right = jb[ic, :, lo:lo + width] if n == 0 else jp[:, lo:lo + width]
            if g == 2:
                right = jnp.concatenate([right, rg[ic] if n == 0 else rgp[...]], 1)
            term = nn(left, right)
            total = term if n == 0 else total + term
        total = total.reshape(4, 4, 32, 384)
        if g == 2:
            total = jnp.concatenate([total[..., :256], total[..., 256:] + gmat[:, :, t]], -1)
            return total
        up = None
        for n in range(2):
            src = (nrt.at[n, pl.ds(pl.multiple_of(t * 128, 128), 128)] if g == 0 else None)
            if g == 0:
                left = src[...]
            else:
                left = jnp.concatenate(
                    [nrt[n, pl.ds(pl.multiple_of(z * 128 + t * 32, 32), 32)] for z in range(4)], 0)
            term = nn(left, kvg[ic, g] if n == 0 else kvgp[g])
            up = term if n == 0 else up + term
        up = up.reshape(16, 8, 512)
        up = jnp.concatenate([up[:, :, j * 128:(j + 1) * 128] for j in range(4)], 1)
        return jnp.concatenate([total, up.reshape(4, 4, 32, 128)], -1)

    rx = (rx0, rx1, rx2)
    ra = (ra0, ra1, ra2)
    for by in (2, 1, -1, 0):
        for g, (width, a1, a2, a3) in enumerate(GROUPS):
            t = step(a1, by)
            value = chunk(g, t)
            right, left = {a1: step(a1, 1)}, {a1: step(a1, -1)}
            if by == 0:
                own[g][...] = value
                continue
            slot = {2: 0, 1: 1, -1: 2}[by]
            pb[g][slot] = value.astype(BF16)
            if by == 2:
                send((1, g, "x", 0), pb[g].at[0, 0:2], rx[g].at[0], right)
                send((1, g, "x", 1), pb[g].at[0, 2:4], rx[g].at[1], left)
            elif by == 1:
                send((1, g, "a", 0, 1), pb[g].at[1, 2:4], ra[g].at[0, 2:4], right)
            else:
                send((1, g, "a", 1, 0), pb[g].at[2, 0:2], ra[g].at[1, 0:2], left)
    for g, (width, a1, a2, a3) in enumerate(GROUPS):
        right, left = {a1: step(a1, 1)}, {a1: step(a1, -1)}
        arrived((1, g, "x", 0), rx[g].at[0])
        pb[g][1, 0:2] = (pb[g][1, 0:2].astype(F32) + rx[g][0].astype(F32)).astype(BF16)
        arrived((1, g, "x", 1), rx[g].at[1])
        pb[g][2, 2:4] = (pb[g][2, 2:4].astype(F32) + rx[g][1].astype(F32)).astype(BF16)
        send((1, g, "a", 0, 0), pb[g].at[1, 0:2], ra[g].at[0, 0:2], right)
        send((1, g, "a", 1, 1), pb[g].at[2, 2:4], ra[g].at[1, 2:4], left)
    for n in range(3, 8):
        token_block(n)

    q = (q0, q1, q2)
    rx2_ = (rx20, rx21, rx22)
    ra2_ = (ra20, ra21, ra22)
    for g, (width, a1, a2, a3) in enumerate(GROUPS):
        for d in range(2):
            for h in range(2):
                arrived((1, g, "a", d, h), ra[g].at[d, h * 2:h * 2 + 2])
        own[g][...] += ra[g][0].astype(F32) + ra[g][1].astype(F32)
        right, left = {a2: step(a2, 1)}, {a2: step(a2, -1)}
        for slot, by in enumerate((2, 1, -1)):
            t = step(a2, by)
            q[g][slot] = (own[g][:, t] if g == 1 else own[g][t]).astype(BF16)
        send((2, g, "x", 0), q[g].at[0, 0:2], rx2_[g].at[0], right)
        send((2, g, "x", 1), q[g].at[0, 2:4], rx2_[g].at[1], left)
        send((2, g, "a", 0, 1), q[g].at[1, 2:4], ra2_[g].at[0, 2:4], right)
        send((2, g, "a", 1, 0), q[g].at[2, 0:2], ra2_[g].at[1, 0:2], left)
    for g, (width, a1, a2, a3) in enumerate(GROUPS):
        right, left = {a2: step(a2, 1)}, {a2: step(a2, -1)}
        arrived((2, g, "x", 0), rx2_[g].at[0])
        q[g][1, 0:2] = (q[g][1, 0:2].astype(F32) + rx2_[g][0].astype(F32)).astype(BF16)
        arrived((2, g, "x", 1), rx2_[g].at[1])
        q[g][2, 2:4] = (q[g][2, 2:4].astype(F32) + rx2_[g][1].astype(F32)).astype(BF16)
        send((2, g, "a", 0, 0), q[g].at[1, 0:2], ra2_[g].at[0, 0:2], right)
        send((2, g, "a", 1, 1), q[g].at[2, 2:4], ra2_[g].at[1, 2:4], left)

    s = (s0, s1, s2)
    rx3 = (rx30, rx31, rx32)
    ra3 = (ra30, ra31, ra32)
    kept = []
    for g, (width, a1, a2, a3) in enumerate(GROUPS):
        for d in range(2):
            for h in range(2):
                arrived((2, g, "a", d, h), ra2_[g].at[d, h * 2:h * 2 + 2])
        mine = own[g].at[:, at[a2]] if g == 1 else own[g].at[at[a2]]
        mine[...] += ra2_[g][0].astype(F32) + ra2_[g][1].astype(F32)
        kept.append(mine)
        right, left = {a3: step(a3, 1)}, {a3: step(a3, -1)}
        for slot, by in enumerate((2, 1, -1)):
            s[g][slot] = mine[step(a3, by)].reshape(2, 16, width).astype(BF16)
        send((3, g, "x", 0), s[g].at[0, 0], rx3[g].at[0], right)
        send((3, g, "x", 1), s[g].at[0, 1], rx3[g].at[1], left)
        send((3, g, "a", 0, 1), s[g].at[1, 1], ra3[g].at[0, 1], right)
        send((3, g, "a", 1, 0), s[g].at[2, 0], ra3[g].at[1, 0], left)
    for g, (width, a1, a2, a3) in enumerate(GROUPS):
        right, left = {a3: step(a3, 1)}, {a3: step(a3, -1)}
        arrived((3, g, "x", 0), rx3[g].at[0])
        s[g][1, 0] = (s[g][1, 0].astype(F32) + rx3[g][0].astype(F32)).astype(BF16)
        arrived((3, g, "x", 1), rx3[g].at[1])
        s[g][2, 1] = (s[g][2, 1].astype(F32) + rx3[g][1].astype(F32)).astype(BF16)
        send((3, g, "a", 0, 0), s[g].at[1, 0], ra3[g].at[0, 0], right)
        send((3, g, "a", 1, 1), s[g].at[2, 1], ra3[g].at[1, 1], left)
    for g, (width, a1, a2, a3) in enumerate(GROUPS):
        for d in range(2):
            for h in range(2):
                arrived((3, g, "a", d, h), ra3[g].at[d, h])
        both = (ra3[g][0].astype(F32) + ra3[g][1].astype(F32)).reshape(32, width)
        fin_ref[ic, :, GOFF[g]:GOFF[g] + width] = kept[g][at[a3]] + both
    send(("fin",), fin_ref.at[ic], fin_ref.at[ic], mate)
    arrived(("fin",), fin_ref.at[other])

    both = fin_ref[...]
    tail = GTOT - 128
    gains = both[0, :, tail:] + both[1, :, tail:]
    body = both[:, :, :tail]
    squares = jnp.sum(jnp.sum(body * body, axis=0), axis=0, keepdims=True)
    row = sum(squares[:, n * 128:(n + 1) * 128] for n in range(10))
    ropes = jnp.where(lane == 32, 0.0, both[0, :, tail:] ** 2 + both[1, :, tail:] ** 2)
    ropes = ropes + jnp.where(lane == 32, gains * gains, 0.0)
    row = row + jnp.sum(ropes, axis=0, keepdims=True)
    row = jnp.broadcast_to(row, (8, 128))
    for n, axis in enumerate((AY, AX, AZ)):
        nbuf[n, 3] = row
        for m, by in enumerate((1, -1, 2)):
            send(("n", n, m), nbuf.at[n, 3], nbuf.at[n, m], {axis: step(axis, by)})
        for m in range(3):
            arrived(("n", n, m), nbuf.at[n, m])
        row = (nbuf[n, 0] + nbuf[n, 1]) + (nbuf[n, 2] + nbuf[n, 3])
    total = jnp.sum(row, axis=-1, keepdims=True)
    clip = jnp.minimum(1.0, lax.rsqrt(total / NPARAM + 1e-06))
    clip_ref[...] = jnp.broadcast_to(clip, (8, 128))

    for d in sends:
        d.wait_send()
    for d in tgd:
        d.wait()
    assert len(table) <= NSEM, len(table)


NSEM = 192


def scratch():
    v = pltpu.VMEM
    shapes = [
        v((512, 2048), BF16), v((512, 1024), BF16), v((512, 128), F32), v((512, 128), F32),
        v((4, 2, 8, 32, WCOL), BF16), v((4, 2, 8, 64, 256), BF16), v((4, 2, 8, 128), F32),
        v((2, 4, 4, 4, 32, 512), BF16), v((512, WCOL), F32),
        v((512, 512), BF16), v((512, 1024), BF16), v((512, 512), BF16), v((2, 512, 512), BF16),
        v((512, 512), F32), v((2, 512, 128), BF16), v((512, 128), F32),
        v((2, 512, 1024), BF16), v((512, 1024), BF16), v((2, 2, 512, 512), BF16), v((2, 512, 512), BF16),
        v((2, 512, 128), BF16), v((512, 128), BF16), v((512, 128), BF16), v((512, 128), F32),
        v((4, 4, 4, 32, 128), F32), v((8, 512, 256), BF16),
    ]
    ws = [w for w, *_ in GROUPS]
    shapes += [v((3, 4, 4, 32, w), BF16) for w in ws]
    shapes += [v((4, 4, 32, w), F32) for w in ws]
    shapes += [v((2, 2, 4, 32, w), BF16) for w in ws]
    shapes += [v((2, 4, 4, 32, w), BF16) for w in ws]
    shapes += [v((3, 4, 32, w), BF16) for w in ws]
    shapes += [v((2, 2, 32, w), BF16) for w in ws]
    shapes += [v((2, 4, 32, w), BF16) for w in ws]
    shapes += [v((3, 2, 16, w), BF16) for w in ws]
    shapes += [v((2, 16, w), BF16) for w in ws]
    shapes += [v((2, 2, 16, w), BF16) for w in ws]
    shapes += [v((3, 4, 8, 128), F32)]
    dma = pltpu.SemaphoreType.DMA
    return shapes + [dma((12,)), dma((NSEM,)), dma((NSEM,))]


def per_device(tokens, d_out, w_query, w_down, w_up, latent_gain):
    cosine, sine = rope_constants()
    vm = pl.BlockSpec(memory_space=pltpu.VMEM)
    anyspace = pl.BlockSpec(memory_space=pl.ANY)
    fin, clip, token_grad = pl.pallas_call(
        mega,
        out_shape=(
            jax.ShapeDtypeStruct((2, 32, GTOT), F32),
            jax.ShapeDtypeStruct((8, 128), F32),
            jax.ShapeDtypeStruct((SEQ, D), BF16),
        ),
        in_specs=[anyspace] * 4 + [vm] * 4,
        out_specs=(vm, vm, anyspace),
        scratch_shapes=scratch(),
        compiler_params=pltpu.CompilerParams(
            collective_id=0, has_side_effects=True, vmem_limit_bytes=67043328),
    )(tokens, d_out, jnp.asarray(cosine), jnp.asarray(sine), w_query, w_down, w_up,
      latent_gain.reshape(1, 64))
    ic = lax.axis_index(AC)
    clip = clip[0, 0]
    rows = lax.dynamic_slice_in_dim(fin, ic * 16, 16, 1)
    plain = jnp.concatenate([rows[0, :, :384], rows[0, :, 512:896], rows[0, :, 1024:1280]], 1)
    rest = jnp.concatenate([rows[1, :, :384], rows[1, :, 512:896], rows[1, :, 1024:1280]], 1)
    grad_query = jnp.concatenate(
        [plain.reshape(16, 8, 128), rest[:, :512].reshape(16, 8, 64)], -1).reshape(16, 1536)
    grad_down = jnp.concatenate([rest[:, 512:], rows[0, :, 1280:1312], rows[1, :, 1280:1312]], 1)
    up = jnp.stack([fin[:, :, 384:512], fin[:, :, 896:1024]], 2).reshape(2, 4, 8, 2, 128)
    up = lax.dynamic_slice_in_dim(up, ic * 4, 4, 2)
    grad_up = up.transpose(2, 0, 1, 3, 4).reshape(4, 2048)
    gain = lax.dynamic_slice_in_dim(fin[:, :, 1312], ic * 4, 4, 1)
    return (
        grad_query * clip,
        grad_down * clip,
        grad_up * clip,
        (gain[0] + gain[1]) * clip,
        token_grad,
    )


def solution(mesh):
    split = Mesh(mesh.devices.reshape(4, 4, 4, 2), NODE_LOCAL)
    return jax.shard_map(
        per_device,
        mesh=split,
        in_specs=(
            P(NODE_LOCAL, None),
            P(NODE_LOCAL, None),
            P(LOCAL, None),
            P(LOCAL, None),
            P(LOCAL, None),
            P(LOCAL),
        ),
        out_specs=(
            P(NODE_LOCAL, None),
            P(NODE_LOCAL, None),
            P(NODE_LOCAL, None),
            P(NODE_LOCAL),
            P(NODE_LOCAL, None),
        ),
        check_vma=False,
    )
```

```python
import math

import jax
import jax.numpy as jnp
import numpy as np
from jax import lax
from jax.experimental import pallas as pl
from jax.experimental.pallas import tpu as pltpu
from jax.sharding import Mesh
from jax.sharding import PartitionSpec as P

H = 8
DN = 128
DR = 64
DV = 128
KVL = 512
SEQ = 512
D = 2048
NPARAM = 5374464
EPSILON = 1e-06
ROPE_BASE = 10000.0
LOCAL = ("local_0", "local_1")
NODE_LOCAL = ("node_0", "node_1", "local_0", "local_1")
MESH = pl.DeviceIdType.MESH
AZ, AX, AY, AC = NODE_LOCAL

WCOL = 2176
SUBS = ((0, 640), (640, 1408), (1408, 2176))
SCALE = 1.0 / math.sqrt(DN + DR)
AXES = ((AZ, AX, AY), (AX, AY, AZ), (AY, AZ, AX))
UNITS = tuple((w,) + AXES[n % 3] for n, w in enumerate((256, 256, 256, 256, 256, 128)))
GOFF = (0, 256, 512, 768, 1024, 1280)
GTOT = 1408
F32 = jnp.float32
BF16 = jnp.bfloat16


def rope_constants():
    position = np.arange(SEQ, dtype=np.float32)[:, None]
    freq = np.float32(ROPE_BASE) ** (-np.arange(DR // 2, dtype=np.float32) * np.float32(2.0 / DR))
    angle = (position * freq[None, :].astype(np.float32)).astype(np.float32)
    cosine = np.cos(angle).astype(np.float32)
    sine = np.sin(angle).astype(np.float32)
    return np.concatenate([cosine] * 4, 1), np.concatenate([-sine, sine] * 2, 1)


def nt(a, b):
    return lax.dot_general(a, b, (((1,), (1,)), ((), ())), preferred_element_type=F32)


def nn(a, b):
    return jnp.dot(a, b, preferred_element_type=F32)


def tn(a, b):
    return lax.dot_general(a, b, (((0,), (0,)), ((), ())), preferred_element_type=F32)


def mega(
    tokens_hbm, dout_hbm, cos_hbm, sin_hbm, wq_ref, wd_ref, wu_ref, gain_ref,
    fin_ref, clip_ref, tg_hbm,
    tokens, dout, cosr, sinr, wbuf, ubuf, gbuf, tokt, acc, qrope, qnope, nrm, nrt, ng, krp, dkr,
    jb, jp, kvg, kvgp, rg, rgp, rgf, invr, gmat, tgb, nbuf, lsem, ssem, rsem, *rest,
):
    nu = len(UNITS)
    part, own, rx, ra, part2, rx2, ra2, part3, ra3 = (rest[n * nu:(n + 1) * nu] for n in range(9))
    iz, ix, iy, ic = (lax.axis_index(a) for a in NODE_LOCAL)
    at = {AZ: iz, AX: ix, AY: iy}
    other = 1 - ic
    STEP = {(a, by): lax.rem(at[a] + (by + 4), 4) for a in at for by in (-1, 0, 1, 2)}

    def step(axis, by):
        return STEP[axis, by]

    sends = []
    table = {}
    scope = []

    def mark(name):
        while scope:
            scope.pop().__exit__(None, None, None)
        if name:
            scope.append(jax.named_scope(name))
            scope[-1].__enter__()

    mark("start")

    def sem_of(key):
        return table.setdefault(key, len(table))

    def send(key, src, dst, peer):
        k = sem_of(key)
        d = pltpu.make_async_remote_copy(
            src_ref=src, dst_ref=dst, send_sem=ssem.at[k], recv_sem=rsem.at[k],
            device_id=peer, device_id_type=MESH)
        d.start()
        sends.append((k, src, dst, peer))

    def arrived(key, dst):
        k = sem_of(key)
        pltpu.make_async_remote_copy(
            src_ref=dst, dst_ref=dst, send_sem=ssem.at[k], recv_sem=rsem.at[k],
            device_id=mate, device_id_type=MESH).wait_recv()

    mate = {AC: other}
    locals_ = []
    for n, (src, dst) in enumerate(((tokens_hbm, tokens), (dout_hbm, dout), (cos_hbm, cosr), (sin_hbm, sinr))):
        d = pltpu.make_async_copy(src, dst, lsem.at[n])
        d.start()
        locals_.append(d)

    barrier = pltpu.get_barrier_semaphore()
    for axis in (AZ, AX, AY):
        for by in (1, -1, 2):
            pl.semaphore_signal(barrier, inc=1, device_id={axis: step(axis, by)}, device_id_type=MESH)
    pl.semaphore_signal(barrier, inc=1, device_id=mate, device_id_type=MESH)

    down = jnp.concatenate([wd_ref[...], jnp.zeros((64, 256), BF16)], 0)
    wbuf[iy, ic, :, :, 0:640] = down.T.reshape(8, 32, 640)
    for n in range(4):
        lo = 640 + n * 384
        h = n * 384
        both = jnp.concatenate([
            wq_ref[:, h:h + 128], wq_ref[:, h + 192:h + 320],
            wq_ref[:, h + 128:h + 192], wq_ref[:, h + 320:h + 384]], 1)
        wbuf[iy, ic, :, :, lo:lo + 384] = both.reshape(8, 32, 384)
    for p in range(8):
        ubuf[iy, ic, p] = wu_ref[:, p * 256:(p + 1) * 256]
    gbuf[iy, ic] = jnp.broadcast_to(
        jnp.concatenate([gain_ref[...].astype(F32), jnp.zeros((1, 64), F32)], 1), (8, 128))
    pl.semaphore_wait(barrier, 10)

    RING = (AX, AZ)
    YO = (step(AY, -1), step(AY, 1), step(AY, 2))
    PIECE = {(k, by): k * 4 + step(RING[k], by) for k in range(2) for by in (-1, 0, 1, 2)}
    KINDS = (0, "u", 1, 2)

    def block_of(kind, yy, core):
        if kind == "u":
            return ubuf.at[yy, core]
        lo, hi = SUBS[kind]
        return wbuf.at[yy, core, :, :, lo:hi]

    def piece(kind, yy, k, by):
        if kind == "u":
            return ubuf.at[yy, ic, PIECE[k, by]]
        lo, hi = SUBS[kind]
        return wbuf.at[yy, ic, PIECE[k, by], :, lo:hi]

    def half_piece(kind, yy, k, by, d):
        if kind == "u":
            return ubuf.at[yy, ic, PIECE[k, by], d * 32:d * 32 + 32]
        lo, hi = SUBS[kind]
        return wbuf.at[yy, ic, PIECE[k, by], d * 16:d * 16 + 16, lo:hi]

    def y_send(kind):
        for k in range(2):
            r = piece(kind, iy, k, 0)
            send((kind, "y", k, 0), r, r, {AY: step(AY, 1)})
            send((kind, "y", k, 1), r, r, {AY: step(AY, -1)})

    def p_send(kind, k, yo):
        r = piece(kind, YO[yo], k, 0)
        send((kind, "p", k, yo, 0), r, r, {RING[k]: step(RING[k], 1)})
        send((kind, "p", k, yo, 1), r, r, {RING[k]: step(RING[k], -1)})

    def y_take(kind):
        for k in range(2):
            for d in range(2):
                arrived((kind, "y", k, d), piece(kind, YO[d], k, 0))
                half = half_piece(kind, YO[d], k, 0, d)
                send((kind, "y2", k, d), half, half, {AY: step(AY, 1 if d == 0 else -1)})
                p_send(kind, k, d)

    def y2_take(kind):
        for k in range(2):
            for d in range(2):
                arrived((kind, "y2", k, d), half_piece(kind, YO[2], k, 0, d))
            p_send(kind, k, 2)

    def p_take(kind, yo):
        for k in range(2):
            for d in range(2):
                by = -1 if d == 0 else 1
                arrived((kind, "p", k, yo, d), piece(kind, YO[yo], k, by))
                half = half_piece(kind, YO[yo], k, by, d)
                send((kind, "p2", k, yo, d), half, half, {RING[k]: step(RING[k], -by)})

    def p2_take(kind, yo):
        for k in range(2):
            for d in range(2):
                arrived((kind, "p2", k, yo, d), half_piece(kind, YO[yo], k, 2, d))
        to_mate(kind, yo)

    def to_mate(kind, yo):
        r = block_of(kind, iy if yo is None else YO[yo], ic)
        send((kind, "d", yo), r, r, mate)

    def from_mate(kind):
        for yo in (None, 0, 1, 2):
            arrived((kind, "d", yo), block_of(kind, iy if yo is None else YO[yo], other))

    def project(lo, hi):
        return nn(tokens[...], wbuf[:, :, :, :, lo:hi].reshape(2048, hi - lo))

    mark("gather")
    y_send(0)
    y_send("u")
    to_mate(0, None)
    g = gbuf.at[iy, ic]
    for n, by in enumerate((1, -1, 2)):
        send(("g", n), g, g, {AY: step(AY, by)})
    send(("gd", 3), g, g, mate)
    to_mate("u", None)
    mark("y0")
    y_take(0)
    y_send(1)
    to_mate(1, None)
    mark("yu")
    y_take("u")
    locals_[0].wait()
    mark("transpose")
    for z in range(2):
        tokt[0, z] = tokens[:, z * 512:(z + 1) * 512].T.reshape(4, 4, 32, 512)
    mark("y20")
    y2_take(0)
    y_send(2)
    to_mate(2, None)
    mark("p0a")
    p_take(0, 0)
    p_take(0, 1)
    mark("y1")
    y_take(1)
    mark("transpose")
    for z in range(2, 4):
        tokt[0, z] = tokens[:, z * 512:(z + 1) * 512].T.reshape(4, 4, 32, 512)
    send(("tok",), tokt.at[0], tokt.at[1], mate)
    mark("y2u")
    y2_take("u")
    mark("pua")
    p_take("u", 0)
    p_take("u", 1)
    mark("p0b")
    p_take(0, 2)
    mark("y21")
    y2_take(1)
    mark("p20")
    p2_take(0, 0)
    p2_take(0, 1)
    mark("y2")
    y_take(2)
    mark("p1a")
    p_take(1, 0)
    p_take(1, 1)
    mark("pub")
    p_take("u", 2)
    mark("p202")
    p2_take(0, 2)
    mark("y22")
    y2_take(2)
    mark("g")
    for n, by in enumerate((-1, 1, 2)):
        gg = gbuf.at[step(AY, by), ic]
        arrived(("g", n), gg)
        send(("gd", n), gg, gg, mate)
    mark("p2u")
    for yo in range(3):
        p2_take("u", yo)
    mark("p1b")
    p_take(1, 2)
    mark("p21")
    p2_take(1, 0)
    p2_take(1, 1)
    mark("p2a")
    p_take(2, 0)
    p_take(2, 1)
    mark("down")
    from_mate(0)
    acc[...] = project(*SUBS[0])
    mark("p212")
    p2_take(1, 2)
    mark("pre")
    for n, by in enumerate((-1, 1, 2)):
        arrived(("gd", n), gbuf.at[step(AY, by), other])
    arrived(("gd", 3), gbuf.at[iy, other])

    for d in locals_[1:]:
        d.wait()

    lane = lax.broadcasted_iota(jnp.int32, (1, 128), 1)
    low = lax.rem(lane, 64) < 32

    def swap(v):
        return jnp.where(low, pltpu.roll(v, 96, 1), pltpu.roll(v, 32, 1))

    def rot(v, sign):
        return v * cosr[...] + swap(v) * (sinr[...] * sign)

    gain = jnp.concatenate([gbuf[y, c, 0:1, 0:64] for y in range(4) for c in range(2)], 1)
    kr = rot(acc[:, 512:640], 1.0)
    krp[0] = jnp.where(lane < 64, kr, 0.0).astype(BF16)
    krp[1] = jnp.where(lane < 64, 0.0, pltpu.roll(kr, 64, 1)).astype(BF16)
    for n in range(4):
        rows = slice(n * 128, (n + 1) * 128)
        latent = acc[rows, 0:512]
        inv = lax.rsqrt(jnp.mean(latent * latent, axis=-1, keepdims=True) + EPSILON)
        unit = latent * inv
        acc[rows, 0:512] = unit
        invr[rows] = jnp.broadcast_to(inv, (128, 128))
        nrm[rows] = (unit * gain).astype(BF16)
    nrt[0] = nrm[...].T
    send(("nrt",), nrt.at[0], nrt.at[1], mate)
    ng[...] = jnp.zeros((512, 512), F32)
    dkr[...] = jnp.zeros((512, 128), F32)
    mark("p2b")
    p_take(2, 2)
    from_mate("u")
    mark("heads")

    tri = (lax.broadcasted_iota(jnp.int32, (256, 256), 0)
           <= lax.broadcasted_iota(jnp.int32, (256, 256), 1))

    def block(kf, v, qf, do):
        rows = kf.shape[0]
        s = nt(kf, qf) * SCALE
        masked = jnp.where(tri, s[rows - 256:], -1e30)
        s = masked if rows == 256 else jnp.concatenate([s[:rows - 256], masked], 0)
        w = jnp.exp(s - jnp.max(s, axis=0, keepdims=True))
        probs = w * (1.0 / jnp.sum(w, axis=0, keepdims=True))
        dp = nt(v, do)
        delta = jnp.sum(probs * dp, axis=0, keepdims=True)
        ds = (probs * (dp - delta) * SCALE).astype(BF16)
        return probs.astype(BF16), ds

    def queries(s):
        from_mate(s + 1)
        lo = SUBS[s + 1][0]
        q = project(lo, lo + 768)
        for m in range(2):
            n = 2 * s + m
            qnope[:, n * 256:(n + 1) * 256] = q[:, m * 384:m * 384 + 256].astype(BF16)
            rope = q[:, m * 384 + 256:m * 384 + 384].astype(BF16).astype(F32)
            qrope[:, n * 128:(n + 1) * 128] = rot(rope, 1.0).astype(BF16)

    def pair(n, carry):
        @pl.when(n == 0)
        def _():
            queries(0)

        @pl.when(n == 1)
        def _():
            p2_take(2, 0)
            p2_take(2, 1)
            p2_take(2, 2)

        @pl.when(n == 2)
        def _():
            queries(1)

        half, m = n // 2, lax.rem(n, 2)
        qr = qrope[:, pl.ds(pl.multiple_of(n * 128, 128), 128)]
        total = None
        for e in range(2):
            h = 2 * n + e
            hc = pl.ds(pl.multiple_of(h * 128, 128), 128)
            jc = pl.ds(pl.multiple_of((m * 2 + e) * 128, 128), 128)
            u = ubuf[:, :, h].reshape(512, 256)
            kv = nn(nrm[...], u).astype(BF16)
            kf = jnp.concatenate([kv[:, :128], krp[e]], 1)
            v = kv[:, 128:]
            qf = jnp.concatenate([qnope[:, hc], qr], 1)
            do = dout[:, hc]
            pa, da = block(kf[:256], v[:256], qf[:256], do[:256])
            pb, db = block(kf, v, qf[256:], do[256:])
            dv = nn(pb, do[256:])
            dv = jnp.concatenate([dv[:256] + nn(pa, do[:256]), dv[256:]], 0)
            dk = nn(db, qf[256:])
            dk = jnp.concatenate([dk[:256] + nn(da, qf[:256]), dk[256:]], 0)
            dq = jnp.concatenate([tn(da, kf[:256]), tn(db, kf)], 0)
            jb[half, :, jc] = dq[:, :128].astype(BF16)
            total = dq[:, 128:] if e == 0 else total + dq[:, 128:]
            keep = lane < 64 if e == 0 else lane >= 64
            dkr[...] += jnp.where(keep, dk[:, 128:], 0.0)
            kg = dk[:, :128].astype(BF16)
            vg = dv.astype(BF16)
            kvg[half, 0, :, jc] = kg
            kvg[half, 1, :, jc] = vg
            ng[...] += nt(jnp.concatenate([kg, vg], 1), u)
        jb[half, :, pl.ds(pl.multiple_of(512 + m * 128, 128), 128)] = rot(total, -1.0).astype(BF16)
        return carry

    lax.fori_loop(0, 4, pair, 0)
    mark("post")
    send(("j",), jb.at[other, :, 0:768], jp.at[:, 0:768], mate)

    gterm = jnp.zeros((1, 512), F32)
    for n in range(4):
        rows = slice(n * 128, (n + 1) * 128)
        unit = acc[rows, 0:512]
        grad = ng[rows]
        gterm = gterm + jnp.sum(grad * unit, axis=0, keepdims=True)
        scaled = grad * gain
        inner = jnp.mean(scaled * unit, axis=-1, keepdims=True)
        value = (invr[rows, 0:1] * (scaled - unit * inner)).astype(BF16)
        jb[0, rows, 768:1024] = value[:, :256]
        jb[1, rows, 768:1024] = value[:, 256:]
    dk = dkr[...]
    rope = jnp.where(lane < 64, rot(dk + pltpu.roll(dk, 64, 1), -1.0), 0.0)
    rgf[...] = rope.astype(BF16)
    rg[0] = jnp.where(lane < 32, rope, 0.0).astype(BF16)
    rg[1] = jnp.where(lane < 32, pltpu.roll(rope, 96, 1), 0.0).astype(BF16)
    send(("kvg",), kvg.at[other], kvgp, mate)
    send(("jl",), jb.at[other, :, 768:1024], jp.at[:, 768:1024], mate)
    send(("rg",), rg.at[other], rgp, mate)
    column = jnp.broadcast_to(gterm, (128, 512)).T
    column = jnp.where(lane == 32, column, 0.0).reshape(64, 8, 128)
    gmat[...] = jnp.concatenate([column, jnp.zeros((64, 24, 128), F32)], 1).reshape(4, 4, 4, 32, 128)

    tgd = []

    def token_block():
        n = len(tgd)
        w = wbuf[n // 2, n % 2].reshape(256, WCOL)
        cols = [jb[0, :, 768:], jb[1, :, 768:], rgf[...]]
        for m in range(4):
            cols += [jb[m // 2, :, m % 2 * 256:m % 2 * 256 + 256],
                     jb[m // 2, :, 512 + m % 2 * 128:640 + m % 2 * 128]]
        tgb[n] = nt(jnp.concatenate(cols, 1), w).astype(BF16)
        d = pltpu.make_async_copy(tgb.at[n], tg_hbm.at[:, n * 256:(n + 1) * 256], lsem.at[4 + n])
        d.start()
        tgd.append(d)

    mark("waitmate")
    arrived(("tok",), tokt.at[1])
    arrived(("nrt",), nrt.at[1])
    arrived(("j",), jp.at[:, 0:768])

    def chunk(u, t):
        g = u % 3
        lo, width = (g * 256, 256) if u < 3 else (768 + g * 128, 128)
        total = None
        for n in range(2):
            src = (tokt.at[n, t], tokt.at[n, :, t], tokt.at[n, :, :, t])[g]
            left = src[...].reshape(512, 512)
            if u == 5:
                right = rg[ic] if n == 0 else rgp[...]
            else:
                right = jb[ic, :, lo:lo + width] if n == 0 else jp[:, lo:lo + width]
            term = nn(left, right)
            total = term if n == 0 else total + term
        total = total.reshape(4, 4, 32, width)
        if u < 3:
            return total
        if u == 5:
            return total + gmat[:, :, t]
        up = None
        for n in range(2):
            if g == 0:
                left = nrt[n, pl.ds(pl.multiple_of(t * 128, 128), 128)]
            else:
                left = jnp.concatenate(
                    [nrt[n, pl.ds(pl.multiple_of(z * 128 + t * 32, 32), 32)] for z in range(4)], 0)
            term = nn(left, kvg[ic, g] if n == 0 else kvgp[g])
            up = term if n == 0 else up + term
        up = up.reshape(16, 8, 512)
        up = jnp.concatenate([up[:, :, j * 128:(j + 1) * 128] for j in range(4)], 1)
        return jnp.concatenate([total, up.reshape(4, 4, 32, 128)], -1)

    def ways(axis):
        return {axis: step(axis, 1)}, {axis: step(axis, -1)}

    def first_sends(us):
        for slot, by in enumerate((2, 1, -1)):
            for u in us:
                right, left = ways(UNITS[u][1])
                part[u][slot] = chunk(u, step(UNITS[u][1], by)).astype(BF16)
                if by == 2:
                    send((1, u, "x", 0), part[u].at[0, 0:2], rx[u].at[0], right)
                    send((1, u, "x", 1), part[u].at[0, 2:4], rx[u].at[1], left)
                elif by == 1:
                    send((1, u, "a", 0, 1), part[u].at[1, 2:4], ra[u].at[0, 2:4], right)
                else:
                    send((1, u, "a", 1, 0), part[u].at[2, 0:2], ra[u].at[1, 0:2], left)

    def relay(phase, us, p, r, a):
        for u in us:
            right, left = ways(UNITS[u][phase])
            arrived((phase, u, "x", 0), r[u].at[0])
            p[u][1, 0:2] = (p[u][1, 0:2].astype(F32) + r[u][0].astype(F32)).astype(BF16)
            arrived((phase, u, "x", 1), r[u].at[1])
            p[u][2, 2:4] = (p[u][2, 2:4].astype(F32) + r[u][1].astype(F32)).astype(BF16)
            send((phase, u, "a", 0, 0), p[u].at[1, 0:2], a[u].at[0, 0:2], right)
            send((phase, u, "a", 1, 1), p[u].at[2, 2:4], a[u].at[1, 2:4], left)

    def own_chunks(us):
        for u in us:
            own[u][...] = chunk(u, at[UNITS[u][1]])

    def settle(phase, u, a):
        for d in range(2):
            for h in range(2):
                arrived((phase, u, "a", d, h), a[u].at[d, h * 2:h * 2 + 2])

    def second(u, t):
        return own[u].at[:, t] if u % 3 == 1 else own[u].at[t]

    def second_sends(us):
        for u in us:
            settle(1, u, ra)
            own[u][...] += ra[u][0].astype(F32) + ra[u][1].astype(F32)
            right, left = ways(UNITS[u][2])
            for slot, by in enumerate((2, 1, -1)):
                part2[u][slot] = second(u, step(UNITS[u][2], by))[...].astype(BF16)
            send((2, u, "x", 0), part2[u].at[0, 0:2], rx2[u].at[0], right)
            send((2, u, "x", 1), part2[u].at[0, 2:4], rx2[u].at[1], left)
            send((2, u, "a", 0, 1), part2[u].at[1, 2:4], ra2[u].at[0, 2:4], right)
            send((2, u, "a", 1, 0), part2[u].at[2, 0:2], ra2[u].at[1, 0:2], left)

    def third_sends(us):
        for u in us:
            settle(2, u, ra2)
            mine = second(u, at[UNITS[u][2]])
            mine[...] += ra2[u][0].astype(F32) + ra2[u][1].astype(F32)
            for slot, by in enumerate((2, 1, -1)):
                part3[u][slot] = mine[step(UNITS[u][3], by)].astype(BF16)
                send((3, u, slot), part3[u].at[slot], ra3[u].at[slot], {UNITS[u][3]: step(UNITS[u][3], by)})

    def last_sums(us):
        for u in us:
            for slot in range(3):
                arrived((3, u, slot), ra3[u].at[slot])
            mine = second(u, at[UNITS[u][2]])[at[UNITS[u][3]]]
            fin_ref[ic, :, GOFF[u]:GOFF[u] + UNITS[u][0]] = mine + (
                ra3[u][0].astype(F32) + ra3[u][1].astype(F32) + ra3[u][2].astype(F32))

    A, B = (0, 1, 2), (3, 4, 5)
    mark("firstA")
    first_sends(A)
    mark("relayA")
    relay(1, A, part, rx, ra)
    mark("mateB")
    arrived(("kvg",), kvgp)
    arrived(("jl",), jp.at[:, 768:1024])
    arrived(("rg",), rgp)
    mark("firstB")
    first_sends(B)
    mark("relayB")
    relay(1, B, part, rx, ra)
    mark("ownA")
    own_chunks(A)
    mark("secondA")
    second_sends(A)
    mark("ownB")
    own_chunks(B)
    mark("tg")
    for n in range(3):
        token_block()
    mark("relay2A")
    relay(2, A, part2, rx2, ra2)
    mark("tg")
    for n in range(2):
        token_block()
    mark("secondB")
    second_sends(B)
    mark("thirdA")
    third_sends(A)
    mark("tg")
    for n in range(1):
        token_block()
    mark("relay2B")
    relay(2, B, part2, rx2, ra2)
    mark("tg")
    for n in range(2):
        token_block()
    mark("lastA")
    last_sums(A)
    send(("fin", 0), fin_ref.at[ic, :, 0:768], fin_ref.at[ic, :, 0:768], mate)
    mark("thirdB")
    third_sends(B)
    mark("lastB")
    last_sums(B)
    send(("fin", 1), fin_ref.at[ic, :, 768:GTOT], fin_ref.at[ic, :, 768:GTOT], mate)
    mark("fin")
    arrived(("fin", 0), fin_ref.at[other, :, 0:768])
    arrived(("fin", 1), fin_ref.at[other, :, 768:GTOT])

    both = fin_ref[...]
    tail = GTOT - 128
    gains = both[0, :, tail:] + both[1, :, tail:]
    body = both[:, :, :tail]
    squares = jnp.sum(jnp.sum(body * body, axis=0), axis=0, keepdims=True)
    row = sum(squares[:, n * 128:(n + 1) * 128] for n in range(10))
    ropes = jnp.where(lane == 32, 0.0, both[0, :, tail:] ** 2 + both[1, :, tail:] ** 2)
    ropes = ropes + jnp.where(lane == 32, gains * gains, 0.0)
    row = row + jnp.sum(ropes, axis=0, keepdims=True)
    row = jnp.broadcast_to(row, (8, 128))
    mark("norm")
    for n, axis in enumerate((AY, AX, AZ)):
        nbuf[n, 3] = row
        for m, by in enumerate((1, -1, 2)):
            send(("n", n, m), nbuf.at[n, 3], nbuf.at[n, m], {axis: step(axis, by)})
        for m in range(3):
            arrived(("n", n, m), nbuf.at[n, m])
        row = (nbuf[n, 0] + nbuf[n, 1]) + (nbuf[n, 2] + nbuf[n, 3])
    total = jnp.sum(row, axis=-1, keepdims=True)
    clip = jnp.minimum(1.0, lax.rsqrt(total / NPARAM + 1e-06))
    clip_ref[...] = jnp.broadcast_to(clip, (8, 128))

    mark("drain")
    for k, src, dst, peer in sends:
        pltpu.make_async_remote_copy(
            src_ref=src, dst_ref=dst, send_sem=ssem.at[k], recv_sem=rsem.at[k],
            device_id=peer, device_id_type=MESH).wait_send()
    for d in tgd:
        d.wait()
    mark(None)
    assert len(table) <= NSEM, len(table)


NSEM = 280


def scratch():
    v = pltpu.VMEM
    dma = pltpu.SemaphoreType.DMA
    shapes = [
        v((512, 2048), BF16), v((512, 1024), BF16), v((512, 128), F32), v((512, 128), F32),
        v((4, 2, 8, 32, WCOL), BF16), v((4, 2, 8, 64, 256), BF16), v((4, 2, 8, 128), F32),
        v((2, 4, 4, 4, 32, 512), BF16), v((512, 640), F32),
        v((512, 512), BF16), v((512, 1024), BF16), v((512, 512), BF16), v((2, 512, 512), BF16),
        v((512, 512), F32), v((2, 512, 128), BF16), v((512, 128), F32),
        v((2, 512, 1024), BF16), v((512, 1024), BF16), v((2, 2, 512, 512), BF16), v((2, 512, 512), BF16),
        v((2, 512, 128), BF16), v((512, 128), BF16), v((512, 128), BF16), v((512, 128), F32),
        v((4, 4, 4, 32, 128), F32), v((8, 512, 256), BF16), v((3, 4, 8, 128), F32),
        dma((12,)), dma((NSEM,)), dma((NSEM,)),
    ]
    ws = [w for w, *_ in UNITS]
    shapes += [v((3, 4, 4, 32, w), BF16) for w in ws]
    shapes += [v((4, 4, 32, w), F32) for w in ws]
    shapes += [v((2, 2, 4, 32, w), BF16) for w in ws]
    shapes += [v((2, 4, 4, 32, w), BF16) for w in ws]
    shapes += [v((3, 4, 32, w), BF16) for w in ws]
    shapes += [v((2, 2, 32, w), BF16) for w in ws]
    shapes += [v((2, 4, 32, w), BF16) for w in ws]
    shapes += [v((3, 32, w), BF16) for w in ws]
    shapes += [v((3, 32, w), BF16) for w in ws]
    return shapes


def last_step(fin_ref, clip_ref, tg_in, gq_ref, gd_ref, gu_ref, gg_ref, tg_out, stage, isem, osem):
    ic = lax.axis_index(AC)
    reads = []
    for n in range(4):
        rows = slice(n * 128, (n + 1) * 128)
        d = pltpu.make_async_copy(tg_in.at[rows], stage.at[n], isem.at[n])
        d.start()
        reads.append(d)
    clip = clip_ref[0:1, 0:1]
    first = ic == 0

    def rows(half, cols):
        return jnp.where(first, fin_ref[half, 0:16, cols], fin_ref[half, 16:32, cols]) * clip

    def cols(lo):
        return slice(lo, lo + 128)

    for n in range(4):
        half, m = n // 2, n % 2
        rope = rows(half, cols(512 + m * 128))
        gq_ref[:, n * 384:(n + 1) * 384] = jnp.concatenate(
            [rows(half, cols(m * 256)), rope[:, :64], rows(half, cols(m * 256 + 128)), rope[:, 64:]], 1)
        gd_ref[:, n * 128:(n + 1) * 128] = rows(half, cols(768 + m * 256))
    tail = slice(GTOT - 128, GTOT)
    gd_ref[:, 512:576] = jnp.concatenate([rows(0, tail)[:, :32], rows(1, tail)[:, :32]], 1)
    for h in range(H):
        half, j = h // 4, h % 4
        for u in range(2):
            block = fin_ref[half, j * 8:j * 8 + 8, cols(896 + u * 256)] * clip
            gu_ref[:, h * 256 + u * 128:h * 256 + u * 128 + 128] = jnp.where(first, block[0:4], block[4:8])
    gain = (fin_ref[0, 0:8, tail] + fin_ref[1, 0:8, tail]) * clip
    gain = jnp.where(first, gain[0:4], gain[4:8])
    spread = (lax.broadcasted_iota(jnp.int32, (4, 128), 0)
              == lax.broadcasted_iota(jnp.int32, (4, 128), 1))
    gg_ref[...] = jnp.sum(jnp.where(spread, gain[:, 32:33], 0.0), axis=0)[0:4]
    writes = []
    for n in range(4):
        rows_n = slice(n * 128, (n + 1) * 128)
        reads[n].wait()
        d = pltpu.make_async_copy(stage.at[n], tg_out.at[rows_n], osem.at[n])
        d.start()
        writes.append(d)
    for d in writes:
        d.wait()


def finish(fin, clip, token_grad):
    vm = pl.BlockSpec(memory_space=pltpu.VMEM)
    anyspace = pl.BlockSpec(memory_space=pl.ANY)
    return pl.pallas_call(
        last_step,
        out_shape=(
            jax.ShapeDtypeStruct((16, 1536), F32),
            jax.ShapeDtypeStruct((16, 576), F32),
            jax.ShapeDtypeStruct((4, 2048), F32),
            jax.ShapeDtypeStruct((4,), F32),
            jax.ShapeDtypeStruct((SEQ, D), BF16),
        ),
        in_specs=[vm, vm, anyspace],
        out_specs=(vm, vm, vm, vm, anyspace),
        scratch_shapes=[
            pltpu.VMEM((4, 128, D), BF16), pltpu.SemaphoreType.DMA((4,)), pltpu.SemaphoreType.DMA((4,))],
    )(fin, clip, token_grad)


def per_device(tokens, d_out, w_query, w_down, w_up, latent_gain):
    cosine, sine = rope_constants()
    vm = pl.BlockSpec(memory_space=pltpu.VMEM)
    anyspace = pl.BlockSpec(memory_space=pl.ANY)
    fin, clip, token_grad = pl.pallas_call(
        mega,
        out_shape=(
            jax.ShapeDtypeStruct((2, 32, GTOT), F32),
            jax.ShapeDtypeStruct((8, 128), F32),
            jax.ShapeDtypeStruct((SEQ, D), BF16),
        ),
        in_specs=[anyspace] * 4 + [vm] * 4,
        out_specs=(vm, vm, anyspace),
        scratch_shapes=scratch(),
        compiler_params=pltpu.CompilerParams(
            collective_id=0, has_side_effects=True, vmem_limit_bytes=67043328),
    )(tokens, d_out, jnp.asarray(cosine), jnp.asarray(sine), w_query, w_down.T, w_up,
      latent_gain.reshape(1, 64))
    return finish(fin, clip, token_grad)


def solution(mesh):
    split = Mesh(mesh.devices.reshape(4, 4, 4, 2), NODE_LOCAL)
    return jax.shard_map(
        per_device,
        mesh=split,
        in_specs=(
            P(NODE_LOCAL, None),
            P(NODE_LOCAL, None),
            P(LOCAL, None),
            P(LOCAL, None),
            P(LOCAL, None),
            P(LOCAL),
        ),
        out_specs=(
            P(NODE_LOCAL, None),
            P(NODE_LOCAL, None),
            P(NODE_LOCAL, None),
            P(NODE_LOCAL),
            P(NODE_LOCAL, None),
        ),
        check_vma=False,
    )
```

```python
import math

import jax
import jax.numpy as jnp
import numpy as np
from jax import lax
from jax.experimental import pallas as pl
from jax.experimental.pallas import tpu as pltpu
from jax.sharding import Mesh
from jax.sharding import PartitionSpec as P

H = 8
DN = 128
DR = 64
DV = 128
KVL = 512
SEQ = 512
D = 2048
NPARAM = 5374464
EPSILON = 1e-06
ROPE_BASE = 10000.0
LOCAL = ("local_0", "local_1")
NODE_LOCAL = ("node_0", "node_1", "local_0", "local_1")
MESH = pl.DeviceIdType.MESH
AZ, AX, AY, AC = NODE_LOCAL

WCOL = 2176
SUBS = ((0, 640), (640, 1408), (1408, 2176))
SCALE = 1.0 / math.sqrt(DN + DR)
AXES = ((AZ, AX, AY), (AX, AY, AZ), (AY, AZ, AX))
UNITS = tuple((w,) + AXES[n % 3] for n, w in enumerate((256, 256, 256, 256, 256, 128)))
GOFF = (0, 256, 512, 768, 1024, 1280)
GTOT = 1408
F32 = jnp.float32
BF16 = jnp.bfloat16


def rope_constants():
    position = np.arange(SEQ, dtype=np.float32)[:, None]
    freq = np.float32(ROPE_BASE) ** (-np.arange(DR // 2, dtype=np.float32) * np.float32(2.0 / DR))
    angle = (position * freq[None, :].astype(np.float32)).astype(np.float32)
    cosine = np.cos(angle).astype(np.float32)
    sine = np.sin(angle).astype(np.float32)
    return np.concatenate([cosine] * 4, 1), np.concatenate([-sine, sine] * 2, 1)


def nt(a, b):
    return lax.dot_general(a, b, (((1,), (1,)), ((), ())), preferred_element_type=F32)


def nn(a, b):
    return jnp.dot(a, b, preferred_element_type=F32)


def tn(a, b):
    return lax.dot_general(a, b, (((0,), (0,)), ((), ())), preferred_element_type=F32)


def mega(
    tokens_hbm, dout_hbm, cos_hbm, sin_hbm, wq_hbm, wd_hbm, wu_hbm, gain_hbm,
    fin_ref, clip_ref, tg_hbm,
    tokens, dout, cosr, sinr, wbuf, ubuf, gbuf, tokt, acc, qrope, qnope, nrm, nrt, ng, krp, dkr,
    jb, jp, kvg, kvgp, rg, rgp, rgf, invr, gmat, tgb, nbuf, wq_ref, wd_ref, gain_ref, lsem, ssem, rsem, *rest,
):
    nu = len(UNITS)
    part, own, rx, ra, part2, rx2, ra2, part3, ra3 = (rest[n * nu:(n + 1) * nu] for n in range(9))
    iz, ix, iy, ic = (lax.axis_index(a) for a in NODE_LOCAL)
    at = {AZ: iz, AX: ix, AY: iy}
    other = 1 - ic
    STEP = {(a, by): lax.rem(at[a] + (by + 4), 4) for a in at for by in (-1, 0, 1, 2)}

    def step(axis, by):
        return STEP[axis, by]

    recv_table, send_table, owed = {}, {}, []
    scope = []

    def mark(name):
        while scope:
            scope.pop().__exit__(None, None, None)
        if name:
            scope.append(jax.named_scope(name))
            scope[-1].__enter__()

    mark("start")

    def index(table, key):
        return table.setdefault(key, len(table))

    def send(key, src, dst, peer, outgoing=None):
        if outgoing is None:
            outgoing = key
            owed.append((key, src))
        pltpu.make_async_remote_copy(
            src_ref=src, dst_ref=dst,
            send_sem=ssem.at[index(send_table, outgoing)], recv_sem=rsem.at[index(recv_table, key)],
            device_id=peer, device_id_type=MESH).start()

    def arrived(key, ref):
        pltpu.make_async_remote_copy(
            src_ref=ref, dst_ref=ref, send_sem=ssem.at[0], recv_sem=rsem.at[index(recv_table, key)],
            device_id=mate, device_id_type=MESH).wait_recv()

    def left(key, ref):
        pltpu.make_async_remote_copy(
            src_ref=ref, dst_ref=ref, send_sem=ssem.at[index(send_table, key)], recv_sem=rsem.at[0],
            device_id=mate, device_id_type=MESH).wait_send()

    mate = {AC: other}
    barrier = pltpu.get_barrier_semaphore()
    for axis in (AZ, AX, AY):
        for by in (1, -1, 2):
            pl.semaphore_signal(barrier, inc=1, device_id={axis: step(axis, by)}, device_id_type=MESH)
    pl.semaphore_signal(barrier, inc=1, device_id=mate, device_id_type=MESH)

    loads = {}

    def load(name, src, dst):
        d = pltpu.make_async_copy(src, dst, lsem.at[len(loads)])
        d.start()
        loads[name] = d

    for p in range(8):
        pltpu.make_async_copy(wu_hbm.at[:, p * 256:(p + 1) * 256], ubuf.at[iy, ic, p], lsem.at[8]).start()

    load("down", wd_hbm, wd_ref)
    load("query", wq_hbm, wq_ref)
    load("gain", gain_hbm, gain_ref)
    load("tokens", tokens_hbm, tokens)
    load("dout", dout_hbm, dout)
    load("cos", cos_hbm, cosr)
    load("sin", sin_hbm, sinr)

    loads["down"].wait()
    down = jnp.concatenate([wd_ref[...], jnp.zeros((64, 256), BF16)], 0)
    wbuf[iy, ic, :, :, 0:640] = down.T.reshape(8, 32, 640)
    loads["query"].wait()
    for n in range(4):
        lo = 640 + n * 384
        h = n * 384
        both = jnp.concatenate([
            wq_ref[:, h:h + 128], wq_ref[:, h + 192:h + 320],
            wq_ref[:, h + 128:h + 192], wq_ref[:, h + 320:h + 384]], 1)
        wbuf[iy, ic, :, :, lo:lo + 384] = both.reshape(8, 32, 384)
    loads["gain"].wait()
    gbuf[iy, ic] = jnp.broadcast_to(
        jnp.concatenate([gain_ref[...].astype(F32), jnp.zeros((1, 64), F32)], 1), (8, 128))
    own_up = ubuf.at[iy, ic]
    pltpu.make_async_copy(own_up, own_up, lsem.at[8]).wait()
    pl.semaphore_wait(barrier, 10)

    RING = (AX, AZ)
    YO = (step(AY, -1), step(AY, 1), step(AY, 2))
    PIECE = {(k, by): k * 4 + step(RING[k], by) for k in range(2) for by in (-1, 0, 1, 2)}
    KINDS = (0, "u", 1, 2)

    def block_of(kind, yy, core):
        if kind == "u":
            return ubuf.at[yy, core]
        lo, hi = SUBS[kind]
        return wbuf.at[yy, core, :, :, lo:hi]

    def piece(kind, yy, k, by):
        if kind == "u":
            return ubuf.at[yy, ic, PIECE[k, by]]
        lo, hi = SUBS[kind]
        return wbuf.at[yy, ic, PIECE[k, by], :, lo:hi]

    def half_piece(kind, yy, k, by, d):
        if kind == "u":
            return ubuf.at[yy, ic, PIECE[k, by], d * 32:d * 32 + 32]
        lo, hi = SUBS[kind]
        return wbuf.at[yy, ic, PIECE[k, by], d * 16:d * 16 + 16, lo:hi]

    def span(kind, n):
        if kind == "u":
            return ubuf.at[0, 0, 0:n]
        lo, hi = SUBS[kind]
        return wbuf.at[0, 0, 0:n, :, lo:hi]

    def link_send(key, kind, r, axis, by):
        send(key, r, r, {axis: step(axis, by)}, ("links", kind))

    def piece_to_mate(kind, yo, k, by):
        r = piece(kind, YO[yo], k, by)
        send(("d", kind), r, r, mate, ("d", kind))

    def y_send(kind):
        for k in range(2):
            r = piece(kind, iy, k, 0)
            link_send(("y", kind), kind, r, AY, 1)
            link_send(("y", kind), kind, r, AY, -1)

    def pset(yo):
        return yo // 2

    def p_send(kind, k, yo):
        r = piece(kind, YO[yo], k, 0)
        link_send(("p", kind, pset(yo)), kind, r, RING[k], 1)
        link_send(("p", kind, pset(yo)), kind, r, RING[k], -1)

    def y_take(kind):
        arrived(("y", kind), span(kind, 4))
        for k in range(2):
            for d in range(2):
                half = half_piece(kind, YO[d], k, 0, d)
                link_send(("y2", kind), kind, half, AY, 1 if d == 0 else -1)
                p_send(kind, k, d)
        for k in range(2):
            for d in range(2):
                piece_to_mate(kind, d, k, 0)

    def y2_take(kind):
        arrived(("y2", kind), span(kind, 2))
        for k in range(2):
            p_send(kind, k, 2)
            piece_to_mate(kind, 2, k, 0)

    def p_take(kind, *yos):
        arrived(("p", kind, pset(yos[0])), span(kind, 4 * len(yos)))
        for yo in yos:
            for k in range(2):
                for d in range(2):
                    by = -1 if d == 0 else 1
                    half = half_piece(kind, YO[yo], k, by, d)
                    link_send(("p2", kind, pset(yo)), kind, half, RING[k], -by)
        for yo in yos:
            for k in range(2):
                for by in (-1, 1):
                    piece_to_mate(kind, yo, k, by)

    def p2_take(kind, *yos):
        arrived(("p2", kind, pset(yos[0])), span(kind, 2 * len(yos)))
        for yo in yos:
            for k in range(2):
                piece_to_mate(kind, yo, k, 2)

    def own_to_mate(kind):
        r = block_of(kind, iy, ic)
        send(("d", kind), r, r, mate, ("d", kind))

    def from_mate(kind):
        if kind == "u":
            arrived(("d", kind), ubuf.at[:, other])
        else:
            lo, hi = SUBS[kind]
            arrived(("d", kind), wbuf.at[:, other, :, :, lo:hi])

    def project(lo, hi):
        return nn(tokens[...], wbuf[:, :, :, :, lo:hi].reshape(2048, hi - lo))

    mark("gather")
    y_send(0)
    y_send("u")
    y_send(1)
    own_to_mate(0)
    g = gbuf.at[iy, ic]
    for n, by in enumerate((1, -1, 2)):
        send("g", g, g, {AY: step(AY, by)}, "g")
    send("gd", g, g, mate, "gd")
    own_to_mate("u")
    mark("y0")
    y_take(0)
    own_to_mate(1)
    mark("yu")
    y_take("u")
    y_send(2)
    own_to_mate(2)
    loads["tokens"].wait()
    mark("transpose")
    for z in range(2):
        tokt[z, :, :, :, 0:512] = tokens[:, z * 512:(z + 1) * 512].T.reshape(4, 4, 32, 512)
    mark("y20")
    y2_take(0)
    mark("p0a")
    p_take(0, 0, 1)
    mark("y1")
    y_take(1)
    mark("y2u")
    y2_take("u")
    mark("pua")
    p_take("u", 0, 1)
    mark("p0b")
    p_take(0, 2)
    mark("transpose")
    for z in range(2, 4):
        tokt[z, :, :, :, 0:512] = tokens[:, z * 512:(z + 1) * 512].T.reshape(4, 4, 32, 512)
    mark("y21")
    y2_take(1)
    mark("p1a")
    p_take(1, 0, 1)
    mark("pub")
    p_take("u", 2)
    mark("p20")
    p2_take(0, 0, 1)
    mark("y2")
    y_take(2)
    mark("p202")
    p2_take(0, 2)
    mark("p1b")
    p_take(1, 2)
    mark("y22")
    y2_take(2)
    mark("g")
    arrived("g", gbuf.at[0:3, 0])
    for by in (-1, 1, 2):
        gg = gbuf.at[step(AY, by), ic]
        send("gd", gg, gg, mate, "gd")
    mark("down")
    from_mate(0)
    acc[...] = project(*SUBS[0])
    mark("p2u")
    p2_take("u", 0, 1)
    p2_take("u", 2)
    mark("p2a")
    p_take(2, 0, 1)
    mark("p21")
    p2_take(1, 0, 1)
    p2_take(1, 2)
    mark("pre")
    arrived("gd", gbuf.at[:, other])

    for name in ("dout", "cos", "sin"):
        loads[name].wait()

    lane = lax.broadcasted_iota(jnp.int32, (1, 128), 1)
    low = lax.rem(lane, 64) < 32

    def swap(v):
        return jnp.where(low, pltpu.roll(v, 96, 1), pltpu.roll(v, 32, 1))

    def rot(v, sign):
        return v * cosr[...] + swap(v) * (sinr[...] * sign)

    gain = jnp.concatenate([gbuf[y, c, 0:1, 0:64] for y in range(4) for c in range(2)], 1)
    kr = rot(acc[:, 512:640], 1.0)
    krp[0] = jnp.where(lane < 64, kr, 0.0).astype(BF16)
    krp[1] = jnp.where(lane < 64, 0.0, pltpu.roll(kr, 64, 1)).astype(BF16)
    for n in range(4):
        rows = slice(n * 128, (n + 1) * 128)
        latent = acc[rows, 0:512]
        inv = lax.rsqrt(jnp.mean(latent * latent, axis=-1, keepdims=True) + EPSILON)
        unit = latent * inv
        acc[rows, 0:512] = unit
        invr[rows] = jnp.broadcast_to(inv, (128, 128))
        nrm[rows] = (unit * gain).astype(BF16)
    nrt[:, 0:512] = nrm[...].T
    send(("nrt",), nrt.at[:, 0:512], nrt.at[:, 512:1024], mate)
    ng[...] = jnp.zeros((512, 512), F32)
    dkr[...] = jnp.zeros((512, 128), F32)
    send(("tok",), tokt.at[:, :, :, :, 0:512], tokt.at[:, :, :, :, 512:1024], mate)
    mark("p2b")
    p_take(2, 2)
    mark("mateu")
    from_mate("u")
    mark("heads")

    tri = (lax.broadcasted_iota(jnp.int32, (256, 256), 0)
           <= lax.broadcasted_iota(jnp.int32, (256, 256), 1))

    def block(kf, v, qf, do):
        rows = kf.shape[0]
        s = nt(kf, qf) * SCALE
        masked = jnp.where(tri, s[rows - 256:], -1e30)
        s = masked if rows == 256 else jnp.concatenate([s[:rows - 256], masked], 0)
        w = jnp.exp(s - jnp.max(s, axis=0, keepdims=True))
        probs = w * (1.0 / jnp.sum(w, axis=0, keepdims=True))
        dp = nt(v, do)
        delta = jnp.sum(probs * dp, axis=0, keepdims=True)
        ds = (probs * (dp - delta) * SCALE).astype(BF16)
        return probs.astype(BF16), ds

    def queries(s):
        from_mate(s + 1)
        lo = SUBS[s + 1][0]
        q = project(lo, lo + 768)
        for m in range(2):
            n = 2 * s + m
            qnope[:, n * 256:(n + 1) * 256] = q[:, m * 384:m * 384 + 256].astype(BF16)
            rope = q[:, m * 384 + 256:m * 384 + 384].astype(BF16).astype(F32)
            qrope[:, n * 128:(n + 1) * 128] = rot(rope, 1.0).astype(BF16)

    def pair(n, carry):
        @pl.when(n == 0)
        def _():
            queries(0)

        @pl.when(n == 1)
        def _():
            p2_take(2, 0, 1)
            p2_take(2, 2)

        @pl.when(n == 2)
        def _():
            queries(1)

        half, m = n // 2, lax.rem(n, 2)
        qr = qrope[:, pl.ds(pl.multiple_of(n * 128, 128), 128)]
        total = None
        for e in range(2):
            h = 2 * n + e
            hc = pl.ds(pl.multiple_of(h * 128, 128), 128)
            jc = pl.ds(pl.multiple_of((m * 2 + e) * 128, 128), 128)
            u = ubuf[:, :, h].reshape(512, 256)
            kv = nn(nrm[...], u).astype(BF16)
            kf = jnp.concatenate([kv[:, :128], krp[e]], 1)
            v = kv[:, 128:]
            qf = jnp.concatenate([qnope[:, hc], qr], 1)
            do = dout[:, hc]
            pa, da = block(kf[:256], v[:256], qf[:256], do[:256])
            pb, db = block(kf, v, qf[256:], do[256:])
            dv = nn(pb, do[256:])
            dv = jnp.concatenate([dv[:256] + nn(pa, do[:256]), dv[256:]], 0)
            dk = nn(db, qf[256:])
            dk = jnp.concatenate([dk[:256] + nn(da, qf[:256]), dk[256:]], 0)
            dq = jnp.concatenate([tn(da, kf[:256]), tn(db, kf)], 0)
            jb[half, :, jc] = dq[:, :128].astype(BF16)
            total = dq[:, 128:] if e == 0 else total + dq[:, 128:]
            keep = lane < 64 if e == 0 else lane >= 64
            dkr[...] += jnp.where(keep, dk[:, 128:], 0.0)
            kg = dk[:, :128].astype(BF16)
            vg = dv.astype(BF16)
            kvg[half, 0, :, jc] = kg
            kvg[half, 1, :, jc] = vg
            ng[...] += nt(jnp.concatenate([kg, vg], 1), u)
        jb[half, :, pl.ds(pl.multiple_of(512 + m * 128, 128), 128)] = rot(total, -1.0).astype(BF16)
        return carry

    lax.fori_loop(0, 4, pair, 0)
    mark("post")
    send(("j",), jb.at[other, :, 0:768], jp.at[:, 0:768], mate)

    gterm = jnp.zeros((1, 512), F32)
    for n in range(4):
        rows = slice(n * 128, (n + 1) * 128)
        unit = acc[rows, 0:512]
        grad = ng[rows]
        gterm = gterm + jnp.sum(grad * unit, axis=0, keepdims=True)
        scaled = grad * gain
        inner = jnp.mean(scaled * unit, axis=-1, keepdims=True)
        value = (invr[rows, 0:1] * (scaled - unit * inner)).astype(BF16)
        jb[0, rows, 768:1024] = value[:, :256]
        jb[1, rows, 768:1024] = value[:, 256:]
    dk = dkr[...]
    rope = jnp.where(lane < 64, rot(dk + pltpu.roll(dk, 64, 1), -1.0), 0.0)
    rgf[...] = rope.astype(BF16)
    rg[0] = jnp.where(lane < 32, rope, 0.0).astype(BF16)
    rg[1] = jnp.where(lane < 32, pltpu.roll(rope, 96, 1), 0.0).astype(BF16)
    send(("kvg",), kvg.at[other], kvgp, mate)
    send(("jl",), jb.at[other, :, 768:1024], jp.at[:, 768:1024], mate)
    send(("rg",), rg.at[other], rgp, mate)
    column = jnp.broadcast_to(gterm, (128, 512)).T
    column = jnp.where(lane == 32, column, 0.0).reshape(64, 8, 128)
    gmat[...] = jnp.concatenate([column, jnp.zeros((64, 24, 128), F32)], 1).reshape(4, 4, 4, 32, 128)

    tgd = []

    def token_block():
        n = len(tgd)
        w = wbuf[n].reshape(512, WCOL)
        cols = [jb[0, :, 768:], jb[1, :, 768:], rgf[...]]
        for m in range(4):
            cols += [jb[m // 2, :, m % 2 * 256:m % 2 * 256 + 256],
                     jb[m // 2, :, 512 + m % 2 * 128:640 + m % 2 * 128]]
        tgb[n] = nt(jnp.concatenate(cols, 1), w).astype(BF16)
        d = pltpu.make_async_copy(tgb.at[n], tg_hbm.at[:, n * 512:(n + 1) * 512], lsem.at[9])
        d.start()
        tgd.append(d)

    mark("waitmate")
    arrived(("tok",), tokt.at[:, :, :, :, 512:1024])
    arrived(("nrt",), nrt.at[:, 512:1024])
    arrived(("j",), jp.at[:, 0:768])

    A, B = (0, 1, 2), (3, 4, 5)
    def keep(u, z, cols, value):
        g = u % 3
        value = value.astype(BF16)
        if g == 0:
            part[u][z, :, :, :, cols] = value
        elif g == 1:
            part[u][:, z, :, :, cols] = value
        else:
            for x in range(4):
                part[u][:, z, x, :, cols] = value[x]

    def token_rows(z):
        return tokt[z].reshape(512, 1024)

    def products_a():
        right = jnp.concatenate([jb[ic, :, 0:768], jp[:, 0:768]], 0)
        for z in range(4):
            both = nn(token_rows(z), right).reshape(4, 4, 32, 768)
            for u in A:
                keep(u, z, slice(0, 256), both[..., u * 256:u * 256 + 256])

    def products_b():
        right = jnp.concatenate([
            jnp.concatenate([jb[ic, :, 768:1024], rg[ic]], 1),
            jnp.concatenate([jp[:, 768:1024], rgp[...]], 1)], 0)
        for z in range(4):
            both = nn(token_rows(z), right).reshape(4, 4, 32, 384)
            for u in (3, 4):
                keep(u, z, slice(0, 128), both[..., (u - 3) * 128:(u - 2) * 128])
            keep(5, z, slice(0, 128), both[..., 256:] + gmat[z])
        for u in (3, 4):
            up = nn(nrt[...], jnp.concatenate([kvg[ic, u - 3], kvgp[u - 3]], 0))
            up = up.reshape(64, 8, 512)
            up = jnp.concatenate([up[:, :, j * 128:(j + 1) * 128] for j in range(4)], 1)
            up = up.reshape(4, 4, 4, 32, 128)
            for z in range(4):
                keep(u, z, slice(128, 256), up[z])

    def ways(axis):
        return {axis: step(axis, 1)}, {axis: step(axis, -1)}

    def ring_sends(phase, u, p, r, a):
        axis = UNITS[u][phase]
        right, left_ = ways(axis)
        far, near, back = (p[u].at[step(axis, by)] for by in (2, 1, -1))
        send(("x", phase, u), far.at[0:2], r[u].at[0], right, ("s", phase, u))
        send(("x", phase, u), far.at[2:4], r[u].at[1], left_, ("s", phase, u))
        send(("a", phase, u), near.at[2:4], a[u].at[0, 2:4], right, ("s", phase, u))
        send(("a", phase, u), back.at[0:2], a[u].at[1, 0:2], left_, ("s", phase, u))

    def relay(phase, us, p, r, a):
        for u in us:
            axis = UNITS[u][phase]
            right, left_ = ways(axis)
            near, back = (p[u].at[step(axis, by)] for by in (1, -1))
            arrived(("x", phase, u), r[u])
            near[0:2] = (near[0:2].astype(F32) + r[u][0].astype(F32)).astype(BF16)
            back[2:4] = (back[2:4].astype(F32) + r[u][1].astype(F32)).astype(BF16)
            send(("a", phase, u), near.at[0:2], a[u].at[0, 0:2], right, ("s", phase, u))
            send(("a", phase, u), back.at[2:4], a[u].at[1, 2:4], left_, ("s", phase, u))

    def second(u, t):
        return own[u].at[:, t] if u % 3 == 1 else own[u].at[t]

    def second_sends(us):
        for u in us:
            arrived(("a", 1, u), ra[u])
            total = part[u][at[UNITS[u][1]]].astype(F32) + (ra[u][0].astype(F32) + ra[u][1].astype(F32))
            own[u][...] = total
            if u % 3 == 1:
                for z in range(4):
                    part2[u][:, z] = total[z].astype(BF16)
            else:
                part2[u][...] = total.astype(BF16)
            ring_sends(2, u, part2, rx2, ra2)

    def third_sends(us):
        for u in us:
            arrived(("a", 2, u), ra2[u])
            mine = second(u, at[UNITS[u][2]])
            mine[...] += ra2[u][0].astype(F32) + ra2[u][1].astype(F32)
            for slot, by in enumerate((2, 1, -1)):
                part3[u][slot] = mine[step(UNITS[u][3], by)].astype(BF16)
                send(("a", 3, u), part3[u].at[slot], ra3[u].at[slot],
                     {UNITS[u][3]: step(UNITS[u][3], by)}, ("s", 3, u))

    def last_sums(us):
        for u in us:
            arrived(("a", 3, u), ra3[u])
            mine = second(u, at[UNITS[u][2]])[at[UNITS[u][3]]]
            fin_ref[ic, :, GOFF[u]:GOFF[u] + UNITS[u][0]] = mine + (
                ra3[u][0].astype(F32) + ra3[u][1].astype(F32) + ra3[u][2].astype(F32))

    mark("firstA")
    products_a()
    for u in A:
        ring_sends(1, u, part, rx, ra)
    mark("mateB")
    arrived(("kvg",), kvgp)
    arrived(("jl",), jp.at[:, 768:1024])
    arrived(("rg",), rgp)
    mark("productsB")
    products_b()
    for u in B:
        ring_sends(1, u, part, rx, ra)
    mark("tg")
    token_block()
    mark("relayA")
    relay(1, A, part, rx, ra)
    mark("tg")
    token_block()
    token_block()
    mark("relayB")
    relay(1, B, part, rx, ra)
    mark("tg")
    token_block()
    mark("secondA")
    second_sends(A)
    mark("secondB")
    second_sends(B)
    mark("relay2A")
    relay(2, A, part2, rx2, ra2)
    mark("relay2B")
    relay(2, B, part2, rx2, ra2)
    mark("thirdA")
    third_sends(A)
    mark("thirdB")
    third_sends(B)
    mark("lastA")
    last_sums(A)
    send(("fin", 0), fin_ref.at[ic, :, 0:768], fin_ref.at[ic, :, 0:768], mate)
    mark("lastB")
    last_sums(B)
    send(("fin", 1), fin_ref.at[ic, :, 768:GTOT], fin_ref.at[ic, :, 768:GTOT], mate)
    mark("fin")
    arrived(("fin", 0), fin_ref.at[other, :, 0:768])
    arrived(("fin", 1), fin_ref.at[other, :, 768:GTOT])

    both = fin_ref[...]
    tail = GTOT - 128
    gains = both[0, :, tail:] + both[1, :, tail:]
    body = both[:, :, :tail]
    squares = jnp.sum(jnp.sum(body * body, axis=0), axis=0, keepdims=True)
    row = sum(squares[:, n * 128:(n + 1) * 128] for n in range(10))
    ropes = jnp.where(lane == 32, 0.0, both[0, :, tail:] ** 2 + both[1, :, tail:] ** 2)
    ropes = ropes + jnp.where(lane == 32, gains * gains, 0.0)
    row = row + jnp.sum(ropes, axis=0, keepdims=True)
    row = jnp.broadcast_to(row, (8, 128))
    mark("norm")
    lead = ic == 1
    for n, axis in enumerate((AY, AX, AZ)):
        @pl.when(lead)
        def _():
            nbuf[n, 3] = row if n == 0 else (nbuf[n - 1, 0] + nbuf[n - 1, 1]) + (nbuf[n - 1, 2] + nbuf[n - 1, 3])
            for m, by in enumerate((1, -1, 2)):
                send(("n", n), nbuf.at[n, 3], nbuf.at[n, m], {axis: step(axis, by)}, ("n", n))

        @pl.when(lead)
        def _():
            arrived(("n", n), nbuf.at[n, 0:3])

    @pl.when(lead)
    def _():
        nbuf[3, 0] = (nbuf[2, 0] + nbuf[2, 1]) + (nbuf[2, 2] + nbuf[2, 3])
        send("nd", nbuf.at[3, 0], nbuf.at[3, 0], mate, "nd")
        for n in range(3):
            left(("n", n), nbuf.at[n, 0:3])
        left("nd", nbuf.at[3, 0])

    @pl.when(jnp.logical_not(lead))
    def _():
        arrived("nd", nbuf.at[3, 0])

    total = jnp.sum(nbuf[3, 0], axis=-1, keepdims=True)
    clip = jnp.minimum(1.0, lax.rsqrt(total / NPARAM + 1e-06))
    clip_ref[...] = jnp.broadcast_to(clip, (8, 128))

    mark("drain")
    for key, ref in owed:
        left(key, ref)
    left("g", gbuf.at[0:3, 0])
    left("gd", gbuf.at[:, 0])
    for kind in KINDS:
        if kind == "u":
            left(("links", kind), ubuf.at[0:3, 0])
            left(("d", kind), ubuf.at[:, 0])
        else:
            lo, hi = SUBS[kind]
            left(("links", kind), wbuf.at[0:3, 0, :, :, lo:hi])
            left(("d", kind), wbuf.at[:, 0, :, :, lo:hi])
    for u in range(nu):
        left(("s", 1, u), part[u].at[0:3])
        left(("s", 2, u), part2[u].at[0:3])
        left(("s", 3, u), part3[u])
    pltpu.make_async_copy(tgb, tgb, lsem.at[9]).wait()
    mark(None)
    assert len(recv_table) == NRECV and len(send_table) == NSEND, (len(recv_table), len(send_table))


NRECV = 72
NSEND = 40


def scratch():
    v = pltpu.VMEM
    dma = pltpu.SemaphoreType.DMA
    shapes = [
        v((512, 2048), BF16), v((512, 1024), BF16), v((512, 128), F32), v((512, 128), F32),
        v((4, 2, 8, 32, WCOL), BF16), v((4, 2, 8, 64, 256), BF16), v((4, 2, 8, 128), F32),
        v((4, 4, 4, 32, 1024), BF16), v((512, 640), F32),
        v((512, 512), BF16), v((512, 1024), BF16), v((512, 512), BF16), v((512, 1024), BF16),
        v((512, 512), F32), v((2, 512, 128), BF16), v((512, 128), F32),
        v((2, 512, 1024), BF16), v((512, 1024), BF16), v((2, 2, 512, 512), BF16), v((2, 512, 512), BF16),
        v((2, 512, 128), BF16), v((512, 128), BF16), v((512, 128), BF16), v((512, 128), F32),
        v((4, 4, 4, 32, 128), F32), v((4, 512, 512), BF16), v((4, 4, 8, 128), F32),
        v((256, 1536), BF16), v((576, 256), BF16), v((1, 64), BF16),
        dma((10,)), dma((NSEND,)), dma((NRECV,)),
    ]
    ws = [w for w, *_ in UNITS]
    shapes += [v((4, 4, 4, 32, w), BF16) for w in ws]
    shapes += [v((4, 4, 32, w), F32) for w in ws]
    shapes += [v((2, 2, 4, 32, w), BF16) for w in ws]
    shapes += [v((2, 4, 4, 32, w), BF16) for w in ws]
    shapes += [v((4, 4, 32, w), BF16) for w in ws]
    shapes += [v((2, 2, 32, w), BF16) for w in ws]
    shapes += [v((2, 4, 32, w), BF16) for w in ws]
    shapes += [v((3, 32, w), BF16) for w in ws]
    shapes += [v((3, 32, w), BF16) for w in ws]
    return shapes


def last_step(fin_hbm, clip_hbm, tg_in, gq_ref, gd_ref, gu_ref, gg_ref, tg_out,
              fin_ref, clip_ref, stage, isem, osem):
    ic = lax.axis_index(AC)
    first_reads = []
    for n, (src, dst) in enumerate(((fin_hbm, fin_ref), (clip_hbm, clip_ref))):
        d = pltpu.make_async_copy(src, dst, isem.at[4 + n])
        d.start()
        first_reads.append(d)
    reads = []
    for n in range(4):
        rows = slice(n * 128, (n + 1) * 128)
        d = pltpu.make_async_copy(tg_in.at[rows], stage.at[n], isem.at[n])
        d.start()
        reads.append(d)
    writes = []
    for n in range(4):
        rows_n = slice(n * 128, (n + 1) * 128)
        reads[n].wait()
        d = pltpu.make_async_copy(stage.at[n], tg_out.at[rows_n], osem.at[n])
        d.start()
        writes.append(d)
    for d in first_reads:
        d.wait()
    clip = clip_ref[0:1, 0:1]
    first = ic == 0

    def rows(half, cols):
        return jnp.where(first, fin_ref[half, 0:16, cols], fin_ref[half, 16:32, cols]) * clip

    def cols(lo):
        return slice(lo, lo + 128)

    for n in range(4):
        half, m = n // 2, n % 2
        rope = rows(half, cols(512 + m * 128))
        gq_ref[:, n * 384:(n + 1) * 384] = jnp.concatenate(
            [rows(half, cols(m * 256)), rope[:, :64], rows(half, cols(m * 256 + 128)), rope[:, 64:]], 1)
        gd_ref[:, n * 128:(n + 1) * 128] = rows(half, cols(768 + m * 256))
    tail = slice(GTOT - 128, GTOT)
    gd_ref[:, 512:576] = jnp.concatenate([rows(0, tail)[:, :32], rows(1, tail)[:, :32]], 1)
    for h in range(H):
        half, j = h // 4, h % 4
        for u in range(2):
            block = fin_ref[half, j * 8:j * 8 + 8, cols(896 + u * 256)] * clip
            gu_ref[:, h * 256 + u * 128:h * 256 + u * 128 + 128] = jnp.where(first, block[0:4], block[4:8])
    gain = (fin_ref[0, 0:8, tail] + fin_ref[1, 0:8, tail]) * clip
    gain = jnp.where(first, gain[0:4], gain[4:8])
    spread = (lax.broadcasted_iota(jnp.int32, (4, 128), 0)
              == lax.broadcasted_iota(jnp.int32, (4, 128), 1))
    gg_ref[...] = jnp.sum(jnp.where(spread, gain[:, 32:33], 0.0), axis=0)[0:4]
    for d in writes:
        d.wait()


def finish(fin, clip, token_grad):
    vm = pl.BlockSpec(memory_space=pltpu.VMEM)
    anyspace = pl.BlockSpec(memory_space=pl.ANY)
    return pl.pallas_call(
        last_step,
        out_shape=(
            jax.ShapeDtypeStruct((16, 1536), F32),
            jax.ShapeDtypeStruct((16, 576), F32),
            jax.ShapeDtypeStruct((4, 2048), F32),
            jax.ShapeDtypeStruct((4,), F32),
            jax.ShapeDtypeStruct((SEQ, D), BF16),
        ),
        in_specs=[anyspace] * 3,
        out_specs=(vm, vm, vm, vm, anyspace),
        scratch_shapes=[
            pltpu.VMEM((2, 32, GTOT), F32), pltpu.VMEM((8, 128), F32),
            pltpu.VMEM((4, 128, D), BF16), pltpu.SemaphoreType.DMA((6,)), pltpu.SemaphoreType.DMA((4,))],
    )(fin, clip, token_grad)


def per_device(tokens, d_out, w_query, w_down, w_up, latent_gain):
    cosine, sine = rope_constants()
    vm = pl.BlockSpec(memory_space=pltpu.VMEM)
    anyspace = pl.BlockSpec(memory_space=pl.ANY)
    fin, clip, token_grad = pl.pallas_call(
        mega,
        out_shape=(
            jax.ShapeDtypeStruct((2, 32, GTOT), F32),
            jax.ShapeDtypeStruct((8, 128), F32),
            jax.ShapeDtypeStruct((SEQ, D), BF16),
        ),
        in_specs=[anyspace] * 8,
        out_specs=(vm, vm, anyspace),
        scratch_shapes=scratch(),
        compiler_params=pltpu.CompilerParams(
            collective_id=0, has_side_effects=True, vmem_limit_bytes=67043328),
    )(tokens, d_out, jnp.asarray(cosine), jnp.asarray(sine), w_query, w_down.T, w_up,
      latent_gain.reshape(1, 64))
    return finish(fin, clip, token_grad)


def solution(mesh):
    split = Mesh(mesh.devices.reshape(4, 4, 4, 2), NODE_LOCAL)
    return jax.shard_map(
        per_device,
        mesh=split,
        in_specs=(
            P(NODE_LOCAL, None),
            P(NODE_LOCAL, None),
            P(LOCAL, None),
            P(LOCAL, None),
            P(LOCAL, None),
            P(LOCAL),
        ),
        out_specs=(
            P(NODE_LOCAL, None),
            P(NODE_LOCAL, None),
            P(NODE_LOCAL, None),
            P(NODE_LOCAL),
            P(NODE_LOCAL, None),
        ),
        check_vma=False,
    )
```

```python
import math

import jax
import jax.numpy as jnp
import numpy as np
from jax import lax
from jax.experimental import pallas as pl
from jax.experimental.pallas import tpu as pltpu
from jax.sharding import Mesh
from jax.sharding import PartitionSpec as P

H = 8
DN = 128
DR = 64
DV = 128
KVL = 512
SEQ = 512
D = 2048
NPARAM = 5374464
EPSILON = 1e-06
ROPE_BASE = 10000.0
LOCAL = ("local_0", "local_1")
NODE_LOCAL = ("node_0", "node_1", "local_0", "local_1")
MESH = pl.DeviceIdType.MESH
AZ, AX, AY, AC = NODE_LOCAL

WCOL = 2176
SUBS = ((0, 640), (640, 1408), (1408, 2176))
SCALE = 1.0 / math.sqrt(DN + DR)
AXES = ((AZ, AX, AY), (AX, AY, AZ), (AY, AZ, AX))
UNITS = tuple((w,) + AXES[n % 3] for n, w in enumerate((128,) * 6 + (256, 256, 128)))
GOFF = (0, 128, 256, 384, 512, 640, 768, 1024, 1280)
GTOT = 1408
F32 = jnp.float32
BF16 = jnp.bfloat16


def rope_constants():
    position = np.arange(SEQ, dtype=np.float32)[:, None]
    freq = np.float32(ROPE_BASE) ** (-np.arange(DR // 2, dtype=np.float32) * np.float32(2.0 / DR))
    angle = (position * freq[None, :].astype(np.float32)).astype(np.float32)
    cosine = np.cos(angle).astype(np.float32)
    sine = np.sin(angle).astype(np.float32)
    return np.concatenate([cosine] * 4, 1), np.concatenate([-sine, sine] * 2, 1)


def nt(a, b):
    return lax.dot_general(a, b, (((1,), (1,)), ((), ())), preferred_element_type=F32)


def nn(a, b):
    return jnp.dot(a, b, preferred_element_type=F32)


def tn(a, b):
    return lax.dot_general(a, b, (((0,), (0,)), ((), ())), preferred_element_type=F32)


def mega(
    tokens_hbm, dout_hbm, cos_hbm, sin_hbm, wq_hbm, wd_hbm, wu_hbm, gain_hbm,
    fin_ref, clip_ref, tg_hbm,
    tokens, dout, cosr, sinr, wbuf, ubuf, gbuf, tokt, acc, qrope, qnope, nrm, nrt, ng, krp, dkr,
    jb, jp, kvg, kvgp, rg, rgp, rgf, invr, gmat, tgb, nbuf, wq_ref, wd_ref, gain_ref, lsem, ssem, rsem, *rest,
):
    nu = len(UNITS)
    part, own, rx, ra, part2, rx2, ra2, part3, ra3 = (rest[n * nu:(n + 1) * nu] for n in range(9))
    iz, ix, iy, ic = (lax.axis_index(a) for a in NODE_LOCAL)
    at = {AZ: iz, AX: ix, AY: iy}
    other = 1 - ic
    STEP = {(a, by): lax.rem(at[a] + (by + 4), 4) for a in at for by in (-1, 0, 1, 2)}

    def step(axis, by):
        return STEP[axis, by]

    recv_table, send_table, owed = {}, {}, []
    scope = []

    def mark(name):
        while scope:
            scope.pop().__exit__(None, None, None)
        if name:
            scope.append(jax.named_scope(name))
            scope[-1].__enter__()

    mark("start")

    def index(table, key):
        return table.setdefault(key, len(table))

    def send(key, src, dst, peer, outgoing=None):
        if outgoing is None:
            outgoing = key
            owed.append((key, src))
        pltpu.make_async_remote_copy(
            src_ref=src, dst_ref=dst,
            send_sem=ssem.at[index(send_table, outgoing)], recv_sem=rsem.at[index(recv_table, key)],
            device_id=peer, device_id_type=MESH).start()

    def arrived(key, ref):
        pltpu.make_async_remote_copy(
            src_ref=ref, dst_ref=ref, send_sem=ssem.at[0], recv_sem=rsem.at[index(recv_table, key)],
            device_id=mate, device_id_type=MESH).wait_recv()

    def left(key, ref):
        pltpu.make_async_remote_copy(
            src_ref=ref, dst_ref=ref, send_sem=ssem.at[index(send_table, key)], recv_sem=rsem.at[0],
            device_id=mate, device_id_type=MESH).wait_send()

    mate = {AC: other}
    barrier = pltpu.get_barrier_semaphore()
    for axis in (AZ, AX, AY):
        for by in (1, -1, 2):
            pl.semaphore_signal(barrier, inc=1, device_id={axis: step(axis, by)}, device_id_type=MESH)
    pl.semaphore_signal(barrier, inc=1, device_id=mate, device_id_type=MESH)

    loads = {}

    def load(name, src, dst):
        d = pltpu.make_async_copy(src, dst, lsem.at[len(loads)])
        d.start()
        loads[name] = d

    for p in range(8):
        pltpu.make_async_copy(wu_hbm.at[:, p * 256:(p + 1) * 256], ubuf.at[iy, ic, p], lsem.at[8]).start()

    load("down", wd_hbm, wd_ref)
    load("query", wq_hbm, wq_ref)
    load("gain", gain_hbm, gain_ref)
    load("tokens", tokens_hbm, tokens)
    load("dout", dout_hbm, dout)
    load("cos", cos_hbm, cosr)
    load("sin", sin_hbm, sinr)

    loads["down"].wait()
    down = jnp.concatenate([wd_ref[...], jnp.zeros((64, 256), BF16)], 0)
    wbuf[iy, ic, :, :, 0:640] = down.T.reshape(8, 32, 640)
    loads["query"].wait()
    for n in range(4):
        lo = 640 + n * 384
        h = n * 384
        both = jnp.concatenate([
            wq_ref[:, h:h + 128], wq_ref[:, h + 192:h + 320],
            wq_ref[:, h + 128:h + 192], wq_ref[:, h + 320:h + 384]], 1)
        wbuf[iy, ic, :, :, lo:lo + 384] = both.reshape(8, 32, 384)
    loads["gain"].wait()
    gbuf[iy, ic] = jnp.broadcast_to(
        jnp.concatenate([gain_ref[...].astype(F32), jnp.zeros((1, 64), F32)], 1), (8, 128))
    own_up = ubuf.at[iy, ic]
    pltpu.make_async_copy(own_up, own_up, lsem.at[8]).wait()
    pl.semaphore_wait(barrier, 10)

    RING = (AX, AZ)
    YO = (step(AY, -1), step(AY, 1), step(AY, 2))
    PIECE = {(k, by): k * 4 + step(RING[k], by) for k in range(2) for by in (-1, 0, 1, 2)}
    KINDS = (0, "u", 1, 2)

    def block_of(kind, yy, core):
        if kind == "u":
            return ubuf.at[yy, core]
        lo, hi = SUBS[kind]
        return wbuf.at[yy, core, :, :, lo:hi]

    def piece(kind, yy, k, by):
        if kind == "u":
            return ubuf.at[yy, ic, PIECE[k, by]]
        lo, hi = SUBS[kind]
        return wbuf.at[yy, ic, PIECE[k, by], :, lo:hi]

    def half_piece(kind, yy, k, by, d):
        if kind == "u":
            return ubuf.at[yy, ic, PIECE[k, by], d * 32:d * 32 + 32]
        lo, hi = SUBS[kind]
        return wbuf.at[yy, ic, PIECE[k, by], d * 16:d * 16 + 16, lo:hi]

    def span(kind, n):
        if kind == "u":
            return ubuf.at[0, 0, 0:n]
        lo, hi = SUBS[kind]
        return wbuf.at[0, 0, 0:n, :, lo:hi]

    def link_send(key, kind, r, axis, by):
        send(key, r, r, {axis: step(axis, by)}, ("links", kind))

    def piece_to_mate(kind, yo, k, by):
        r = piece(kind, YO[yo], k, by)
        send(("d", kind), r, r, mate, ("d", kind))

    def y_send(kind):
        for k in range(2):
            r = piece(kind, iy, k, 0)
            link_send(("y", kind), kind, r, AY, 1)
            link_send(("y", kind), kind, r, AY, -1)

    def pset(yo):
        return yo // 2

    def p_send(kind, k, yo):
        r = piece(kind, YO[yo], k, 0)
        link_send(("p", kind, pset(yo)), kind, r, RING[k], 1)
        link_send(("p", kind, pset(yo)), kind, r, RING[k], -1)

    def y_take(kind):
        arrived(("y", kind), span(kind, 4))
        for k in range(2):
            for d in range(2):
                half = half_piece(kind, YO[d], k, 0, d)
                link_send(("y2", kind), kind, half, AY, 1 if d == 0 else -1)
                p_send(kind, k, d)
        for k in range(2):
            for d in range(2):
                piece_to_mate(kind, d, k, 0)

    def y2_take(kind):
        arrived(("y2", kind), span(kind, 2))
        for k in range(2):
            p_send(kind, k, 2)
            piece_to_mate(kind, 2, k, 0)

    def p_take(kind, *yos):
        arrived(("p", kind, pset(yos[0])), span(kind, 4 * len(yos)))
        for yo in yos:
            for k in range(2):
                for d in range(2):
                    by = -1 if d == 0 else 1
                    half = half_piece(kind, YO[yo], k, by, d)
                    link_send(("p2", kind, pset(yo)), kind, half, RING[k], -by)
        for yo in yos:
            for k in range(2):
                for by in (-1, 1):
                    piece_to_mate(kind, yo, k, by)

    def p2_take(kind, *yos):
        arrived(("p2", kind, pset(yos[0])), span(kind, 2 * len(yos)))
        for yo in yos:
            for k in range(2):
                piece_to_mate(kind, yo, k, 2)

    def own_to_mate(kind):
        r = block_of(kind, iy, ic)
        send(("d", kind), r, r, mate, ("d", kind))

    def from_mate(kind):
        if kind == "u":
            arrived(("d", kind), ubuf.at[:, other])
        else:
            lo, hi = SUBS[kind]
            arrived(("d", kind), wbuf.at[:, other, :, :, lo:hi])

    def project(lo, hi):
        return nn(tokens[...], wbuf[:, :, :, :, lo:hi].reshape(2048, hi - lo))

    mark("gather")
    y_send(0)
    y_send("u")
    y_send(1)
    own_to_mate(0)
    g = gbuf.at[iy, ic]
    for n, by in enumerate((1, -1, 2)):
        send("g", g, g, {AY: step(AY, by)}, "g")
    send("gd", g, g, mate, "gd")
    own_to_mate("u")
    mark("y0")
    y_take(0)
    own_to_mate(1)
    mark("yu")
    y_take("u")
    y_send(2)
    own_to_mate(2)
    loads["tokens"].wait()
    mark("transpose")
    for z in range(2):
        tokt[z, :, :, :, 0:512] = tokens[:, z * 512:(z + 1) * 512].T.reshape(4, 4, 32, 512)
    mark("y20")
    y2_take(0)
    mark("p0a")
    p_take(0, 0, 1)
    mark("y1")
    y_take(1)
    mark("y2u")
    y2_take("u")
    mark("pua")
    p_take("u", 0, 1)
    mark("p0b")
    p_take(0, 2)
    mark("transpose")
    for z in range(2, 4):
        tokt[z, :, :, :, 0:512] = tokens[:, z * 512:(z + 1) * 512].T.reshape(4, 4, 32, 512)
    mark("y21")
    y2_take(1)
    mark("p1a")
    p_take(1, 0, 1)
    mark("pub")
    p_take("u", 2)
    mark("p20")
    p2_take(0, 0, 1)
    mark("y2")
    y_take(2)
    mark("p202")
    p2_take(0, 2)
    mark("p1b")
    p_take(1, 2)
    mark("y22")
    y2_take(2)
    mark("g")
    arrived("g", gbuf.at[0:3, 0])
    for by in (-1, 1, 2):
        gg = gbuf.at[step(AY, by), ic]
        send("gd", gg, gg, mate, "gd")
    mark("down")
    from_mate(0)
    acc[...] = project(*SUBS[0])
    mark("p2u")
    p2_take("u", 0, 1)
    p2_take("u", 2)
    mark("p2a")
    p_take(2, 0, 1)
    mark("p21")
    p2_take(1, 0, 1)
    p2_take(1, 2)
    mark("pre")
    arrived("gd", gbuf.at[:, other])

    for name in ("dout", "cos", "sin"):
        loads[name].wait()

    lane = lax.broadcasted_iota(jnp.int32, (1, 128), 1)
    low = lax.rem(lane, 64) < 32

    def swap(v):
        return jnp.where(low, pltpu.roll(v, 96, 1), pltpu.roll(v, 32, 1))

    def rot(v, sign):
        return v * cosr[...] + swap(v) * (sinr[...] * sign)

    gain = jnp.concatenate([gbuf[y, c, 0:1, 0:64] for y in range(4) for c in range(2)], 1)
    kr = rot(acc[:, 512:640], 1.0)
    krp[0] = jnp.where(lane < 64, kr, 0.0).astype(BF16)
    krp[1] = jnp.where(lane < 64, 0.0, pltpu.roll(kr, 64, 1)).astype(BF16)
    for n in range(4):
        rows = slice(n * 128, (n + 1) * 128)
        latent = acc[rows, 0:512]
        inv = lax.rsqrt(jnp.mean(latent * latent, axis=-1, keepdims=True) + EPSILON)
        unit = latent * inv
        acc[rows, 0:512] = unit
        invr[rows] = jnp.broadcast_to(inv, (128, 128))
        nrm[rows] = (unit * gain).astype(BF16)
    nrt[:, 0:512] = nrm[...].T
    send(("nrt",), nrt.at[:, 0:512], nrt.at[:, 512:1024], mate)
    ng[...] = jnp.zeros((512, 512), F32)
    dkr[...] = jnp.zeros((512, 128), F32)
    send("tok", tokt.at[:, :, :, :, 0:512], tokt.at[:, :, :, :, 512:1024], mate)
    mark("p2b")
    p_take(2, 2)
    mark("mateu")
    from_mate("u")
    mark("heads")

    tri = (lax.broadcasted_iota(jnp.int32, (256, 256), 0)
           <= lax.broadcasted_iota(jnp.int32, (256, 256), 1))

    def block(kf, v, qf, do):
        rows = kf.shape[0]
        s = nt(kf, qf) * SCALE
        masked = jnp.where(tri, s[rows - 256:], -1e30)
        s = masked if rows == 256 else jnp.concatenate([s[:rows - 256], masked], 0)
        w = jnp.exp(s - jnp.max(s, axis=0, keepdims=True))
        probs = w * (1.0 / jnp.sum(w, axis=0, keepdims=True))
        dp = nt(v, do)
        delta = jnp.sum(probs * dp, axis=0, keepdims=True)
        ds = (probs * (dp - delta) * SCALE).astype(BF16)
        return probs.astype(BF16), ds

    A0, A1, B = (0, 1, 2), (3, 4, 5), (6, 7, 8)
    def keep(u, z, cols, value):
        g = u % 3
        value = value.astype(BF16)
        if g == 0:
            part[u][z, :, :, :, cols] = value
        elif g == 1:
            part[u][:, z, :, :, cols] = value
        else:
            for x in range(4):
                part[u][:, z, x, :, cols] = value[x]

    def token_rows(z):
        return tokt[z].reshape(512, 1024)

    def products(slot):
        cols = slice(slot * 384, slot * 384 + 384)
        right = jnp.concatenate([jb[ic, :, cols], jp[:, cols]], 0)
        us = A1 if slot else A0
        for z in range(4):
            both = nn(token_rows(z), right).reshape(4, 4, 32, 384)
            for n, u in enumerate(us):
                keep(u, z, slice(0, 128), both[..., n * 128:n * 128 + 128])
        for u in us:
            ring_sends(1, u, part, rx, ra)

    def products_b():
        right = jnp.concatenate([
            jnp.concatenate([jb[ic, :, 768:1024], rg[ic]], 1),
            jnp.concatenate([jp[:, 768:1024], rgp[...]], 1)], 0)
        for z in range(4):
            both = nn(token_rows(z), right).reshape(4, 4, 32, 384)
            for u in (6, 7):
                keep(u, z, slice(0, 128), both[..., (u - 6) * 128:(u - 5) * 128])
            keep(8, z, slice(0, 128), both[..., 256:] + gmat[z])
        for u in (6, 7):
            up = nn(nrt[...], jnp.concatenate([kvg[ic, u - 6], kvgp[u - 6]], 0))
            up = up.reshape(64, 8, 512)
            up = jnp.concatenate([up[:, :, j * 128:(j + 1) * 128] for j in range(4)], 1)
            up = up.reshape(4, 4, 4, 32, 128)
            for z in range(4):
                keep(u, z, slice(128, 256), up[z])

    def ways(axis):
        return {axis: step(axis, 1)}, {axis: step(axis, -1)}

    def ring_sends(phase, u, p, r, a):
        axis = UNITS[u][phase]
        right, left_ = ways(axis)
        far, near, back = (p[u].at[step(axis, by)] for by in (2, 1, -1))
        send(("x", phase, u), far.at[0:2], r[u].at[0], right, ("s", phase, u))
        send(("x", phase, u), far.at[2:4], r[u].at[1], left_, ("s", phase, u))
        send(("a", phase, u), near.at[2:4], a[u].at[0, 2:4], right, ("s", phase, u))
        send(("a", phase, u), back.at[0:2], a[u].at[1, 0:2], left_, ("s", phase, u))

    def relay(phase, us, p, r, a):
        for u in us:
            axis = UNITS[u][phase]
            right, left_ = ways(axis)
            near, back = (p[u].at[step(axis, by)] for by in (1, -1))
            arrived(("x", phase, u), r[u])
            near[0:2] = (near[0:2].astype(F32) + r[u][0].astype(F32)).astype(BF16)
            back[2:4] = (back[2:4].astype(F32) + r[u][1].astype(F32)).astype(BF16)
            send(("a", phase, u), near.at[0:2], a[u].at[0, 0:2], right, ("s", phase, u))
            send(("a", phase, u), back.at[2:4], a[u].at[1, 2:4], left_, ("s", phase, u))

    def second(u, t):
        return own[u].at[:, t] if u % 3 == 1 else own[u].at[t]

    def second_sends(us):
        for u in us:
            arrived(("a", 1, u), ra[u])
            total = part[u][at[UNITS[u][1]]].astype(F32) + (ra[u][0].astype(F32) + ra[u][1].astype(F32))
            own[u][...] = total
            if u % 3 == 1:
                for z in range(4):
                    part2[u][:, z] = total[z].astype(BF16)
            else:
                part2[u][...] = total.astype(BF16)
            ring_sends(2, u, part2, rx2, ra2)

    def third_sends(us):
        for u in us:
            arrived(("a", 2, u), ra2[u])
            mine = second(u, at[UNITS[u][2]])
            mine[...] += ra2[u][0].astype(F32) + ra2[u][1].astype(F32)
            for slot, by in enumerate((2, 1, -1)):
                part3[u][slot] = mine[step(UNITS[u][3], by)].astype(BF16)
                send(("a", 3, u), part3[u].at[slot], ra3[u].at[slot],
                     {UNITS[u][3]: step(UNITS[u][3], by)}, ("s", 3, u))

    def last_sums(us):
        for u in us:
            arrived(("a", 3, u), ra3[u])
            mine = second(u, at[UNITS[u][2]])[at[UNITS[u][3]]]
            fin_ref[ic, :, GOFF[u]:GOFF[u] + UNITS[u][0]] = mine + (
                ra3[u][0].astype(F32) + ra3[u][1].astype(F32) + ra3[u][2].astype(F32))

    def queries(s):
        from_mate(s + 1)
        lo = SUBS[s + 1][0]
        q = project(lo, lo + 768)
        for m in range(2):
            n = 2 * s + m
            qnope[:, n * 256:(n + 1) * 256] = q[:, m * 384:m * 384 + 256].astype(BF16)
            rope = q[:, m * 384 + 256:m * 384 + 384].astype(BF16).astype(F32)
            qrope[:, n * 128:(n + 1) * 128] = rot(rope, 1.0).astype(BF16)

    def pair(n, carry):
        @pl.when(n == 0)
        def _():
            queries(0)

        @pl.when(n == 1)
        def _():
            p2_take(2, 0, 1)
            p2_take(2, 2)

        @pl.when(n == 2)
        def _():
            queries(1)
            arrived("tok", tokt.at[:, :, :, :, 512:1024])
            arrived("j0", jp.at[:, 0:384])
            products(0)

        half, m = lax.rem(n, 2), n // 2
        base = m * 384
        qr = qrope[:, pl.ds(pl.multiple_of(n * 128, 128), 128)]
        stage = []
        for e in range(2):
            h = 2 * n + e
            hc = pl.ds(pl.multiple_of(h * 128, 128), 128)
            u = ubuf[:, :, h].reshape(512, 256)
            kv = nn(nrm[...], u).astype(BF16)
            kf = jnp.concatenate([kv[:, :128], krp[e]], 1)
            v = kv[:, 128:]
            qf = jnp.concatenate([qnope[:, hc], qr], 1)
            do = dout[:, hc]
            stage.append((u, kf, v, qf, do))
        mids = []
        for u, kf, v, qf, do in stage:
            mids.append((block(kf[:256], v[:256], qf[:256], do[:256]), block(kf, v, qf[256:], do[256:])))
        total = None
        for e in range(2):
            u, kf, v, qf, do = stage[e]
            (pa, da), (pb, db) = mids[e]
            dv = nn(pb, do[256:])
            dv = jnp.concatenate([dv[:256] + nn(pa, do[:256]), dv[256:]], 0)
            dk = nn(db, qf[256:])
            dk = jnp.concatenate([dk[:256] + nn(da, qf[:256]), dk[256:]], 0)
            dq = jnp.concatenate([tn(da, kf[:256]), tn(db, kf)], 0)
            jb[half, :, pl.ds(pl.multiple_of(base + e * 128, 128), 128)] = dq[:, :128].astype(BF16)
            total = dq[:, 128:] if e == 0 else total + dq[:, 128:]
            keep_lanes = lane < 64 if e == 0 else lane >= 64
            dkr[...] += jnp.where(keep_lanes, dk[:, 128:], 0.0)
            kg = dk[:, :128].astype(BF16)
            vg = dv.astype(BF16)
            jc = pl.ds(pl.multiple_of((m * 2 + e) * 128, 128), 128)
            kvg[half, 0, :, jc] = kg
            kvg[half, 1, :, jc] = vg
            ng[...] += nt(jnp.concatenate([kg, vg], 1), u)
        jb[half, :, pl.ds(pl.multiple_of(base + 256, 128), 128)] = rot(total, -1.0).astype(BF16)

        @pl.when(n == 1)
        def _():
            send("j0", jb.at[other, :, 0:384], jp.at[:, 0:384], mate, "j0")

        return carry

    lax.fori_loop(0, 4, pair, 0)
    mark("post")
    send("j1", jb.at[other, :, 384:768], jp.at[:, 384:768], mate)
    relay(1, A0, part, rx, ra)

    gterm = jnp.zeros((1, 512), F32)
    for n in range(4):
        rows = slice(n * 128, (n + 1) * 128)
        unit = acc[rows, 0:512]
        grad = ng[rows]
        gterm = gterm + jnp.sum(grad * unit, axis=0, keepdims=True)
        scaled = grad * gain
        inner = jnp.mean(scaled * unit, axis=-1, keepdims=True)
        value = (invr[rows, 0:1] * (scaled - unit * inner)).astype(BF16)
        jb[0, rows, 768:1024] = value[:, :256]
        jb[1, rows, 768:1024] = value[:, 256:]
    dk = dkr[...]
    rope = jnp.where(lane < 64, rot(dk + pltpu.roll(dk, 64, 1), -1.0), 0.0)
    rgf[...] = rope.astype(BF16)
    rg[0] = jnp.where(lane < 32, rope, 0.0).astype(BF16)
    rg[1] = jnp.where(lane < 32, pltpu.roll(rope, 96, 1), 0.0).astype(BF16)
    send(("kvg",), kvg.at[other], kvgp, mate)
    send(("jl",), jb.at[other, :, 768:1024], jp.at[:, 768:1024], mate)
    send(("rg",), rg.at[other], rgp, mate)
    column = jnp.broadcast_to(gterm, (128, 512)).T
    column = jnp.where(lane == 32, column, 0.0).reshape(64, 8, 128)
    gmat[...] = jnp.concatenate([column, jnp.zeros((64, 24, 128), F32)], 1).reshape(4, 4, 4, 32, 128)

    tgd = []

    def token_block():
        n = len(tgd)
        w = wbuf[n].reshape(512, WCOL)
        cols = [jb[0, :, 768:], jb[1, :, 768:], rgf[...]]
        cols += [jb[m % 2, :, m // 2 * 384:m // 2 * 384 + 384] for m in range(4)]
        tgb[n] = nt(jnp.concatenate(cols, 1), w).astype(BF16)
        d = pltpu.make_async_copy(tgb.at[n], tg_hbm.at[:, n * 512:(n + 1) * 512], lsem.at[9])
        d.start()
        tgd.append(d)

    mark("waitmate")
    arrived(("nrt",), nrt.at[:, 512:1024])
    arrived("j1", jp.at[:, 384:768])
    mark("firstA1")
    products(1)
    mark("secondA0")
    second_sends(A0)
    arrived(("kvg",), kvgp)
    arrived(("jl",), jp.at[:, 768:1024])
    arrived(("rg",), rgp)
    mark("productsB")
    products_b()
    for u in B:
        ring_sends(1, u, part, rx, ra)
    mark("relayA1")
    relay(1, A1, part, rx, ra)
    mark("relay2A0")
    relay(2, A0, part2, rx2, ra2)
    mark("tg")
    token_block()
    token_block()
    token_block()
    mark("relayB")
    relay(1, B, part, rx, ra)
    mark("tg")
    token_block()
    mark("thirdA0")
    third_sends(A0)
    mark("secondA1")
    second_sends(A1)
    mark("secondB")
    second_sends(B)
    mark("relay2A1")
    relay(2, A1, part2, rx2, ra2)
    mark("relay2B")
    relay(2, B, part2, rx2, ra2)
    mark("thirdA1")
    third_sends(A1)
    mark("thirdB")
    third_sends(B)
    mark("lastA0")
    last_sums(A0)
    mark("lastA1")
    last_sums(A1)
    send(("fin", 0), fin_ref.at[ic, :, 0:768], fin_ref.at[ic, :, 0:768], mate)
    mark("lastB")
    last_sums(B)
    send(("fin", 1), fin_ref.at[ic, :, 768:GTOT], fin_ref.at[ic, :, 768:GTOT], mate)
    mark("fin")
    arrived(("fin", 0), fin_ref.at[other, :, 0:768])
    arrived(("fin", 1), fin_ref.at[other, :, 768:GTOT])

    both = fin_ref[...]
    tail = GTOT - 128
    gains = both[0, :, tail:] + both[1, :, tail:]
    body = both[:, :, :tail]
    squares = jnp.sum(jnp.sum(body * body, axis=0), axis=0, keepdims=True)
    row = sum(squares[:, n * 128:(n + 1) * 128] for n in range(10))
    ropes = jnp.where(lane == 32, 0.0, both[0, :, tail:] ** 2 + both[1, :, tail:] ** 2)
    ropes = ropes + jnp.where(lane == 32, gains * gains, 0.0)
    row = row + jnp.sum(ropes, axis=0, keepdims=True)
    row = jnp.broadcast_to(row, (8, 128))
    mark("norm")
    lead = ic == 1
    for n, axis in enumerate((AY, AX, AZ)):
        @pl.when(lead)
        def _():
            nbuf[n, 3] = row if n == 0 else (nbuf[n - 1, 0] + nbuf[n - 1, 1]) + (nbuf[n - 1, 2] + nbuf[n - 1, 3])
            for m, by in enumerate((1, -1, 2)):
                send(("n", n), nbuf.at[n, 3], nbuf.at[n, m], {axis: step(axis, by)}, ("n", n))

        @pl.when(lead)
        def _():
            arrived(("n", n), nbuf.at[n, 0:3])

    @pl.when(lead)
    def _():
        nbuf[3, 0] = (nbuf[2, 0] + nbuf[2, 1]) + (nbuf[2, 2] + nbuf[2, 3])
        send("nd", nbuf.at[3, 0], nbuf.at[3, 0], mate, "nd")
        for n in range(3):
            left(("n", n), nbuf.at[n, 0:3])
        left("nd", nbuf.at[3, 0])

    @pl.when(jnp.logical_not(lead))
    def _():
        arrived("nd", nbuf.at[3, 0])

    total = jnp.sum(nbuf[3, 0], axis=-1, keepdims=True)
    clip = jnp.minimum(1.0, lax.rsqrt(total / NPARAM + 1e-06))
    clip_ref[...] = jnp.broadcast_to(clip, (8, 128))

    mark("drain")
    for key, ref in owed:
        left(key, ref)
    left("j0", jb.at[0, :, 0:384])
    left("g", gbuf.at[0:3, 0])
    left("gd", gbuf.at[:, 0])
    for kind in KINDS:
        if kind == "u":
            left(("links", kind), ubuf.at[0:3, 0])
            left(("d", kind), ubuf.at[:, 0])
        else:
            lo, hi = SUBS[kind]
            left(("links", kind), wbuf.at[0:3, 0, :, :, lo:hi])
            left(("d", kind), wbuf.at[:, 0, :, :, lo:hi])
    for u in range(nu):
        left(("s", 1, u), part[u].at[0:3])
        left(("s", 2, u), part2[u].at[0:3])
        left(("s", 3, u), part3[u])
    pltpu.make_async_copy(tgb, tgb, lsem.at[9]).wait()
    mark(None)
    assert len(recv_table) == NRECV and len(send_table) == NSEND, (len(recv_table), len(send_table))


NRECV = 88
NSEND = 50


def scratch():
    v = pltpu.VMEM
    dma = pltpu.SemaphoreType.DMA
    shapes = [
        v((512, 2048), BF16), v((512, 1024), BF16), v((512, 128), F32), v((512, 128), F32),
        v((4, 2, 8, 32, WCOL), BF16), v((4, 2, 8, 64, 256), BF16), v((4, 2, 8, 128), F32),
        v((4, 4, 4, 32, 1024), BF16), v((512, 640), F32),
        v((512, 512), BF16), v((512, 1024), BF16), v((512, 512), BF16), v((512, 1024), BF16),
        v((512, 512), F32), v((2, 512, 128), BF16), v((512, 128), F32),
        v((2, 512, 1024), BF16), v((512, 1024), BF16), v((2, 2, 512, 512), BF16), v((2, 512, 512), BF16),
        v((2, 512, 128), BF16), v((512, 128), BF16), v((512, 128), BF16), v((512, 128), F32),
        v((4, 4, 4, 32, 128), F32), v((4, 512, 512), BF16), v((4, 4, 8, 128), F32),
        v((256, 1536), BF16), v((576, 256), BF16), v((1, 64), BF16),
        dma((10,)), dma((NSEND,)), dma((NRECV,)),
    ]
    ws = [w for w, *_ in UNITS]
    shapes += [v((4, 4, 4, 32, w), BF16) for w in ws]
    shapes += [v((4, 4, 32, w), F32) for w in ws]
    shapes += [v((2, 2, 4, 32, w), BF16) for w in ws]
    shapes += [v((2, 4, 4, 32, w), BF16) for w in ws]
    shapes += [v((4, 4, 32, w), BF16) for w in ws]
    shapes += [v((2, 2, 32, w), BF16) for w in ws]
    shapes += [v((2, 4, 32, w), BF16) for w in ws]
    shapes += [v((3, 32, w), BF16) for w in ws]
    shapes += [v((3, 32, w), BF16) for w in ws]
    return shapes


def last_step(fin_hbm, clip_hbm, tg_in, gq_ref, gd_ref, gu_ref, gg_ref, tg_out,
              fin_ref, clip_ref, stage, isem, osem):
    ic = lax.axis_index(AC)
    first_reads = []
    for n, (src, dst) in enumerate(((fin_hbm, fin_ref), (clip_hbm, clip_ref))):
        d = pltpu.make_async_copy(src, dst, isem.at[4 + n])
        d.start()
        first_reads.append(d)
    reads = []
    for n in range(4):
        rows = slice(n * 128, (n + 1) * 128)
        d = pltpu.make_async_copy(tg_in.at[rows], stage.at[n], isem.at[n])
        d.start()
        reads.append(d)
    writes = []
    for n in range(4):
        rows_n = slice(n * 128, (n + 1) * 128)
        reads[n].wait()
        d = pltpu.make_async_copy(stage.at[n], tg_out.at[rows_n], osem.at[n])
        d.start()
        writes.append(d)
    for d in first_reads:
        d.wait()
    clip = clip_ref[0:1, 0:1]
    first = ic == 0

    def rows(half, cols):
        return jnp.where(first, fin_ref[half, 0:16, cols], fin_ref[half, 16:32, cols]) * clip

    def cols(lo):
        return slice(lo, lo + 128)

    for n in range(4):
        half, lo = n % 2, n // 2 * 384
        rope = rows(half, cols(lo + 256))
        gq_ref[:, n * 384:(n + 1) * 384] = jnp.concatenate(
            [rows(half, cols(lo)), rope[:, :64], rows(half, cols(lo + 128)), rope[:, 64:]], 1)
        gd_ref[:, n * 128:(n + 1) * 128] = rows(n // 2, cols(768 + n % 2 * 256))
    tail = slice(GTOT - 128, GTOT)
    gd_ref[:, 512:576] = jnp.concatenate([rows(0, tail)[:, :32], rows(1, tail)[:, :32]], 1)
    for h in range(H):
        half, j = h // 2 % 2, h // 4 * 2 + h % 2
        for u in range(2):
            block = fin_ref[half, j * 8:j * 8 + 8, cols(896 + u * 256)] * clip
            gu_ref[:, h * 256 + u * 128:h * 256 + u * 128 + 128] = jnp.where(first, block[0:4], block[4:8])
    gain = (fin_ref[0, 0:8, tail] + fin_ref[1, 0:8, tail]) * clip
    gain = jnp.where(first, gain[0:4], gain[4:8])
    spread = (lax.broadcasted_iota(jnp.int32, (4, 128), 0)
              == lax.broadcasted_iota(jnp.int32, (4, 128), 1))
    gg_ref[...] = jnp.sum(jnp.where(spread, gain[:, 32:33], 0.0), axis=0)[0:4]
    for d in writes:
        d.wait()


def finish(fin, clip, token_grad):
    vm = pl.BlockSpec(memory_space=pltpu.VMEM)
    anyspace = pl.BlockSpec(memory_space=pl.ANY)
    return pl.pallas_call(
        last_step,
        out_shape=(
            jax.ShapeDtypeStruct((16, 1536), F32),
            jax.ShapeDtypeStruct((16, 576), F32),
            jax.ShapeDtypeStruct((4, 2048), F32),
            jax.ShapeDtypeStruct((4,), F32),
            jax.ShapeDtypeStruct((SEQ, D), BF16),
        ),
        in_specs=[anyspace] * 3,
        out_specs=(vm, vm, vm, vm, anyspace),
        scratch_shapes=[
            pltpu.VMEM((2, 32, GTOT), F32), pltpu.VMEM((8, 128), F32),
            pltpu.VMEM((4, 128, D), BF16), pltpu.SemaphoreType.DMA((6,)), pltpu.SemaphoreType.DMA((4,))],
    )(fin, clip, token_grad)


def per_device(tokens, d_out, w_query, w_down, w_up, latent_gain):
    cosine, sine = rope_constants()
    vm = pl.BlockSpec(memory_space=pltpu.VMEM)
    anyspace = pl.BlockSpec(memory_space=pl.ANY)
    fin, clip, token_grad = pl.pallas_call(
        mega,
        out_shape=(
            jax.ShapeDtypeStruct((2, 32, GTOT), F32),
            jax.ShapeDtypeStruct((8, 128), F32),
            jax.ShapeDtypeStruct((SEQ, D), BF16),
        ),
        in_specs=[anyspace] * 8,
        out_specs=(vm, vm, anyspace),
        scratch_shapes=scratch(),
        compiler_params=pltpu.CompilerParams(
            collective_id=0, has_side_effects=True, vmem_limit_bytes=67043328),
    )(tokens, d_out, jnp.asarray(cosine), jnp.asarray(sine), w_query, w_down.T, w_up,
      latent_gain.reshape(1, 64))
    return finish(fin, clip, token_grad)


def solution(mesh):
    split = Mesh(mesh.devices.reshape(4, 4, 4, 2), NODE_LOCAL)
    return jax.shard_map(
        per_device,
        mesh=split,
        in_specs=(
            P(NODE_LOCAL, None),
            P(NODE_LOCAL, None),
            P(LOCAL, None),
            P(LOCAL, None),
            P(LOCAL, None),
            P(LOCAL),
        ),
        out_specs=(
            P(NODE_LOCAL, None),
            P(NODE_LOCAL, None),
            P(NODE_LOCAL, None),
            P(NODE_LOCAL),
            P(NODE_LOCAL, None),
        ),
        check_vma=False,
    )
```

```python
import math

import jax
import jax.numpy as jnp
import numpy as np
from jax import lax
from jax.experimental import pallas as pl
from jax.experimental.pallas import tpu as pltpu
from jax.sharding import Mesh
from jax.sharding import PartitionSpec as P

H = 8
DN = 128
DR = 64
DV = 128
KVL = 512
SEQ = 512
D = 2048
NPARAM = 5374464
EPSILON = 1e-06
ROPE_BASE = 10000.0
LOCAL = ("local_0", "local_1")
NODE_LOCAL = ("node_0", "node_1", "local_0", "local_1")
MESH = pl.DeviceIdType.MESH
AZ, AX, AY, AC = NODE_LOCAL

WCOL = 2176
SUBS = ((0, 640), (640, 1408), (1408, 2176))
SCALE = 1.0 / math.sqrt(DN + DR)
AXES = ((AZ, AX, AY), (AX, AY, AZ), (AY, AZ, AX))
GRP = (0, 1, 2, 0, 1, 2, 0, 1, 0, 1, 2)
UNITS = tuple((128,) + AXES[g] for g in GRP)
GOFF = tuple(128 * n for n in range(len(GRP)))
GTOT = 1408
F32 = jnp.float32
BF16 = jnp.bfloat16


def rope_constants():
    position = np.arange(SEQ, dtype=np.float32)[:, None]
    freq = np.float32(ROPE_BASE) ** (-np.arange(DR // 2, dtype=np.float32) * np.float32(2.0 / DR))
    angle = (position * freq[None, :].astype(np.float32)).astype(np.float32)
    cosine = np.cos(angle).astype(np.float32)
    sine = np.sin(angle).astype(np.float32)
    return np.concatenate([cosine] * 4, 1), np.concatenate([-sine, sine] * 2, 1)


def nt(a, b):
    return lax.dot_general(a, b, (((1,), (1,)), ((), ())), preferred_element_type=F32)


def nn(a, b):
    return jnp.dot(a, b, preferred_element_type=F32)


def tn(a, b):
    return lax.dot_general(a, b, (((0,), (0,)), ((), ())), preferred_element_type=F32)


def mega(
    tokens_hbm, dout_hbm, cos_hbm, sin_hbm, wq_hbm, wd_hbm, wu_hbm, gain_hbm,
    fin_ref, clip_ref, tg_hbm,
    tokens, dout, cosr, sinr, wbuf, ubuf, gbuf, tokt, acc, qrope, qnope, nrm, nrt, ng, krp, dkr,
    jb, jp, kvg, kvgp, rg, rgp, rgf, invr, gmat, tgb, nbuf, wq_ref, wd_ref, gain_ref, lsem, ssem, rsem, *rest,
):
    nu = len(UNITS)
    part, own, rx, ra, part2, rx2, ra2, part3, ra3 = (rest[n * nu:(n + 1) * nu] for n in range(9))
    iz, ix, iy, ic = (lax.axis_index(a) for a in NODE_LOCAL)
    at = {AZ: iz, AX: ix, AY: iy}
    other = 1 - ic
    STEP = {(a, by): lax.rem(at[a] + (by + 4), 4) for a in at for by in (-1, 0, 1, 2)}

    def step(axis, by):
        return STEP[axis, by]

    recv_table, send_table, owed = {}, {}, []
    scope = []

    def mark(name):
        while scope:
            scope.pop().__exit__(None, None, None)
        if name:
            scope.append(jax.named_scope(name))
            scope[-1].__enter__()

    mark("start")

    def index(table, key):
        return table.setdefault(key, len(table))

    def send(key, src, dst, peer, outgoing=None):
        if outgoing is None:
            outgoing = key
            owed.append((key, src))
        pltpu.make_async_remote_copy(
            src_ref=src, dst_ref=dst,
            send_sem=ssem.at[index(send_table, outgoing)], recv_sem=rsem.at[index(recv_table, key)],
            device_id=peer, device_id_type=MESH).start()

    def arrived(key, ref):
        pltpu.make_async_remote_copy(
            src_ref=ref, dst_ref=ref, send_sem=ssem.at[0], recv_sem=rsem.at[index(recv_table, key)],
            device_id=mate, device_id_type=MESH).wait_recv()

    def left(key, ref):
        pltpu.make_async_remote_copy(
            src_ref=ref, dst_ref=ref, send_sem=ssem.at[index(send_table, key)], recv_sem=rsem.at[0],
            device_id=mate, device_id_type=MESH).wait_send()

    mate = {AC: other}
    barrier = pltpu.get_barrier_semaphore()
    for axis in (AZ, AX, AY):
        for by in (1, -1, 2):
            pl.semaphore_signal(barrier, inc=1, device_id={axis: step(axis, by)}, device_id_type=MESH)
    pl.semaphore_signal(barrier, inc=1, device_id=mate, device_id_type=MESH)

    loads = {}

    def load(name, src, dst):
        d = pltpu.make_async_copy(src, dst, lsem.at[len(loads)])
        d.start()
        loads[name] = d

    for p in range(8):
        pltpu.make_async_copy(wu_hbm.at[:, p * 256:(p + 1) * 256], ubuf.at[iy, ic, p], lsem.at[8]).start()

    load("down", wd_hbm, wd_ref)
    load("query", wq_hbm, wq_ref)
    load("gain", gain_hbm, gain_ref)
    load("tokens", tokens_hbm, tokens)
    load("dout", dout_hbm, dout)
    load("cos", cos_hbm, cosr)
    load("sin", sin_hbm, sinr)

    loads["down"].wait()
    down = jnp.concatenate([wd_ref[...], jnp.zeros((64, 256), BF16)], 0)
    wbuf[iy, ic, :, :, 0:640] = down.T.reshape(8, 32, 640)
    loads["query"].wait()
    for n in range(4):
        lo = 640 + n * 384
        h = n * 384
        both = jnp.concatenate([
            wq_ref[:, h:h + 128], wq_ref[:, h + 192:h + 320],
            wq_ref[:, h + 128:h + 192], wq_ref[:, h + 320:h + 384]], 1)
        wbuf[iy, ic, :, :, lo:lo + 384] = both.reshape(8, 32, 384)
    loads["gain"].wait()
    gbuf[iy, ic] = jnp.broadcast_to(
        jnp.concatenate([gain_ref[...].astype(F32), jnp.zeros((1, 64), F32)], 1), (8, 128))
    own_up = ubuf.at[iy, ic]
    pltpu.make_async_copy(own_up, own_up, lsem.at[8]).wait()
    pl.semaphore_wait(barrier, 10)

    RING = (AX, AZ)
    YO = (step(AY, -1), step(AY, 1), step(AY, 2))
    PIECE = {(k, by): k * 4 + step(RING[k], by) for k in range(2) for by in (-1, 0, 1, 2)}
    KINDS = (0, "u", 1, 2)

    def block_of(kind, yy, core):
        if kind == "u":
            return ubuf.at[yy, core]
        lo, hi = SUBS[kind]
        return wbuf.at[yy, core, :, :, lo:hi]

    def piece(kind, yy, k, by):
        if kind == "u":
            return ubuf.at[yy, ic, PIECE[k, by]]
        lo, hi = SUBS[kind]
        return wbuf.at[yy, ic, PIECE[k, by], :, lo:hi]

    def half_piece(kind, yy, k, by, d):
        if kind == "u":
            return ubuf.at[yy, ic, PIECE[k, by], d * 32:d * 32 + 32]
        lo, hi = SUBS[kind]
        return wbuf.at[yy, ic, PIECE[k, by], d * 16:d * 16 + 16, lo:hi]

    def span(kind, n):
        if kind == "u":
            return ubuf.at[0, 0, 0:n]
        lo, hi = SUBS[kind]
        return wbuf.at[0, 0, 0:n, :, lo:hi]

    def link_send(key, kind, r, axis, by):
        send(key, r, r, {axis: step(axis, by)}, ("links", kind))

    def piece_to_mate(kind, yo, k, by):
        r = piece(kind, YO[yo], k, by)
        send(("d", kind), r, r, mate, ("d", kind))

    def y_send(kind):
        for k in range(2):
            r = piece(kind, iy, k, 0)
            link_send(("y", kind), kind, r, AY, 1)
            link_send(("y", kind), kind, r, AY, -1)

    def pset(yo):
        return yo // 2

    def p_send(kind, k, yo):
        r = piece(kind, YO[yo], k, 0)
        link_send(("p", kind, pset(yo)), kind, r, RING[k], 1)
        link_send(("p", kind, pset(yo)), kind, r, RING[k], -1)

    def y_take(kind):
        arrived(("y", kind), span(kind, 4))
        for k in range(2):
            for d in range(2):
                half = half_piece(kind, YO[d], k, 0, d)
                link_send(("y2", kind), kind, half, AY, 1 if d == 0 else -1)
                p_send(kind, k, d)
        for k in range(2):
            for d in range(2):
                piece_to_mate(kind, d, k, 0)

    def y2_take(kind):
        arrived(("y2", kind), span(kind, 2))
        for k in range(2):
            p_send(kind, k, 2)
            piece_to_mate(kind, 2, k, 0)

    def p_take(kind, *yos):
        arrived(("p", kind, pset(yos[0])), span(kind, 4 * len(yos)))
        for yo in yos:
            for k in range(2):
                for d in range(2):
                    by = -1 if d == 0 else 1
                    half = half_piece(kind, YO[yo], k, by, d)
                    link_send(("p2", kind, pset(yo)), kind, half, RING[k], -by)
        for yo in yos:
            for k in range(2):
                for by in (-1, 1):
                    piece_to_mate(kind, yo, k, by)

    def p2_take(kind, *yos):
        arrived(("p2", kind, pset(yos[0])), span(kind, 2 * len(yos)))
        for yo in yos:
            for k in range(2):
                piece_to_mate(kind, yo, k, 2)

    def own_to_mate(kind):
        r = block_of(kind, iy, ic)
        send(("d", kind), r, r, mate, ("d", kind))

    def from_mate(kind):
        if kind == "u":
            arrived(("d", kind), ubuf.at[:, other])
        else:
            lo, hi = SUBS[kind]
            arrived(("d", kind), wbuf.at[:, other, :, :, lo:hi])

    def project(lo, hi):
        return nn(tokens[...], wbuf[:, :, :, :, lo:hi].reshape(2048, hi - lo))

    mark("gather")
    y_send(0)
    y_send("u")
    y_send(1)
    own_to_mate(0)
    g = gbuf.at[iy, ic]
    for n, by in enumerate((1, -1, 2)):
        send("g", g, g, {AY: step(AY, by)}, "g")
    send("gd", g, g, mate, "gd")
    own_to_mate("u")
    mark("y0")
    y_take(0)
    own_to_mate(1)
    mark("yu")
    y_take("u")
    y_send(2)
    own_to_mate(2)
    loads["tokens"].wait()
    mark("transpose")
    for z in range(2):
        tokt[z, :, :, :, 0:512] = tokens[:, z * 512:(z + 1) * 512].T.reshape(4, 4, 32, 512)
    mark("y20")
    y2_take(0)
    mark("p0a")
    p_take(0, 0, 1)
    mark("y1")
    y_take(1)
    mark("y2u")
    y2_take("u")
    mark("pua")
    p_take("u", 0, 1)
    mark("p0b")
    p_take(0, 2)
    mark("transpose")
    for z in range(2, 4):
        tokt[z, :, :, :, 0:512] = tokens[:, z * 512:(z + 1) * 512].T.reshape(4, 4, 32, 512)
    mark("y21")
    y2_take(1)
    mark("p1a")
    p_take(1, 0, 1)
    mark("pub")
    p_take("u", 2)
    mark("p20")
    p2_take(0, 0, 1)
    mark("y2")
    y_take(2)
    mark("p202")
    p2_take(0, 2)
    mark("p1b")
    p_take(1, 2)
    mark("y22")
    y2_take(2)
    mark("g")
    arrived("g", gbuf.at[0:3, 0])
    for by in (-1, 1, 2):
        gg = gbuf.at[step(AY, by), ic]
        send("gd", gg, gg, mate, "gd")
    mark("down")
    from_mate(0)
    acc[...] = project(*SUBS[0])
    mark("p2u")
    p2_take("u", 0, 1)
    p2_take("u", 2)
    mark("p2a")
    p_take(2, 0, 1)
    mark("p21")
    p2_take(1, 0, 1)
    p2_take(1, 2)
    mark("pre")
    arrived("gd", gbuf.at[:, other])

    for name in ("dout", "cos", "sin"):
        loads[name].wait()

    lane = lax.broadcasted_iota(jnp.int32, (1, 128), 1)
    low = lax.rem(lane, 64) < 32

    def swap(v):
        return jnp.where(low, pltpu.roll(v, 96, 1), pltpu.roll(v, 32, 1))

    def rot(v, sign):
        return v * cosr[...] + swap(v) * (sinr[...] * sign)

    gain = jnp.concatenate([gbuf[y, c, 0:1, 0:64] for y in range(4) for c in range(2)], 1)
    kr = rot(acc[:, 512:640], 1.0)
    krp[0] = jnp.where(lane < 64, kr, 0.0).astype(BF16)
    krp[1] = jnp.where(lane < 64, 0.0, pltpu.roll(kr, 64, 1)).astype(BF16)
    for n in range(4):
        rows = slice(n * 128, (n + 1) * 128)
        latent = acc[rows, 0:512]
        inv = lax.rsqrt(jnp.mean(latent * latent, axis=-1, keepdims=True) + EPSILON)
        unit = latent * inv
        acc[rows, 0:512] = unit
        invr[rows] = jnp.broadcast_to(inv, (128, 128))
        nrm[rows] = (unit * gain).astype(BF16)
    nrt[:, 0:512] = nrm[...].T
    send(("nrt",), nrt.at[:, 0:512], nrt.at[:, 512:1024], mate)
    ng[...] = jnp.zeros((512, 512), F32)
    dkr[...] = jnp.zeros((512, 128), F32)
    send("tok", tokt.at[:, :, :, :, 0:512], tokt.at[:, :, :, :, 512:1024], mate)
    mark("p2b")
    p_take(2, 2)
    mark("mateu")
    from_mate("u")
    mark("heads")

    tri = (lax.broadcasted_iota(jnp.int32, (256, 256), 0)
           <= lax.broadcasted_iota(jnp.int32, (256, 256), 1))

    def block(kf, v, qf, do):
        rows = kf.shape[0]
        s = nt(kf, qf) * SCALE
        masked = jnp.where(tri, s[rows - 256:], -1e30)
        s = masked if rows == 256 else jnp.concatenate([s[:rows - 256], masked], 0)
        w = jnp.exp(s - jnp.max(s, axis=0, keepdims=True))
        probs = w * (1.0 / jnp.sum(w, axis=0, keepdims=True))
        dp = nt(v, do)
        delta = jnp.sum(probs * dp, axis=0, keepdims=True)
        ds = (probs * (dp - delta) * SCALE).astype(BF16)
        return probs.astype(BF16), ds

    A0, A1, U, B = (0, 1, 2), (3, 4, 5), (6, 7), (8, 9, 10)
    def keep(u, z, cols, value):
        g = GRP[u]
        value = value.astype(BF16)
        if g == 0:
            part[u][z, :, :, :, cols] = value
        elif g == 1:
            part[u][:, z, :, :, cols] = value
        else:
            for x in range(4):
                part[u][:, z, x, :, cols] = value[x]

    def token_rows(z):
        return tokt[z].reshape(512, 1024)

    def products(slot):
        cols = slice(slot * 384, slot * 384 + 384)
        right = jnp.concatenate([jb[ic, :, cols], jp[:, cols]], 0)
        us = A1 if slot else A0
        for z in range(4):
            both = nn(token_rows(z), right).reshape(4, 4, 32, 384)
            for n, u in enumerate(us):
                keep(u, z, slice(0, 128), both[..., n * 128:n * 128 + 128])
        for u in us:
            ring_sends(1, u, part, rx, ra)

    def products_b():
        right = jnp.concatenate([
            jnp.concatenate([jb[ic, :, 768:1024], rg[ic]], 1),
            jnp.concatenate([jp[:, 768:1024], rgp[...]], 1)], 0)
        for z in range(4):
            both = nn(token_rows(z), right).reshape(4, 4, 32, 384)
            for u in (8, 9):
                keep(u, z, slice(0, 128), both[..., (u - 8) * 128:(u - 7) * 128])
            keep(10, z, slice(0, 128), both[..., 256:] + gmat[z])
        for u in B:
            ring_sends(1, u, part, rx, ra)

    def products_u():
        for u in U:
            up = nn(nrt[...], jnp.concatenate([kvg[ic, u - 6], kvgp[u - 6]], 0))
            up = up.reshape(64, 8, 512)
            up = jnp.concatenate([up[:, :, j * 128:(j + 1) * 128] for j in range(4)], 1)
            up = up.reshape(4, 4, 4, 32, 128)
            for z in range(4):
                keep(u, z, slice(0, 128), up[z])
            ring_sends(1, u, part, rx, ra)

    def ways(axis):
        return {axis: step(axis, 1)}, {axis: step(axis, -1)}

    def ring_sends(phase, u, p, r, a):
        axis = UNITS[u][phase]
        right, left_ = ways(axis)
        far, near, back = (p[u].at[step(axis, by)] for by in (2, 1, -1))
        send(("x", phase, u), far.at[0:2], r[u].at[0], right, ("s", phase, u))
        send(("x", phase, u), far.at[2:4], r[u].at[1], left_, ("s", phase, u))
        send(("a", phase, u), near.at[2:4], a[u].at[0, 2:4], right, ("s", phase, u))
        send(("a", phase, u), back.at[0:2], a[u].at[1, 0:2], left_, ("s", phase, u))

    def relay(phase, us, p, r, a):
        for u in us:
            axis = UNITS[u][phase]
            right, left_ = ways(axis)
            near, back = (p[u].at[step(axis, by)] for by in (1, -1))
            arrived(("x", phase, u), r[u])
            near[0:2] = (near[0:2].astype(F32) + r[u][0].astype(F32)).astype(BF16)
            back[2:4] = (back[2:4].astype(F32) + r[u][1].astype(F32)).astype(BF16)
            send(("a", phase, u), near.at[0:2], a[u].at[0, 0:2], right, ("s", phase, u))
            send(("a", phase, u), back.at[2:4], a[u].at[1, 2:4], left_, ("s", phase, u))

    def second(u, t):
        return own[u].at[:, t] if GRP[u] == 1 else own[u].at[t]

    def second_sends(us):
        for u in us:
            arrived(("a", 1, u), ra[u])
            total = part[u][at[UNITS[u][1]]].astype(F32) + (ra[u][0].astype(F32) + ra[u][1].astype(F32))
            own[u][...] = total
            if GRP[u] == 1:
                for z in range(4):
                    part2[u][:, z] = total[z].astype(BF16)
            else:
                part2[u][...] = total.astype(BF16)
            ring_sends(2, u, part2, rx2, ra2)

    def third_sends(us):
        for u in us:
            arrived(("a", 2, u), ra2[u])
            mine = second(u, at[UNITS[u][2]])
            mine[...] += ra2[u][0].astype(F32) + ra2[u][1].astype(F32)
            for slot, by in enumerate((2, 1, -1)):
                part3[u][slot] = mine[step(UNITS[u][3], by)].astype(BF16)
                send(("a", 3, u), part3[u].at[slot], ra3[u].at[slot],
                     {UNITS[u][3]: step(UNITS[u][3], by)}, ("s", 3, u))

    def last_sums(us):
        for u in us:
            arrived(("a", 3, u), ra3[u])
            mine = second(u, at[UNITS[u][2]])[at[UNITS[u][3]]]
            fin_ref[ic, :, GOFF[u]:GOFF[u] + UNITS[u][0]] = mine + (
                ra3[u][0].astype(F32) + ra3[u][1].astype(F32) + ra3[u][2].astype(F32))

    def queries(s):
        from_mate(s + 1)
        lo = SUBS[s + 1][0]
        q = project(lo, lo + 768)
        for m in range(2):
            n = 2 * s + m
            qnope[:, n * 256:(n + 1) * 256] = q[:, m * 384:m * 384 + 256].astype(BF16)
            rope = q[:, m * 384 + 256:m * 384 + 384].astype(BF16).astype(F32)
            qrope[:, n * 128:(n + 1) * 128] = rot(rope, 1.0).astype(BF16)

    def pair(n, carry):
        @pl.when(n == 0)
        def _():
            queries(0)

        @pl.when(n == 1)
        def _():
            p2_take(2, 0, 1)
            p2_take(2, 2)

        @pl.when(n == 2)
        def _():
            queries(1)
            arrived("tok", tokt.at[:, :, :, :, 512:1024])
            arrived("j0", jp.at[:, 0:384])
            products(0)

        half, m = lax.rem(n, 2), n // 2
        base = m * 384
        qr = qrope[:, pl.ds(pl.multiple_of(n * 128, 128), 128)]
        stage = []
        for e in range(2):
            h = 2 * n + e
            hc = pl.ds(pl.multiple_of(h * 128, 128), 128)
            u = ubuf[:, :, h].reshape(512, 256)
            kv = nn(nrm[...], u).astype(BF16)
            kf = jnp.concatenate([kv[:, :128], krp[e]], 1)
            v = kv[:, 128:]
            qf = jnp.concatenate([qnope[:, hc], qr], 1)
            do = dout[:, hc]
            stage.append((u, kf, v, qf, do))
        mids = []
        for u, kf, v, qf, do in stage:
            mids.append((block(kf[:256], v[:256], qf[:256], do[:256]), block(kf, v, qf[256:], do[256:])))
        total = None
        for e in range(2):
            u, kf, v, qf, do = stage[e]
            (pa, da), (pb, db) = mids[e]
            dv = nn(pb, do[256:])
            dv = jnp.concatenate([dv[:256] + nn(pa, do[:256]), dv[256:]], 0)
            dk = nn(db, qf[256:])
            dk = jnp.concatenate([dk[:256] + nn(da, qf[:256]), dk[256:]], 0)
            dq = jnp.concatenate([tn(da, kf[:256]), tn(db, kf)], 0)
            jb[half, :, pl.ds(pl.multiple_of(base + e * 128, 128), 128)] = dq[:, :128].astype(BF16)
            total = dq[:, 128:] if e == 0 else total + dq[:, 128:]
            keep_lanes = lane < 64 if e == 0 else lane >= 64
            dkr[...] += jnp.where(keep_lanes, dk[:, 128:], 0.0)
            kg = dk[:, :128].astype(BF16)
            vg = dv.astype(BF16)
            jc = pl.ds(pl.multiple_of((m * 2 + e) * 128, 128), 128)
            kvg[half, 0, :, jc] = kg
            kvg[half, 1, :, jc] = vg
            ng[...] += nt(jnp.concatenate([kg, vg], 1), u)
        jb[half, :, pl.ds(pl.multiple_of(base + 256, 128), 128)] = rot(total, -1.0).astype(BF16)

        @pl.when(n == 1)
        def _():
            send("j0", jb.at[other, :, 0:384], jp.at[:, 0:384], mate, "j0")
            send("kv0", kvg.at[other, :, :, 0:256], kvgp.at[:, :, 0:256], mate, "kv0")

        return carry

    lax.fori_loop(0, 4, pair, 0)
    mark("post")
    send("j1", jb.at[other, :, 384:768], jp.at[:, 384:768], mate)
    send("kv1", kvg.at[other, :, :, 256:512], kvgp.at[:, :, 256:512], mate)
    relay(1, A0, part, rx, ra)

    gterm = jnp.zeros((1, 512), F32)
    for n in range(4):
        rows = slice(n * 128, (n + 1) * 128)
        unit = acc[rows, 0:512]
        grad = ng[rows]
        gterm = gterm + jnp.sum(grad * unit, axis=0, keepdims=True)
        scaled = grad * gain
        inner = jnp.mean(scaled * unit, axis=-1, keepdims=True)
        value = (invr[rows, 0:1] * (scaled - unit * inner)).astype(BF16)
        jb[0, rows, 768:1024] = value[:, :256]
        jb[1, rows, 768:1024] = value[:, 256:]
    dk = dkr[...]
    rope = jnp.where(lane < 64, rot(dk + pltpu.roll(dk, 64, 1), -1.0), 0.0)
    rgf[...] = rope.astype(BF16)
    rg[0] = jnp.where(lane < 32, rope, 0.0).astype(BF16)
    rg[1] = jnp.where(lane < 32, pltpu.roll(rope, 96, 1), 0.0).astype(BF16)
    send(("jl",), jb.at[other, :, 768:1024], jp.at[:, 768:1024], mate)
    send(("rg",), rg.at[other], rgp, mate)
    column = jnp.broadcast_to(gterm, (128, 512)).T
    column = jnp.where(lane == 32, column, 0.0).reshape(64, 8, 128)
    gmat[...] = jnp.concatenate([column, jnp.zeros((64, 24, 128), F32)], 1).reshape(4, 4, 4, 32, 128)

    tgd = []

    def token_block():
        n = len(tgd)
        w = wbuf[n].reshape(512, WCOL)
        cols = [jb[0, :, 768:], jb[1, :, 768:], rgf[...]]
        cols += [jb[m % 2, :, m // 2 * 384:m // 2 * 384 + 384] for m in range(4)]
        tgb[n] = nt(jnp.concatenate(cols, 1), w).astype(BF16)
        d = pltpu.make_async_copy(tgb.at[n], tg_hbm.at[:, n * 512:(n + 1) * 512], lsem.at[9])
        d.start()
        tgd.append(d)

    mark("waitmate")
    arrived(("nrt",), nrt.at[:, 512:1024])
    arrived("kv0", kvgp.at[:, :, 0:256])
    arrived("kv1", kvgp.at[:, :, 256:512])
    mark("firstU")
    products_u()
    arrived("j1", jp.at[:, 384:768])
    mark("firstA1")
    products(1)
    mark("secondA0")
    second_sends(A0)
    arrived(("jl",), jp.at[:, 768:1024])
    arrived(("rg",), rgp)
    mark("productsB")
    products_b()
    mark("relayU")
    relay(1, U, part, rx, ra)
    mark("relayA1")
    relay(1, A1, part, rx, ra)
    mark("relay2A0")
    relay(2, A0, part2, rx2, ra2)
    mark("tg")
    token_block()
    token_block()
    mark("relayB")
    relay(1, B, part, rx, ra)
    mark("tg")
    token_block()
    token_block()
    mark("thirdA0")
    third_sends(A0)
    mark("secondU")
    second_sends(U)
    mark("secondA1")
    second_sends(A1)
    mark("secondB")
    second_sends(B)
    mark("relay2U")
    relay(2, U, part2, rx2, ra2)
    mark("relay2A1")
    relay(2, A1, part2, rx2, ra2)
    mark("relay2B")
    relay(2, B, part2, rx2, ra2)
    mark("thirdA1")
    third_sends(U)
    third_sends(A1)
    mark("thirdB")
    third_sends(B)
    mark("lastA")
    last_sums(A0)
    last_sums(U)
    last_sums(A1)
    send(("fin", 0), fin_ref.at[ic, :, 0:1024], fin_ref.at[ic, :, 0:1024], mate)
    mark("lastB")
    last_sums(B)
    send(("fin", 1), fin_ref.at[ic, :, 1024:GTOT], fin_ref.at[ic, :, 1024:GTOT], mate)
    mark("fin")
    arrived(("fin", 0), fin_ref.at[other, :, 0:1024])
    arrived(("fin", 1), fin_ref.at[other, :, 1024:GTOT])

    both = fin_ref[...]
    tail = GTOT - 128
    gains = both[0, :, tail:] + both[1, :, tail:]
    body = both[:, :, :tail]
    squares = jnp.sum(jnp.sum(body * body, axis=0), axis=0, keepdims=True)
    row = sum(squares[:, n * 128:(n + 1) * 128] for n in range(10))
    ropes = jnp.where(lane == 32, 0.0, both[0, :, tail:] ** 2 + both[1, :, tail:] ** 2)
    ropes = ropes + jnp.where(lane == 32, gains * gains, 0.0)
    row = row + jnp.sum(ropes, axis=0, keepdims=True)
    row = jnp.broadcast_to(row, (8, 128))
    mark("norm")
    lead = ic == 1
    for n, axis in enumerate((AY, AX, AZ)):
        @pl.when(lead)
        def _():
            nbuf[n, 3] = row if n == 0 else (nbuf[n - 1, 0] + nbuf[n - 1, 1]) + (nbuf[n - 1, 2] + nbuf[n - 1, 3])
            for m, by in enumerate((1, -1, 2)):
                send(("n", n), nbuf.at[n, 3], nbuf.at[n, m], {axis: step(axis, by)}, ("n", n))

        @pl.when(lead)
        def _():
            arrived(("n", n), nbuf.at[n, 0:3])

    @pl.when(lead)
    def _():
        nbuf[3, 0] = (nbuf[2, 0] + nbuf[2, 1]) + (nbuf[2, 2] + nbuf[2, 3])
        send("nd", nbuf.at[3, 0], nbuf.at[3, 0], mate, "nd")
        for n in range(3):
            left(("n", n), nbuf.at[n, 0:3])
        left("nd", nbuf.at[3, 0])

    @pl.when(jnp.logical_not(lead))
    def _():
        arrived("nd", nbuf.at[3, 0])

    total = jnp.sum(nbuf[3, 0], axis=-1, keepdims=True)
    clip = jnp.minimum(1.0, lax.rsqrt(total / NPARAM + 1e-06))
    clip_ref[...] = jnp.broadcast_to(clip, (8, 128))

    mark("drain")
    for key, ref in owed:
        left(key, ref)
    left("j0", jb.at[0, :, 0:384])
    left("kv0", kvg.at[0, :, :, 0:256])
    left("g", gbuf.at[0:3, 0])
    left("gd", gbuf.at[:, 0])
    for kind in KINDS:
        if kind == "u":
            left(("links", kind), ubuf.at[0:3, 0])
            left(("d", kind), ubuf.at[:, 0])
        else:
            lo, hi = SUBS[kind]
            left(("links", kind), wbuf.at[0:3, 0, :, :, lo:hi])
            left(("d", kind), wbuf.at[:, 0, :, :, lo:hi])
    for u in range(nu):
        left(("s", 1, u), part[u].at[0:3])
        left(("s", 2, u), part2[u].at[0:3])
        left(("s", 3, u), part3[u])
    pltpu.make_async_copy(tgb, tgb, lsem.at[9]).wait()
    mark(None)
    assert len(recv_table) == NRECV and len(send_table) == NSEND, (len(recv_table), len(send_table))


NRECV = 99
NSEND = 57


def scratch():
    v = pltpu.VMEM
    dma = pltpu.SemaphoreType.DMA
    shapes = [
        v((512, 2048), BF16), v((512, 1024), BF16), v((512, 128), F32), v((512, 128), F32),
        v((4, 2, 8, 32, WCOL), BF16), v((4, 2, 8, 64, 256), BF16), v((4, 2, 8, 128), F32),
        v((4, 4, 4, 32, 1024), BF16), v((512, 640), F32),
        v((512, 512), BF16), v((512, 1024), BF16), v((512, 512), BF16), v((512, 1024), BF16),
        v((512, 512), F32), v((2, 512, 128), BF16), v((512, 128), F32),
        v((2, 512, 1024), BF16), v((512, 1024), BF16), v((2, 2, 512, 512), BF16), v((2, 512, 512), BF16),
        v((2, 512, 128), BF16), v((512, 128), BF16), v((512, 128), BF16), v((512, 128), F32),
        v((4, 4, 4, 32, 128), F32), v((4, 512, 512), BF16), v((4, 4, 8, 128), F32),
        v((256, 1536), BF16), v((576, 256), BF16), v((1, 64), BF16),
        dma((10,)), dma((NSEND,)), dma((NRECV,)),
    ]
    ws = [w for w, *_ in UNITS]
    shapes += [v((4, 4, 4, 32, w), BF16) for w in ws]
    shapes += [v((4, 4, 32, w), F32) for w in ws]
    shapes += [v((2, 2, 4, 32, w), BF16) for w in ws]
    shapes += [v((2, 4, 4, 32, w), BF16) for w in ws]
    shapes += [v((4, 4, 32, w), BF16) for w in ws]
    shapes += [v((2, 2, 32, w), BF16) for w in ws]
    shapes += [v((2, 4, 32, w), BF16) for w in ws]
    shapes += [v((3, 32, w), BF16) for w in ws]
    shapes += [v((3, 32, w), BF16) for w in ws]
    return shapes


def last_step(fin_hbm, clip_hbm, tg_in, gq_ref, gd_ref, gu_ref, gg_ref, tg_out,
              fin_ref, clip_ref, stage, isem, osem):
    ic = lax.axis_index(AC)
    first_reads = []
    for n, (src, dst) in enumerate(((fin_hbm, fin_ref), (clip_hbm, clip_ref))):
        d = pltpu.make_async_copy(src, dst, isem.at[4 + n])
        d.start()
        first_reads.append(d)
    reads = []
    for n in range(4):
        rows = slice(n * 128, (n + 1) * 128)
        d = pltpu.make_async_copy(tg_in.at[rows], stage.at[n], isem.at[n])
        d.start()
        reads.append(d)
    writes = []
    for n in range(4):
        rows_n = slice(n * 128, (n + 1) * 128)
        reads[n].wait()
        d = pltpu.make_async_copy(stage.at[n], tg_out.at[rows_n], osem.at[n])
        d.start()
        writes.append(d)
    for d in first_reads:
        d.wait()
    clip = clip_ref[0:1, 0:1]
    first = ic == 0

    def rows(half, cols):
        return jnp.where(first, fin_ref[half, 0:16, cols], fin_ref[half, 16:32, cols]) * clip

    def cols(lo):
        return slice(lo, lo + 128)

    for n in range(4):
        half, lo = n % 2, n // 2 * 384
        rope = rows(half, cols(lo + 256))
        gq_ref[:, n * 384:(n + 1) * 384] = jnp.concatenate(
            [rows(half, cols(lo)), rope[:, :64], rows(half, cols(lo + 128)), rope[:, 64:]], 1)
        gd_ref[:, n * 128:(n + 1) * 128] = rows(n // 2, cols(1024 + n % 2 * 128))
    tail = slice(GTOT - 128, GTOT)
    gd_ref[:, 512:576] = jnp.concatenate([rows(0, tail)[:, :32], rows(1, tail)[:, :32]], 1)
    for h in range(H):
        half, j = h // 2 % 2, h // 4 * 2 + h % 2
        for u in range(2):
            block = fin_ref[half, j * 8:j * 8 + 8, cols(768 + u * 128)] * clip
            gu_ref[:, h * 256 + u * 128:h * 256 + u * 128 + 128] = jnp.where(first, block[0:4], block[4:8])
    gain = (fin_ref[0, 0:8, tail] + fin_ref[1, 0:8, tail]) * clip
    gain = jnp.where(first, gain[0:4], gain[4:8])
    spread = (lax.broadcasted_iota(jnp.int32, (4, 128), 0)
              == lax.broadcasted_iota(jnp.int32, (4, 128), 1))
    gg_ref[...] = jnp.sum(jnp.where(spread, gain[:, 32:33], 0.0), axis=0)[0:4]
    for d in writes:
        d.wait()


def finish(fin, clip, token_grad):
    vm = pl.BlockSpec(memory_space=pltpu.VMEM)
    anyspace = pl.BlockSpec(memory_space=pl.ANY)
    return pl.pallas_call(
        last_step,
        out_shape=(
            jax.ShapeDtypeStruct((16, 1536), F32),
            jax.ShapeDtypeStruct((16, 576), F32),
            jax.ShapeDtypeStruct((4, 2048), F32),
            jax.ShapeDtypeStruct((4,), F32),
            jax.ShapeDtypeStruct((SEQ, D), BF16),
        ),
        in_specs=[anyspace] * 3,
        out_specs=(vm, vm, vm, vm, anyspace),
        scratch_shapes=[
            pltpu.VMEM((2, 32, GTOT), F32), pltpu.VMEM((8, 128), F32),
            pltpu.VMEM((4, 128, D), BF16), pltpu.SemaphoreType.DMA((6,)), pltpu.SemaphoreType.DMA((4,))],
    )(fin, clip, token_grad)


def per_device(tokens, d_out, w_query, w_down, w_up, latent_gain):
    cosine, sine = rope_constants()
    vm = pl.BlockSpec(memory_space=pltpu.VMEM)
    anyspace = pl.BlockSpec(memory_space=pl.ANY)
    fin, clip, token_grad = pl.pallas_call(
        mega,
        out_shape=(
            jax.ShapeDtypeStruct((2, 32, GTOT), F32),
            jax.ShapeDtypeStruct((8, 128), F32),
            jax.ShapeDtypeStruct((SEQ, D), BF16),
        ),
        in_specs=[anyspace] * 8,
        out_specs=(vm, vm, anyspace),
        scratch_shapes=scratch(),
        compiler_params=pltpu.CompilerParams(
            collective_id=0, has_side_effects=True, vmem_limit_bytes=67043328),
    )(tokens, d_out, jnp.asarray(cosine), jnp.asarray(sine), w_query, w_down.T, w_up,
      latent_gain.reshape(1, 64))
    return finish(fin, clip, token_grad)


def solution(mesh):
    split = Mesh(mesh.devices.reshape(4, 4, 4, 2), NODE_LOCAL)
    return jax.shard_map(
        per_device,
        mesh=split,
        in_specs=(
            P(NODE_LOCAL, None),
            P(NODE_LOCAL, None),
            P(LOCAL, None),
            P(LOCAL, None),
            P(LOCAL, None),
            P(LOCAL),
        ),
        out_specs=(
            P(NODE_LOCAL, None),
            P(NODE_LOCAL, None),
            P(NODE_LOCAL, None),
            P(NODE_LOCAL),
            P(NODE_LOCAL, None),
        ),
        check_vma=False,
    )
```

```python
import math

import jax
import jax.numpy as jnp
import numpy as np
from jax import lax
from jax.experimental import pallas as pl
from jax.experimental.pallas import tpu as pltpu
from jax.sharding import Mesh
from jax.sharding import PartitionSpec as P

H = 8
DN = 128
DR = 64
DV = 128
KVL = 512
SEQ = 512
D = 2048
NPARAM = 5374464
EPSILON = 1e-06
ROPE_BASE = 10000.0
LOCAL = ("local_0", "local_1")
NODE_LOCAL = ("node_0", "node_1", "local_0", "local_1")
MESH = pl.DeviceIdType.MESH
AZ, AX, AY, AC = NODE_LOCAL

WCOL = 2176
SUBS = ((0, 640), (640, 1408), (1408, 2176))
SCALE = 1.0 / math.sqrt(DN + DR)
AXES = ((AZ, AX, AY), (AX, AY, AZ), (AY, AZ, AX))
GRP = (0, 1, 2, 0, 1, 2, 0, 1, 0, 1, 2)
UNITS = tuple((128,) + AXES[g] for g in GRP)
GOFF = tuple(128 * n for n in range(len(GRP)))
GTOT = 1408
F32 = jnp.float32
BF16 = jnp.bfloat16


def rope_constants():
    position = np.arange(SEQ, dtype=np.float32)[:, None]
    freq = np.float32(ROPE_BASE) ** (-np.arange(DR // 2, dtype=np.float32) * np.float32(2.0 / DR))
    angle = (position * freq[None, :].astype(np.float32)).astype(np.float32)
    cosine = np.cos(angle).astype(np.float32)
    sine = np.sin(angle).astype(np.float32)
    return np.concatenate([cosine] * 4, 1), np.concatenate([-sine, sine] * 2, 1)


def nt(a, b):
    return lax.dot_general(a, b, (((1,), (1,)), ((), ())), preferred_element_type=F32)


def nn(a, b):
    return jnp.dot(a, b, preferred_element_type=F32)


def tn(a, b):
    return lax.dot_general(a, b, (((0,), (0,)), ((), ())), preferred_element_type=F32)


def mega(
    tokens_hbm, dout_hbm, cos_hbm, sin_hbm, wq_hbm, wd_hbm, wu_hbm, gain_hbm,
    fin_ref, clip_ref, tg_ref,
    tokens, dout, cosr, sinr, wbuf, ubuf, gbuf, tokt, acc, qrope, qnope, nrm, nrt, ng, krp, dkr,
    jb, jp, kvg, kvgp, rg, rgp, rgf, invr, gmat, nbuf, wq_ref, wd_ref, gain_ref, lsem, ssem, rsem, *rest,
):
    nu = len(UNITS)
    part, own, rx, ra, part2, rx2, ra2, part3, ra3 = (rest[n * nu:(n + 1) * nu] for n in range(9))
    iz, ix, iy, ic = (lax.axis_index(a) for a in NODE_LOCAL)
    at = {AZ: iz, AX: ix, AY: iy}
    other = 1 - ic
    STEP = {(a, by): lax.rem(at[a] + (by + 4), 4) for a in at for by in (-1, 0, 1, 2)}

    def step(axis, by):
        return STEP[axis, by]

    recv_table, send_table, owed = {}, {}, []
    scope = []

    def mark(name):
        while scope:
            scope.pop().__exit__(None, None, None)
        if name:
            scope.append(jax.named_scope(name))
            scope[-1].__enter__()

    mark("start")

    def index(table, key):
        return table.setdefault(key, len(table))

    def send(key, src, dst, peer, outgoing=None):
        if outgoing is None:
            outgoing = key
            owed.append((key, src))
        pltpu.make_async_remote_copy(
            src_ref=src, dst_ref=dst,
            send_sem=ssem.at[index(send_table, outgoing)], recv_sem=rsem.at[index(recv_table, key)],
            device_id=peer, device_id_type=MESH).start()

    def arrived(key, ref):
        pltpu.make_async_remote_copy(
            src_ref=ref, dst_ref=ref, send_sem=ssem.at[0], recv_sem=rsem.at[index(recv_table, key)],
            device_id=mate, device_id_type=MESH).wait_recv()

    def left(key, ref):
        pltpu.make_async_remote_copy(
            src_ref=ref, dst_ref=ref, send_sem=ssem.at[index(send_table, key)], recv_sem=rsem.at[0],
            device_id=mate, device_id_type=MESH).wait_send()

    mate = {AC: other}
    barrier = pltpu.get_barrier_semaphore()
    for axis in (AZ, AX, AY):
        for by in (1, -1, 2):
            pl.semaphore_signal(barrier, inc=1, device_id={axis: step(axis, by)}, device_id_type=MESH)
    pl.semaphore_signal(barrier, inc=1, device_id=mate, device_id_type=MESH)

    loads = {}

    def load(name, src, dst):
        d = pltpu.make_async_copy(src, dst, lsem.at[len(loads)])
        d.start()
        loads[name] = d

    for p in range(8):
        pltpu.make_async_copy(wu_hbm.at[:, p * 256:(p + 1) * 256], ubuf.at[iy, ic, p], lsem.at[8]).start()

    load("down", wd_hbm, wd_ref)
    load("query", wq_hbm, wq_ref)
    load("gain", gain_hbm, gain_ref)
    load("tokens", tokens_hbm, tokens)
    load("dout", dout_hbm, dout)
    load("cos", cos_hbm, cosr)
    load("sin", sin_hbm, sinr)

    loads["down"].wait()
    down = jnp.concatenate([wd_ref[...], jnp.zeros((64, 256), BF16)], 0)
    wbuf[iy, ic, :, :, 0:640] = down.T.reshape(8, 32, 640)
    loads["query"].wait()
    for n in range(4):
        lo = 640 + n * 384
        h = n * 384
        both = jnp.concatenate([
            wq_ref[:, h:h + 128], wq_ref[:, h + 192:h + 320],
            wq_ref[:, h + 128:h + 192], wq_ref[:, h + 320:h + 384]], 1)
        wbuf[iy, ic, :, :, lo:lo + 384] = both.reshape(8, 32, 384)
    loads["gain"].wait()
    gbuf[iy, ic] = jnp.broadcast_to(
        jnp.concatenate([gain_ref[...].astype(F32), jnp.zeros((1, 64), F32)], 1), (8, 128))
    own_up = ubuf.at[iy, ic]
    pltpu.make_async_copy(own_up, own_up, lsem.at[8]).wait()
    pl.semaphore_wait(barrier, 10)

    RING = (AX, AZ)
    YO = (step(AY, -1), step(AY, 1), step(AY, 2))
    PIECE = {(k, by): k * 4 + step(RING[k], by) for k in range(2) for by in (-1, 0, 1, 2)}
    KINDS = (0, "u", 1, 2)

    def block_of(kind, yy, core):
        if kind == "u":
            return ubuf.at[yy, core]
        lo, hi = SUBS[kind]
        return wbuf.at[yy, core, :, :, lo:hi]

    def piece(kind, yy, k, by):
        if kind == "u":
            return ubuf.at[yy, ic, PIECE[k, by]]
        lo, hi = SUBS[kind]
        return wbuf.at[yy, ic, PIECE[k, by], :, lo:hi]

    def half_piece(kind, yy, k, by, d):
        if kind == "u":
            return ubuf.at[yy, ic, PIECE[k, by], d * 32:d * 32 + 32]
        lo, hi = SUBS[kind]
        return wbuf.at[yy, ic, PIECE[k, by], d * 16:d * 16 + 16, lo:hi]

    def span(kind, n):
        if kind == "u":
            return ubuf.at[0, 0, 0:n]
        lo, hi = SUBS[kind]
        return wbuf.at[0, 0, 0:n, :, lo:hi]

    def link_send(key, kind, r, axis, by):
        send(key, r, r, {axis: step(axis, by)}, ("links", kind))

    def piece_to_mate(kind, yo, k, by):
        r = piece(kind, YO[yo], k, by)
        send(("d", kind), r, r, mate, ("d", kind))

    def y_send(kind):
        for k in range(2):
            r = piece(kind, iy, k, 0)
            link_send(("y", kind), kind, r, AY, 1)
            link_send(("y", kind), kind, r, AY, -1)

    def pset(yo):
        return yo // 2

    def p_send(kind, k, yo):
        r = piece(kind, YO[yo], k, 0)
        link_send(("p", kind, pset(yo)), kind, r, RING[k], 1)
        link_send(("p", kind, pset(yo)), kind, r, RING[k], -1)

    def y_take(kind):
        arrived(("y", kind), span(kind, 4))
        for k in range(2):
            for d in range(2):
                half = half_piece(kind, YO[d], k, 0, d)
                link_send(("y2", kind), kind, half, AY, 1 if d == 0 else -1)
                p_send(kind, k, d)
        for k in range(2):
            for d in range(2):
                piece_to_mate(kind, d, k, 0)

    def y2_take(kind):
        arrived(("y2", kind), span(kind, 2))
        for k in range(2):
            p_send(kind, k, 2)
            piece_to_mate(kind, 2, k, 0)

    def p_take(kind, *yos):
        arrived(("p", kind, pset(yos[0])), span(kind, 4 * len(yos)))
        for yo in yos:
            for k in range(2):
                for d in range(2):
                    by = -1 if d == 0 else 1
                    half = half_piece(kind, YO[yo], k, by, d)
                    link_send(("p2", kind, pset(yo)), kind, half, RING[k], -by)
        for yo in yos:
            for k in range(2):
                for by in (-1, 1):
                    piece_to_mate(kind, yo, k, by)

    def p2_take(kind, *yos):
        arrived(("p2", kind, pset(yos[0])), span(kind, 2 * len(yos)))
        for yo in yos:
            for k in range(2):
                piece_to_mate(kind, yo, k, 2)

    def own_to_mate(kind):
        r = block_of(kind, iy, ic)
        send(("d", kind), r, r, mate, ("d", kind))

    def from_mate(kind):
        if kind == "u":
            arrived(("d", kind), ubuf.at[:, other])
        else:
            lo, hi = SUBS[kind]
            arrived(("d", kind), wbuf.at[:, other, :, :, lo:hi])

    def project(lo, hi):
        return nn(tokens[...], wbuf[:, :, :, :, lo:hi].reshape(2048, hi - lo))

    mark("gather")
    y_send(0)
    y_send("u")
    y_send(1)
    own_to_mate(0)
    g = gbuf.at[iy, ic]
    for n, by in enumerate((1, -1, 2)):
        send("g", g, g, {AY: step(AY, by)}, "g")
    send("gd", g, g, mate, "gd")
    own_to_mate("u")
    mark("y0")
    y_take(0)
    own_to_mate(1)
    mark("yu")
    y_take("u")
    y_send(2)
    own_to_mate(2)
    loads["tokens"].wait()
    mark("transpose")
    for z in range(2):
        tokt[z, :, :, :, 0:512] = tokens[:, z * 512:(z + 1) * 512].T.reshape(4, 4, 32, 512)
    mark("y20")
    y2_take(0)
    mark("p0a")
    p_take(0, 0, 1)
    mark("y1")
    y_take(1)
    mark("y2u")
    y2_take("u")
    mark("pua")
    p_take("u", 0, 1)
    mark("p0b")
    p_take(0, 2)
    mark("transpose")
    for z in range(2, 4):
        tokt[z, :, :, :, 0:512] = tokens[:, z * 512:(z + 1) * 512].T.reshape(4, 4, 32, 512)
    mark("y21")
    y2_take(1)
    mark("p1a")
    p_take(1, 0, 1)
    mark("pub")
    p_take("u", 2)
    mark("p20")
    p2_take(0, 0, 1)
    mark("y2")
    y_take(2)
    mark("p202")
    p2_take(0, 2)
    mark("p1b")
    p_take(1, 2)
    mark("y22")
    y2_take(2)
    mark("g")
    arrived("g", gbuf.at[0:3, 0])
    for by in (-1, 1, 2):
        gg = gbuf.at[step(AY, by), ic]
        send("gd", gg, gg, mate, "gd")
    mark("down")
    from_mate(0)
    acc[...] = project(*SUBS[0])
    mark("p2u")
    p2_take("u", 0, 1)
    p2_take("u", 2)
    mark("p2a")
    p_take(2, 0, 1)
    mark("p21")
    p2_take(1, 0, 1)
    p2_take(1, 2)
    mark("pre")
    arrived("gd", gbuf.at[:, other])

    for name in ("dout", "cos", "sin"):
        loads[name].wait()

    lane = lax.broadcasted_iota(jnp.int32, (1, 128), 1)
    low = lax.rem(lane, 64) < 32

    def swap(v):
        return jnp.where(low, pltpu.roll(v, 96, 1), pltpu.roll(v, 32, 1))

    def rot(v, sign):
        return v * cosr[...] + swap(v) * (sinr[...] * sign)

    gain = jnp.concatenate([gbuf[y, c, 0:1, 0:64] for y in range(4) for c in range(2)], 1)
    kr = rot(acc[:, 512:640], 1.0)
    krp[0] = jnp.where(lane < 64, kr, 0.0).astype(BF16)
    krp[1] = jnp.where(lane < 64, 0.0, pltpu.roll(kr, 64, 1)).astype(BF16)
    for n in range(4):
        rows = slice(n * 128, (n + 1) * 128)
        latent = acc[rows, 0:512]
        inv = lax.rsqrt(jnp.mean(latent * latent, axis=-1, keepdims=True) + EPSILON)
        unit = latent * inv
        acc[rows, 0:512] = unit
        invr[rows] = jnp.broadcast_to(inv, (128, 128))
        nrm[rows] = (unit * gain).astype(BF16)
    nrt[:, 0:512] = nrm[...].T
    send(("nrt",), nrt.at[:, 0:512], nrt.at[:, 512:1024], mate)
    ng[...] = jnp.zeros((512, 512), F32)
    dkr[...] = jnp.zeros((512, 128), F32)
    send("tok", tokt.at[:, :, :, :, 0:512], tokt.at[:, :, :, :, 512:1024], mate)
    mark("p2b")
    p_take(2, 2)
    mark("mateu")
    from_mate("u")
    mark("heads")

    tri = (lax.broadcasted_iota(jnp.int32, (256, 256), 0)
           <= lax.broadcasted_iota(jnp.int32, (256, 256), 1))

    def block(kf, v, qf, do):
        rows = kf.shape[0]
        s = nt(kf, qf) * SCALE
        masked = jnp.where(tri, s[rows - 256:], -1e30)
        s = masked if rows == 256 else jnp.concatenate([s[:rows - 256], masked], 0)
        w = jnp.exp(s - jnp.max(s, axis=0, keepdims=True))
        probs = w * (1.0 / jnp.sum(w, axis=0, keepdims=True))
        dp = nt(v, do)
        delta = jnp.sum(probs * dp, axis=0, keepdims=True)
        ds = (probs * (dp - delta) * SCALE).astype(BF16)
        return probs.astype(BF16), ds

    A0, A1, U, B = (0, 1, 2), (3, 4, 5), (6, 7), (8, 9, 10)
    def keep(u, z, cols, value):
        g = GRP[u]
        value = value.astype(BF16)
        if g == 0:
            part[u][z, :, :, :, cols] = value
        elif g == 1:
            part[u][:, z, :, :, cols] = value
        else:
            for x in range(4):
                part[u][:, z, x, :, cols] = value[x]

    def token_rows(z):
        return tokt[z].reshape(512, 1024)

    def products(slot):
        cols = slice(slot * 384, slot * 384 + 384)
        right = jnp.concatenate([jb[ic, :, cols], jp[:, cols]], 0)
        us = A1 if slot else A0
        for z in range(4):
            both = nn(token_rows(z), right).reshape(4, 4, 32, 384)
            for n, u in enumerate(us):
                keep(u, z, slice(0, 128), both[..., n * 128:n * 128 + 128])
        for u in us:
            ring_sends(1, u, part, rx, ra)

    def products_b():
        right = jnp.concatenate([
            jnp.concatenate([jb[ic, :, 768:1024], rg[ic]], 1),
            jnp.concatenate([jp[:, 768:1024], rgp[...]], 1)], 0)
        for z in range(4):
            both = nn(token_rows(z), right).reshape(4, 4, 32, 384)
            for u in (8, 9):
                keep(u, z, slice(0, 128), both[..., (u - 8) * 128:(u - 7) * 128])
            keep(10, z, slice(0, 128), both[..., 256:] + gmat[z])
        for u in B:
            ring_sends(1, u, part, rx, ra)

    def products_u():
        for u in U:
            up = nn(nrt[...], jnp.concatenate([kvg[ic, u - 6], kvgp[u - 6]], 0))
            up = up.reshape(64, 8, 512)
            up = jnp.concatenate([up[:, :, j * 128:(j + 1) * 128] for j in range(4)], 1)
            up = up.reshape(4, 4, 4, 32, 128)
            for z in range(4):
                keep(u, z, slice(0, 128), up[z])
            ring_sends(1, u, part, rx, ra)

    def ways(axis):
        return {axis: step(axis, 1)}, {axis: step(axis, -1)}

    def ring_sends(phase, u, p, r, a):
        axis = UNITS[u][phase]
        right, left_ = ways(axis)
        far, near, back = (p[u].at[step(axis, by)] for by in (2, 1, -1))
        send(("x", phase, u), far.at[0:2], r[u].at[0], right, ("s", phase, u))
        send(("x", phase, u), far.at[2:4], r[u].at[1], left_, ("s", phase, u))
        send(("a", phase, u), near.at[2:4], a[u].at[0, 2:4], right, ("s", phase, u))
        send(("a", phase, u), back.at[0:2], a[u].at[1, 0:2], left_, ("s", phase, u))

    def relay(phase, us, p, r, a):
        for u in us:
            axis = UNITS[u][phase]
            right, left_ = ways(axis)
            near, back = (p[u].at[step(axis, by)] for by in (1, -1))
            arrived(("x", phase, u), r[u])
            near[0:2] = (near[0:2].astype(F32) + r[u][0].astype(F32)).astype(BF16)
            back[2:4] = (back[2:4].astype(F32) + r[u][1].astype(F32)).astype(BF16)
            send(("a", phase, u), near.at[0:2], a[u].at[0, 0:2], right, ("s", phase, u))
            send(("a", phase, u), back.at[2:4], a[u].at[1, 2:4], left_, ("s", phase, u))

    def second(u, t):
        return own[u].at[:, t] if GRP[u] == 1 else own[u].at[t]

    def second_sends(us):
        for u in us:
            arrived(("a", 1, u), ra[u])
            total = part[u][at[UNITS[u][1]]].astype(F32) + (ra[u][0].astype(F32) + ra[u][1].astype(F32))
            own[u][...] = total
            if GRP[u] == 1:
                for z in range(4):
                    part2[u][:, z] = total[z].astype(BF16)
            else:
                part2[u][...] = total.astype(BF16)
            ring_sends(2, u, part2, rx2, ra2)

    def third_sends(us):
        for u in us:
            arrived(("a", 2, u), ra2[u])
            mine = second(u, at[UNITS[u][2]])
            mine[...] += ra2[u][0].astype(F32) + ra2[u][1].astype(F32)
            for slot, by in enumerate((2, 1, -1)):
                part3[u][slot] = mine[step(UNITS[u][3], by)].astype(BF16)
                send(("a", 3, u), part3[u].at[slot], ra3[u].at[slot],
                     {UNITS[u][3]: step(UNITS[u][3], by)}, ("s", 3, u))

    def last_sums(us):
        for u in us:
            arrived(("a", 3, u), ra3[u])
            mine = second(u, at[UNITS[u][2]])[at[UNITS[u][3]]]
            fin_ref[ic, :, GOFF[u]:GOFF[u] + UNITS[u][0]] = mine + (
                ra3[u][0].astype(F32) + ra3[u][1].astype(F32) + ra3[u][2].astype(F32))

    def queries(s):
        from_mate(s + 1)
        lo = SUBS[s + 1][0]
        q = project(lo, lo + 768)
        for m in range(2):
            n = 2 * s + m
            qnope[:, n * 256:(n + 1) * 256] = q[:, m * 384:m * 384 + 256].astype(BF16)
            rope = q[:, m * 384 + 256:m * 384 + 384].astype(BF16).astype(F32)
            qrope[:, n * 128:(n + 1) * 128] = rot(rope, 1.0).astype(BF16)

    def pair(n, carry):
        @pl.when(n == 0)
        def _():
            queries(0)

        @pl.when(n == 1)
        def _():
            p2_take(2, 0, 1)
            p2_take(2, 2)

        @pl.when(n == 2)
        def _():
            queries(1)
            arrived("tok", tokt.at[:, :, :, :, 512:1024])
            arrived("j0", jp.at[:, 0:384])
            products(0)

        half, m = lax.rem(n, 2), n // 2
        base = m * 384
        qr = qrope[:, pl.ds(pl.multiple_of(n * 128, 128), 128)]
        stage = []
        for e in range(2):
            h = 2 * n + e
            hc = pl.ds(pl.multiple_of(h * 128, 128), 128)
            u = ubuf[:, :, h].reshape(512, 256)
            kv = nn(nrm[...], u).astype(BF16)
            kf = jnp.concatenate([kv[:, :128], krp[e]], 1)
            v = kv[:, 128:]
            qf = jnp.concatenate([qnope[:, hc], qr], 1)
            do = dout[:, hc]
            stage.append((u, kf, v, qf, do))
        mids = []
        for u, kf, v, qf, do in stage:
            mids.append((block(kf[:256], v[:256], qf[:256], do[:256]), block(kf, v, qf[256:], do[256:])))
        total = None
        for e in range(2):
            u, kf, v, qf, do = stage[e]
            (pa, da), (pb, db) = mids[e]
            dv = nn(pb, do[256:])
            dv = jnp.concatenate([dv[:256] + nn(pa, do[:256]), dv[256:]], 0)
            dk = nn(db, qf[256:])
            dk = jnp.concatenate([dk[:256] + nn(da, qf[:256]), dk[256:]], 0)
            dq = jnp.concatenate([tn(da, kf[:256]), tn(db, kf)], 0)
            jb[half, :, pl.ds(pl.multiple_of(base + e * 128, 128), 128)] = dq[:, :128].astype(BF16)
            total = dq[:, 128:] if e == 0 else total + dq[:, 128:]
            keep_lanes = lane < 64 if e == 0 else lane >= 64
            dkr[...] += jnp.where(keep_lanes, dk[:, 128:], 0.0)
            kg = dk[:, :128].astype(BF16)
            vg = dv.astype(BF16)
            jc = pl.ds(pl.multiple_of((m * 2 + e) * 128, 128), 128)
            kvg[half, 0, :, jc] = kg
            kvg[half, 1, :, jc] = vg
            ng[...] += nt(jnp.concatenate([kg, vg], 1), u)
        jb[half, :, pl.ds(pl.multiple_of(base + 256, 128), 128)] = rot(total, -1.0).astype(BF16)

        @pl.when(n == 1)
        def _():
            send("j0", jb.at[other, :, 0:384], jp.at[:, 0:384], mate, "j0")
            send("kv0", kvg.at[other, :, :, 0:256], kvgp.at[:, :, 0:256], mate, "kv0")

        return carry

    lax.fori_loop(0, 4, pair, 0)
    mark("post")
    send("j1", jb.at[other, :, 384:768], jp.at[:, 384:768], mate)
    send("kv1", kvg.at[other, :, :, 256:512], kvgp.at[:, :, 256:512], mate)
    relay(1, A0, part, rx, ra)

    gterm = jnp.zeros((1, 512), F32)
    for n in range(4):
        rows = slice(n * 128, (n + 1) * 128)
        unit = acc[rows, 0:512]
        grad = ng[rows]
        gterm = gterm + jnp.sum(grad * unit, axis=0, keepdims=True)
        scaled = grad * gain
        inner = jnp.mean(scaled * unit, axis=-1, keepdims=True)
        value = (invr[rows, 0:1] * (scaled - unit * inner)).astype(BF16)
        jb[0, rows, 768:1024] = value[:, :256]
        jb[1, rows, 768:1024] = value[:, 256:]
    dk = dkr[...]
    rope = jnp.where(lane < 64, rot(dk + pltpu.roll(dk, 64, 1), -1.0), 0.0)
    rgf[...] = rope.astype(BF16)
    rg[0] = jnp.where(lane < 32, rope, 0.0).astype(BF16)
    rg[1] = jnp.where(lane < 32, pltpu.roll(rope, 96, 1), 0.0).astype(BF16)
    send(("jl",), jb.at[other, :, 768:1024], jp.at[:, 768:1024], mate)
    send(("rg",), rg.at[other], rgp, mate)
    column = jnp.broadcast_to(gterm, (128, 512)).T
    column = jnp.where(lane == 32, column, 0.0).reshape(64, 8, 128)
    gmat[...] = jnp.concatenate([column, jnp.zeros((64, 24, 128), F32)], 1).reshape(4, 4, 4, 32, 128)

    tgd = []

    def token_block():
        n = len(tgd)
        w = wbuf[n].reshape(512, WCOL)
        cols = [jb[0, :, 768:], jb[1, :, 768:], rgf[...]]
        cols += [jb[m % 2, :, m // 2 * 384:m // 2 * 384 + 384] for m in range(4)]
        tg_ref[:, n * 512:(n + 1) * 512] = nt(jnp.concatenate(cols, 1), w).astype(BF16)
        tgd.append(n)

    mark("waitmate")
    arrived(("nrt",), nrt.at[:, 512:1024])
    arrived("kv0", kvgp.at[:, :, 0:256])
    arrived("kv1", kvgp.at[:, :, 256:512])
    mark("firstU")
    products_u()
    arrived("j1", jp.at[:, 384:768])
    mark("firstA1")
    products(1)
    mark("secondA0")
    second_sends(A0)
    arrived(("jl",), jp.at[:, 768:1024])
    arrived(("rg",), rgp)
    mark("productsB")
    products_b()
    mark("relayU")
    relay(1, U, part, rx, ra)
    mark("relayA1")
    relay(1, A1, part, rx, ra)
    mark("relay2A0")
    relay(2, A0, part2, rx2, ra2)
    mark("tg")
    token_block()
    token_block()
    mark("relayB")
    relay(1, B, part, rx, ra)
    mark("tg")
    token_block()
    token_block()
    mark("thirdA0")
    third_sends(A0)
    mark("secondU")
    second_sends(U)
    mark("secondA1")
    second_sends(A1)
    mark("secondB")
    second_sends(B)
    mark("relay2U")
    relay(2, U, part2, rx2, ra2)
    mark("relay2A1")
    relay(2, A1, part2, rx2, ra2)
    mark("relay2B")
    relay(2, B, part2, rx2, ra2)
    mark("thirdA1")
    third_sends(U)
    third_sends(A1)
    mark("thirdB")
    third_sends(B)
    mark("lastA")
    last_sums(A0)
    last_sums(U)
    last_sums(A1)
    send(("fin", 0), fin_ref.at[ic, :, 0:1024], fin_ref.at[ic, :, 0:1024], mate)
    mark("lastB")
    last_sums(B)
    send(("fin", 1), fin_ref.at[ic, :, 1024:GTOT], fin_ref.at[ic, :, 1024:GTOT], mate)
    mark("fin")
    arrived(("fin", 0), fin_ref.at[other, :, 0:1024])
    arrived(("fin", 1), fin_ref.at[other, :, 1024:GTOT])

    both = fin_ref[...]
    tail = GTOT - 128
    gains = both[0, :, tail:] + both[1, :, tail:]
    body = both[:, :, :tail]
    squares = jnp.sum(jnp.sum(body * body, axis=0), axis=0, keepdims=True)
    row = sum(squares[:, n * 128:(n + 1) * 128] for n in range(10))
    ropes = jnp.where(lane == 32, 0.0, both[0, :, tail:] ** 2 + both[1, :, tail:] ** 2)
    ropes = ropes + jnp.where(lane == 32, gains * gains, 0.0)
    row = row + jnp.sum(ropes, axis=0, keepdims=True)
    row = jnp.broadcast_to(row, (8, 128))
    mark("norm")
    lead = ic == 1
    for n, axis in enumerate((AY, AX, AZ)):
        @pl.when(lead)
        def _():
            nbuf[n, 3] = row if n == 0 else (nbuf[n - 1, 0] + nbuf[n - 1, 1]) + (nbuf[n - 1, 2] + nbuf[n - 1, 3])
            for m, by in enumerate((1, -1, 2)):
                send(("n", n), nbuf.at[n, 3], nbuf.at[n, m], {axis: step(axis, by)}, ("n", n))

        @pl.when(lead)
        def _():
            arrived(("n", n), nbuf.at[n, 0:3])

    @pl.when(lead)
    def _():
        nbuf[3, 0] = (nbuf[2, 0] + nbuf[2, 1]) + (nbuf[2, 2] + nbuf[2, 3])
        send("nd", nbuf.at[3, 0], nbuf.at[3, 0], mate, "nd")
        for n in range(3):
            left(("n", n), nbuf.at[n, 0:3])
        left("nd", nbuf.at[3, 0])

    @pl.when(jnp.logical_not(lead))
    def _():
        arrived("nd", nbuf.at[3, 0])

    total = jnp.sum(nbuf[3, 0], axis=-1, keepdims=True)
    clip = jnp.minimum(1.0, lax.rsqrt(total / NPARAM + 1e-06))
    clip_ref[...] = jnp.broadcast_to(clip, (8, 128))

    mark("drain")
    for key, ref in owed:
        left(key, ref)
    left("j0", jb.at[0, :, 0:384])
    left("kv0", kvg.at[0, :, :, 0:256])
    left("g", gbuf.at[0:3, 0])
    left("gd", gbuf.at[:, 0])
    for kind in KINDS:
        if kind == "u":
            left(("links", kind), ubuf.at[0:3, 0])
            left(("d", kind), ubuf.at[:, 0])
        else:
            lo, hi = SUBS[kind]
            left(("links", kind), wbuf.at[0:3, 0, :, :, lo:hi])
            left(("d", kind), wbuf.at[:, 0, :, :, lo:hi])
    for u in range(nu):
        left(("s", 1, u), part[u].at[0:3])
        left(("s", 2, u), part2[u].at[0:3])
        left(("s", 3, u), part3[u])
    mark(None)
    assert len(recv_table) == NRECV and len(send_table) == NSEND, (len(recv_table), len(send_table))


NRECV = 99
NSEND = 57


def scratch():
    v = pltpu.VMEM
    dma = pltpu.SemaphoreType.DMA
    shapes = [
        v((512, 2048), BF16), v((512, 1024), BF16), v((512, 128), F32), v((512, 128), F32),
        v((4, 2, 8, 32, WCOL), BF16), v((4, 2, 8, 64, 256), BF16), v((4, 2, 8, 128), F32),
        v((4, 4, 4, 32, 1024), BF16), v((512, 640), F32),
        v((512, 512), BF16), v((512, 1024), BF16), v((512, 512), BF16), v((512, 1024), BF16),
        v((512, 512), F32), v((2, 512, 128), BF16), v((512, 128), F32),
        v((2, 512, 1024), BF16), v((512, 1024), BF16), v((2, 2, 512, 512), BF16), v((2, 512, 512), BF16),
        v((2, 512, 128), BF16), v((512, 128), BF16), v((512, 128), BF16), v((512, 128), F32),
        v((4, 4, 4, 32, 128), F32), v((4, 4, 8, 128), F32),
        v((256, 1536), BF16), v((576, 256), BF16), v((1, 64), BF16),
        dma((10,)), dma((NSEND,)), dma((NRECV,)),
    ]
    ws = [w for w, *_ in UNITS]
    shapes += [v((4, 4, 4, 32, w), BF16) for w in ws]
    shapes += [v((4, 4, 32, w), F32) for w in ws]
    shapes += [v((2, 2, 4, 32, w), BF16) for w in ws]
    shapes += [v((2, 4, 4, 32, w), BF16) for w in ws]
    shapes += [v((4, 4, 32, w), BF16) for w in ws]
    shapes += [v((2, 2, 32, w), BF16) for w in ws]
    shapes += [v((2, 4, 32, w), BF16) for w in ws]
    shapes += [v((3, 32, w), BF16) for w in ws]
    shapes += [v((3, 32, w), BF16) for w in ws]
    return shapes


def last_step(fin_ref, clip_ref, tg_ref, gq_ref, gd_ref, gu_ref, gg_ref, tg_hbm, sem):
    whole = pltpu.make_async_copy(tg_ref, tg_hbm, sem)
    whole.start()
    ic = lax.axis_index(AC)
    clip = clip_ref[0:1, 0:1]
    first = ic == 0

    def rows(half, cols):
        return jnp.where(first, fin_ref[half, 0:16, cols], fin_ref[half, 16:32, cols]) * clip

    def cols(lo):
        return slice(lo, lo + 128)

    for n in range(4):
        half, lo = n % 2, n // 2 * 384
        rope = rows(half, cols(lo + 256))
        gq_ref[:, n * 384:(n + 1) * 384] = jnp.concatenate(
            [rows(half, cols(lo)), rope[:, :64], rows(half, cols(lo + 128)), rope[:, 64:]], 1)
        gd_ref[:, n * 128:(n + 1) * 128] = rows(n // 2, cols(1024 + n % 2 * 128))
    tail = slice(GTOT - 128, GTOT)
    gd_ref[:, 512:576] = jnp.concatenate([rows(0, tail)[:, :32], rows(1, tail)[:, :32]], 1)
    for h in range(H):
        half, j = h // 2 % 2, h // 4 * 2 + h % 2
        for u in range(2):
            block = fin_ref[half, j * 8:j * 8 + 8, cols(768 + u * 128)] * clip
            gu_ref[:, h * 256 + u * 128:h * 256 + u * 128 + 128] = jnp.where(first, block[0:4], block[4:8])
    gain = (fin_ref[0, 0:8, tail] + fin_ref[1, 0:8, tail]) * clip
    gain = jnp.where(first, gain[0:4], gain[4:8])
    spread = (lax.broadcasted_iota(jnp.int32, (4, 128), 0)
              == lax.broadcasted_iota(jnp.int32, (4, 128), 1))
    gg_ref[...] = jnp.sum(jnp.where(spread, gain[:, 32:33], 0.0), axis=0)[0:4]
    whole.wait()


def finish(fin, clip, token_grad):
    vm = pl.BlockSpec(memory_space=pltpu.VMEM)
    return tuple(pl.pallas_call(
        last_step,
        out_shape=(
            jax.ShapeDtypeStruct((16, 1536), F32),
            jax.ShapeDtypeStruct((16, 576), F32),
            jax.ShapeDtypeStruct((4, 2048), F32),
            jax.ShapeDtypeStruct((4,), F32),
            jax.ShapeDtypeStruct((SEQ, D), BF16),
        ),
        in_specs=[vm, vm, vm],
        out_specs=(vm, vm, vm, vm, pl.BlockSpec(memory_space=pl.ANY)),
        scratch_shapes=[pltpu.SemaphoreType.DMA],
        compiler_params=pltpu.CompilerParams(vmem_limit_bytes=16 * 1024 * 1024),
        cost_estimate=pl.CostEstimate(flops=4000000, bytes_accessed=800000, transcendentals=0),
    )(fin, clip, token_grad))


def per_device(tokens, d_out, w_query, w_down, w_up, latent_gain):
    cosine, sine = rope_constants()
    vm = pl.BlockSpec(memory_space=pltpu.VMEM)
    anyspace = pl.BlockSpec(memory_space=pl.ANY)
    fin, clip, token_grad = pl.pallas_call(
        mega,
        out_shape=(
            pltpu.VMEM((2, 32, GTOT), F32),
            pltpu.VMEM((8, 128), F32),
            pltpu.VMEM((SEQ, D), BF16),
        ),
        in_specs=[anyspace] * 8,
        out_specs=(vm, vm, vm),
        scratch_shapes=scratch(),
        compiler_params=pltpu.CompilerParams(
            collective_id=0, has_side_effects=True, vmem_limit_bytes=58 * 1024 * 1024),
    )(tokens, d_out, jnp.asarray(cosine), jnp.asarray(sine), w_query, w_down.T, w_up,
      latent_gain.reshape(1, 64))
    return finish(fin, clip, token_grad)


def solution(mesh):
    split = Mesh(mesh.devices.reshape(4, 4, 4, 2), NODE_LOCAL)
    return jax.shard_map(
        per_device,
        mesh=split,
        in_specs=(
            P(NODE_LOCAL, None),
            P(NODE_LOCAL, None),
            P(LOCAL, None),
            P(LOCAL, None),
            P(LOCAL, None),
            P(LOCAL),
        ),
        out_specs=(
            P(NODE_LOCAL, None),
            P(NODE_LOCAL, None),
            P(NODE_LOCAL, None),
            P(NODE_LOCAL),
            P(NODE_LOCAL, None),
        ),
        check_vma=False,
    )
```
